8 devices in a mesh: dp: 1 (over z), tp: 2 (over y), ep: 4 (over x, core).
Axes of the slice: x: 2, y: 2, z: 1, core: 2. Of those that a mesh axis runs over, the one named last changes fastest.
Arguments:
- hidden_in: bfloat16 [32, 256, 768], P(('dp', 'ep'), 'tp')
- ln_attn: float32 [2, 768], replicated
- ln_ffn: float32 [2, 768], replicated
- w_query: bfloat16 [2, 768, 768], P(None, None, 'tp')
- w_key: bfloat16 [2, 768, 768], P(None, None, 'tp')
- w_value: bfloat16 [2, 768, 768], P(None, None, 'tp')
- w_out: bfloat16 [2, 768, 768], P(None, 'tp')
- bias_table: float32 [2, 12, 32], P(None, 'tp')
- w_gate: bfloat16 [768, 3072], P(None, 'tp')
- w_up: bfloat16 [768, 3072], P(None, 'tp')
- w_down: bfloat16 [3072, 768], P('tp')
- w_router: float32 [768, 64], replicated
- expert_in: bfloat16 [64, 768, 3072], P(('tp', 'ep'))
- expert_out: bfloat16 [64, 3072, 768], P(('tp', 'ep'))
- expert_ids: int32 [32, 256, 2], P(('dp', 'ep'), 'tp')
Outputs:
- output 1: bfloat16 [32, 256, 768], P(('dp', 'ep'), 'tp')
- output 2: bfloat16 [2, 32, 12, 256, 64], P(None, ('dp', 'ep'), 'tp')
- output 3: bfloat16 [2, 32, 12, 256, 64], P(None, ('dp', 'ep'), 'tp')
All inputs are finite; a program needn't handle non-finite values.
Results may differ from the reference program's by a relative error of at most 0.0120267.
Values are sent between devices in bfloat16 or wider.
A program may use at most 1 GiB of HBM per device.

```python
import jax
import jax.numpy as jnp
from jax import lax

D_MODEL = 768
NUM_HEADS = 12
HEAD_DIM = 64
FF_DIM = 3072
NUM_EXPERTS = 64
EP_SIZE = 4
TP_SIZE = 2
BATCH = 32
SEQ_LEN = 256
NUM_BUCKETS = 32
EXACT_BUCKETS = 16

THRESHOLDS = (18, 20, 23, 26, 30, 34, 39, 45, 51, 58, 66, 76, 86, 98, 112)
EPSILON = 1e-6
INNER = NUM_HEADS * HEAD_DIM
LOCAL_BATCH = BATCH // EP_SIZE
LOCAL_SEQ = SEQ_LEN // TP_SIZE
LOCAL_TOKENS = LOCAL_BATCH * LOCAL_SEQ
NUM_GROUPS = EP_SIZE * TP_SIZE
CAPACITY = 4 * LOCAL_TOKENS // NUM_EXPERTS


def draw_ids(id_key):
    coin_key, hot_key, start_key, uniform_key, second_key = jax.random.split(id_key, 5)
    id_shape = (BATCH, SEQ_LEN)
    hot_width = max(NUM_EXPERTS // 8, 1)
    hot_start = jax.random.randint(start_key, (), 0, NUM_EXPERTS)
    hot_pick = (hot_start + jax.random.randint(hot_key, id_shape, 0, hot_width)) % NUM_EXPERTS
    uniform_pick = jax.random.randint(uniform_key, id_shape, 0, NUM_EXPERTS)
    coin_flip = jax.random.randint(coin_key, id_shape, 0, 4)
    first_pick = jnp.where(coin_flip == 0, hot_pick, uniform_pick)
    flat_pos = jnp.arange(BATCH * SEQ_LEN).reshape(id_shape)
    first_pick = jnp.where(flat_pos < NUM_EXPERTS, flat_pos, first_pick)
    second_pick = (first_pick + 1 + jax.random.randint(second_key, id_shape, 0, NUM_EXPERTS - 1)) % NUM_EXPERTS
    return jnp.stack([first_pick, second_pick], axis=-1).astype(jnp.int32)


def setup_inputs(seed: int = 0, part: int = 0) -> dict:
    keys_all = jax.random.split(jax.random.key(seed), 16)
    part_key = jax.random.fold_in(keys_all[0], part)
    act_key, id_key = jax.random.split(part_key)

    def normal(sub_key, dim_tuple, scale_by):
        return jax.random.normal(sub_key, dim_tuple, jnp.float32) * scale_by

    return {
        'hidden_in': normal(act_key, (BATCH, SEQ_LEN, D_MODEL), 1.0).astype(jnp.bfloat16),
        'ln_attn': jax.random.uniform(keys_all[1], (2, D_MODEL), jnp.float32, 0.5, 1.5),
        'ln_ffn': jax.random.uniform(keys_all[2], (2, D_MODEL), jnp.float32, 0.5, 1.5),
        'w_query': normal(keys_all[3], (2, D_MODEL, INNER), D_MODEL ** -0.5).astype(jnp.bfloat16),
        'w_key': normal(keys_all[4], (2, D_MODEL, INNER), D_MODEL ** -0.5).astype(jnp.bfloat16),
        'w_value': normal(keys_all[5], (2, D_MODEL, INNER), D_MODEL ** -0.5).astype(jnp.bfloat16),
        'w_out': normal(keys_all[6], (2, INNER, D_MODEL), INNER ** -0.5).astype(jnp.bfloat16),
        'bias_table': normal(keys_all[7], (2, NUM_HEADS, NUM_BUCKETS), 1.5),
        'w_gate': normal(keys_all[8], (D_MODEL, FF_DIM), D_MODEL ** -0.5).astype(jnp.bfloat16),
        'w_up': normal(keys_all[9], (D_MODEL, FF_DIM), D_MODEL ** -0.5).astype(jnp.bfloat16),
        'w_down': normal(keys_all[10], (FF_DIM, D_MODEL), FF_DIM ** -0.5).astype(jnp.bfloat16),
        'w_router': normal(keys_all[11], (D_MODEL, NUM_EXPERTS), D_MODEL ** -0.5),
        'expert_in': normal(keys_all[12], (NUM_EXPERTS, D_MODEL, FF_DIM), D_MODEL ** -0.5).astype(jnp.bfloat16),
        'expert_out': normal(keys_all[13], (NUM_EXPERTS, FF_DIM, D_MODEL), FF_DIM ** -0.5).astype(jnp.bfloat16),
        'expert_ids': draw_ids(id_key),
    }


def bucket_of(rel_pos):
    bucket_idx = jnp.minimum(rel_pos, EXACT_BUCKETS)
    for threshold in THRESHOLDS:
        bucket_idx = bucket_idx + (rel_pos >= threshold).astype(jnp.int32)
    return bucket_idx


def rms_norm(rows_in, ln_scale):
    wide_rows = rows_in.astype(jnp.float32)
    inv_rms = lax.rsqrt(jnp.mean(wide_rows * wide_rows, axis=-1, keepdims=True) + EPSILON)
    return (wide_rows * inv_rms * ln_scale).astype(jnp.bfloat16)


def causal_bias(bias_rows):
    positions = jnp.arange(SEQ_LEN)
    rel_pos = positions[:, None] - positions[None, :]
    bias_full = jnp.take(bias_rows, bucket_of(jnp.maximum(rel_pos, 0)), axis=1)
    return jnp.where(rel_pos[None] >= 0, bias_full, -jnp.inf)


def attention(hidden, ln_scale, w_query, w_key, w_value, w_out, bias_rows):
    normed = rms_norm(hidden, ln_scale).reshape(BATCH * SEQ_LEN, D_MODEL)

    def project(weight):
        projected = jnp.dot(normed, weight, preferred_element_type=jnp.float32)
        return projected.astype(jnp.bfloat16).reshape(BATCH, SEQ_LEN, NUM_HEADS, HEAD_DIM)

    queries = project(w_query)
    keys_full = project(w_key)
    values_full = project(w_value)
    bias_full = causal_bias(bias_rows)

    def one_sequence(operands):
        query_seq, key_seq, value_seq = operands
        scores = jnp.einsum('qhd,khd->hqk', query_seq.astype(jnp.float32), key_seq.astype(jnp.float32))
        scores = scores * (HEAD_DIM ** -0.5) + bias_full
        attn_probs = jax.nn.softmax(scores, axis=-1).astype(jnp.bfloat16)
        context = jnp.einsum('hqk,khd->qhd', attn_probs.astype(jnp.float32), value_seq.astype(jnp.float32))
        return context.astype(jnp.bfloat16)

    context = lax.map(one_sequence, (queries, keys_full, values_full)).reshape(BATCH * SEQ_LEN, INNER)
    attn_out = jnp.dot(context, w_out, preferred_element_type=jnp.float32).reshape(BATCH, SEQ_LEN, D_MODEL)
    new_hidden = (hidden.astype(jnp.float32) + attn_out).astype(jnp.bfloat16)
    return new_hidden, jnp.swapaxes(keys_full, 1, 2), jnp.swapaxes(values_full, 1, 2)


def dense_ffn(hidden, ln_scale, w_gate, w_up, w_down):
    normed = rms_norm(hidden, ln_scale).reshape(BATCH * SEQ_LEN, D_MODEL)
    gate_pre = jnp.dot(normed, w_gate, preferred_element_type=jnp.float32)
    up_pre = jnp.dot(normed, w_up, preferred_element_type=jnp.float32)
    ffn_hidden = (jax.nn.gelu(gate_pre) * up_pre).astype(jnp.bfloat16)
    ffn_out = jnp.dot(ffn_hidden, w_down, preferred_element_type=jnp.float32).reshape(BATCH, SEQ_LEN, D_MODEL)
    return (hidden.astype(jnp.float32) + ffn_out).astype(jnp.bfloat16)


def to_groups(array_in):
    tail_dims = array_in.shape[2:]
    split_view = array_in.reshape((EP_SIZE, LOCAL_BATCH, TP_SIZE, LOCAL_SEQ) + tail_dims)
    return jnp.swapaxes(split_view, 1, 2).reshape((NUM_GROUPS, LOCAL_TOKENS) + tail_dims)


def from_groups(array_in):
    tail_dims = array_in.shape[2:]
    split_view = array_in.reshape((EP_SIZE, TP_SIZE, LOCAL_BATCH, LOCAL_SEQ) + tail_dims)
    return jnp.swapaxes(split_view, 1, 2).reshape((BATCH, SEQ_LEN) + tail_dims)


def slot_table(choices):
    experts = jnp.arange(NUM_EXPERTS, dtype=jnp.int32)
    first_hot = (choices[..., 0:1] == experts).astype(jnp.int32)
    second_hot = (choices[..., 1:2] == experts).astype(jnp.int32)
    first_pos = jnp.sum((jnp.cumsum(first_hot, axis=-2) - 1) * first_hot, axis=-1)
    second_base = jnp.cumsum(second_hot, axis=-2) - 1 + jnp.sum(first_hot, axis=-2, keepdims=True)
    second_pos = jnp.sum(second_base * second_hot, axis=-1)
    position = jnp.stack([first_pos, second_pos], axis=-1)
    return jnp.where(position < CAPACITY, choices * CAPACITY + position, NUM_EXPERTS * CAPACITY)


def dispatch(group_rows, slot_ids):
    buffer_rows = jnp.zeros((NUM_EXPERTS * CAPACITY + 1, D_MODEL), jnp.bfloat16)
    buffer_rows = buffer_rows.at[slot_ids[:, 0]].set(group_rows).at[slot_ids[:, 1]].set(group_rows)
    return buffer_rows[:-1]


def run_expert(operands):
    rows_in, weight_in, weight_out = operands
    expert_hidden = jax.nn.gelu(jnp.dot(rows_in, weight_in, preferred_element_type=jnp.float32)).astype(jnp.bfloat16)
    return jnp.dot(expert_hidden, weight_out, preferred_element_type=jnp.float32).astype(jnp.bfloat16)


def gather_rows(table_rows, slot_ids):
    return jnp.take(table_rows, slot_ids, axis=0)


def moe_layer(hidden, ln_scale, w_router, expert_in, expert_out, expert_ids):
    tok_rows = to_groups(rms_norm(hidden, ln_scale))
    choices = to_groups(expert_ids)
    logits = jnp.einsum('gnd,de->gne', tok_rows.astype(jnp.float32), w_router)
    router_probs = jax.nn.softmax(logits, axis=-1)
    picked = jnp.take_along_axis(router_probs, choices, axis=-1)
    gate_weights = picked / jnp.sum(picked, axis=-1, keepdims=True)
    slot_ids = slot_table(choices)
    buffers = jax.vmap(dispatch)(tok_rows, slot_ids)
    per_expert = jnp.swapaxes(buffers.reshape(NUM_GROUPS, NUM_EXPERTS, CAPACITY, D_MODEL), 0, 1)
    per_expert = per_expert.reshape(NUM_EXPERTS, NUM_GROUPS * CAPACITY, D_MODEL)
    expert_result = lax.map(run_expert, (per_expert, expert_in, expert_out))
    returned = jnp.swapaxes(expert_result.reshape(NUM_EXPERTS, NUM_GROUPS, CAPACITY, D_MODEL), 0, 1)
    returned = returned.reshape(NUM_GROUPS, NUM_EXPERTS * CAPACITY, D_MODEL)
    padded = jnp.concatenate([returned, jnp.zeros((NUM_GROUPS, 1, D_MODEL), jnp.bfloat16)], axis=1)
    gathered_out = jax.vmap(gather_rows)(padded, slot_ids)
    moe_sum = jnp.sum(gate_weights[..., None] * gathered_out.astype(jnp.float32), axis=2)
    return (hidden.astype(jnp.float32) + from_groups(moe_sum)).astype(jnp.bfloat16)


def reference(hidden_in, ln_attn, ln_ffn, w_query, w_key, w_value, w_out, bias_table, w_gate, w_up, w_down, w_router, expert_in, expert_out, expert_ids):
    hidden, keys_zero, values_zero = attention(hidden_in, ln_attn[0], w_query[0], w_key[0], w_value[0], w_out[0], bias_table[0])
    hidden = dense_ffn(hidden, ln_ffn[0], w_gate, w_up, w_down)
    hidden, keys_one, values_one = attention(hidden, ln_attn[1], w_query[1], w_key[1], w_value[1], w_out[1], bias_table[1])
    hidden = moe_layer(hidden, ln_ffn[1], w_router, expert_in, expert_out, expert_ids)
    return hidden, jnp.stack([keys_zero, keys_one]), jnp.stack([values_zero, values_one])
```

```python
import functools

import jax
import jax.numpy as jnp
import numpy as np
from jax import lax
from jax.experimental import pallas as pl
from jax.experimental.pallas import tpu as pltpu
from jax.sharding import PartitionSpec as P

EXACT_BUCKETS = 16
THRESHOLDS = (18, 20, 23, 26, 30, 34, 39, 45, 51, 58, 66, 76, 86, 98, 112)
EPSILON = 1e-6
BF16 = jnp.bfloat16
F32 = jnp.float32

TP_SWAP = [(0, 1), (1, 0)]
CORE_SWAP = [(0, 1), (1, 0), (2, 3), (3, 2)]
X_SWAP = [(0, 2), (2, 0), (1, 3), (3, 1)]


def rms_norm(rows_in, ln_scale):
    wide_rows = rows_in.astype(F32)
    inv_rms = lax.rsqrt(jnp.mean(wide_rows * wide_rows, axis=-1, keepdims=True) + EPSILON)
    return (wide_rows * inv_rms * ln_scale).astype(BF16)


def swap(array_in, axis_name, pairs):
    return lax.ppermute(array_in, axis_name, pairs)


def gather_quarters(mine):
    q0 = swap(mine, 'tp', TP_SWAP)
    q1 = swap(q0, 'ep', CORE_SWAP)
    q2 = swap(q0, 'ep', X_SWAP)
    q3 = swap(q2, 'ep', CORE_SWAP)
    return q0, q1, q2, q3


def assemble(quarters, ep):
    rows = quarters[0].shape[0]
    full = jnp.zeros((4 * rows,) + quarters[0].shape[1:], quarters[0].dtype)
    for j, quarter in enumerate(quarters):
        full = lax.dynamic_update_slice(full, quarter, ((ep ^ j) * rows, 0))
    return full


def bias_vectors(bias_rows, seq_len):
    rel = (-np.arange(seq_len)) % seq_len
    bucket = np.minimum(rel, EXACT_BUCKETS)
    for threshold in THRESHOLDS:
        bucket = bucket + (rel >= threshold)
    hot = jnp.asarray(bucket, jnp.int32)[None, None, :] == jnp.arange(bias_rows.shape[1])[None, :, None]
    return jnp.sum(jnp.where(hot, bias_rows[:, :, None], 0.0), axis=1)


def attn_kernel(qkv_ref, u_ref, o_ref, bias_ref):
    heads = u_ref.shape[0]
    seq = qkv_ref.shape[1]
    width = heads * 64
    half = seq // 2

    @pl.when(pl.program_id(0) == 0)
    def _():
        row = lax.broadcasted_iota(jnp.int32, (seq, seq), 0)
        col = lax.broadcasted_iota(jnp.int32, (seq, seq), 1)
        for h in range(heads):
            line = jnp.broadcast_to(u_ref[h:h + 1, :], (seq, seq))
            toeplitz = pltpu.roll(line, 0, 1, stride=1, stride_axis=0)
            bias_ref[h] = jnp.where(col <= row, toeplitz, -jnp.inf)

    lane = lax.broadcasted_iota(jnp.int32, (half, 128), 1)
    for pair in range(heads // 2):
        lo = pair * 128
        for blk in range(2):
            keys = half * (blk + 1)
            q = qkv_ref[0, blk * half:(blk + 1) * half, lo:lo + 128]
            k = qkv_ref[0, 0:keys, width + lo:width + lo + 128]
            v = qkv_ref[0, 0:keys, 2 * width + lo:2 * width + lo + 128]
            outs = []
            for side in range(2):
                mine = (lane < 64) if side == 0 else (lane >= 64)
                qh = jnp.where(mine, q, jnp.zeros_like(q))
                s = lax.dot_general(qh, k, (((1,), (1,)), ((), ())), preferred_element_type=F32)
                s = s * 0.125 + bias_ref[2 * pair + side, blk * half:(blk + 1) * half, 0:keys]
                p = jnp.exp(s - jnp.max(s, axis=1, keepdims=True))
                p = (p * (1.0 / jnp.sum(p, axis=1, keepdims=True))).astype(BF16)
                outs.append(jnp.dot(p, v, preferred_element_type=F32))
            o_ref[0, blk * half:(blk + 1) * half, lo:lo + 128] = jnp.where(lane < 64, outs[0], outs[1]).astype(BF16)


def attend(qkv, u):
    batch, seq, width3 = qkv.shape
    heads = u.shape[0]
    width = width3 // 3
    return pl.pallas_call(
        attn_kernel,
        grid=(batch,),
        in_specs=[pl.BlockSpec((1, seq, width3), lambda b: (b, 0, 0)),
                  pl.BlockSpec((heads, seq), lambda b: (0, 0))],
        out_specs=pl.BlockSpec((1, seq, width), lambda b: (b, 0, 0)),
        out_shape=jax.ShapeDtypeStruct((batch, seq, width), BF16),
        scratch_shapes=[pltpu.VMEM((heads, seq, seq), F32)],
        compiler_params=pltpu.CompilerParams(dimension_semantics=("arbitrary",)),
        cost_estimate=pl.CostEstimate(flops=batch * heads * seq * seq * 64 * 16, bytes_accessed=batch * seq * width * 8,
                                      transcendentals=batch * heads * seq * seq),
    )(qkv, u)


def mm(a, b):
    return jnp.dot(a, b, preferred_element_type=F32)


def attention_block(x, ln_scale, wqkv_own, wqkv_peer, wout_own, wout_peer, u_own, u_peer):
    batch, seq, d_model = x.shape
    a = rms_norm(x, ln_scale).reshape(batch * seq, d_model)
    qkv_own = mm(a, wqkv_own).astype(BF16).reshape(batch, seq, -1)
    o_own = attend(qkv_own, u_own)
    qkv_peer = mm(a, wqkv_peer).astype(BF16).reshape(batch, seq, -1)
    o_peer = attend(qkv_peer, u_peer)
    width = o_own.shape[-1]
    out = mm(o_own.reshape(-1, width), wout_own) + mm(o_peer.reshape(-1, width), wout_peer)
    new_x = (x.astype(F32) + out.reshape(x.shape)).astype(BF16)
    kv_own = qkv_own[:, :, width:]
    kv_sent = swap(qkv_peer[:, :, width:], 'tp', TP_SWAP)
    return new_x, kv_own, kv_sent


def by_tp(tp, first, second, axis):
    return jnp.where(tp == 0, jnp.concatenate([first, second], axis), jnp.concatenate([second, first], axis))


def cache_of(tp, kv_own, kv_got, which):
    batch, seq, width2 = kv_own.shape
    width = width2 // 2
    both = by_tp(tp, kv_own[:, :, which * width:(which + 1) * width], kv_got[:, :, which * width:(which + 1) * width], 0)
    return jnp.swapaxes(both.reshape(2 * batch, seq, width // 64, 64), 1, 2)


def ffn_part(b, w_gate, w_up, w_down):
    hid = (jax.nn.gelu(mm(b, w_gate)) * mm(b, w_up)).astype(BF16)
    return mm(hid, w_down)


def slot_ids_of(choices, num_experts, capacity):
    tokens = choices.shape[0]
    experts = jnp.arange(num_experts, dtype=jnp.int32)
    first_hot = choices[:, 0:1] == experts
    second_hot = choices[:, 1:2] == experts
    tri = (jnp.arange(tokens)[:, None] > jnp.arange(tokens)[None, :]).astype(BF16)
    before = mm(tri, jnp.concatenate([first_hot, second_hot], 1).astype(BF16))
    first_pos = jnp.sum(jnp.where(first_hot, before[:, :num_experts], 0.0), axis=1)
    totals = jnp.sum(first_hot.astype(F32), axis=0, keepdims=True)
    second_pos = jnp.sum(jnp.where(second_hot, before[:, num_experts:] + totals, 0.0), axis=1)
    position = jnp.stack([first_pos, second_pos], axis=1).astype(jnp.int32)
    return jnp.where(position < capacity, choices * capacity + position, -1)


def solution(mesh):
    act_spec = P(('dp', 'ep'), 'tp', None)
    col_spec = P(None, None, 'tp')
    row_spec = P(None, 'tp', None)
    expert_spec = P(('tp', 'ep'), None, None)
    cache_spec = P(None, ('dp', 'ep'), 'tp', None, None)
    in_specs = (act_spec, P(), P(), col_spec, col_spec, col_spec, row_spec, row_spec,
                P(None, 'tp'), P(None, 'tp'), P('tp', None), P(), expert_spec, expert_spec, act_spec)

    def device_fn(hidden_in, ln_attn, ln_ffn, w_query, w_key, w_value, w_out, bias_table, w_gate, w_up, w_down, w_router, expert_in, expert_out, expert_ids):
        tp = lax.axis_index('tp')
        ep = lax.axis_index('ep')
        nb, npos, d_model = hidden_in.shape
        hb = nb // 2
        seq = 2 * npos
        tokens = nb * npos
        num_experts = w_router.shape[1]
        local_experts = expert_in.shape[0]
        groups = num_experts // local_experts
        capacity = 4 * tokens // num_experts

        mine = lax.dynamic_slice_in_dim(hidden_in, tp * hb, hb, 0)
        got = swap(lax.dynamic_slice_in_dim(hidden_in, (1 - tp) * hb, hb, 0), 'tp', TP_SWAP)
        x = by_tp(tp, mine, got, 1)

        bias_peer = swap(bias_table, 'tp', TP_SWAP)
        wqkv = [jnp.concatenate([w_query[l], w_key[l], w_value[l]], 1) for l in range(2)]
        qr = d_model // 4
        orow = w_out.shape[1] // 4
        fq = w_gate.shape[1] // 4
        wqkv_peer = [assemble(gather_quarters(lax.dynamic_slice_in_dim(w, ep * qr, qr, 0)), ep) for w in wqkv]
        wout_q = gather_quarters(lax.dynamic_slice_in_dim(w_out, ep * orow, orow, 1))
        wout_peer = [assemble([q[l] for q in wout_q], ep) for l in range(2)]
        ffn_q = jnp.concatenate([
            jnp.concatenate([lax.dynamic_slice_in_dim(w_gate, ep * fq, fq, 1), lax.dynamic_slice_in_dim(w_up, ep * fq, fq, 1)], 1),
            lax.dynamic_slice_in_dim(w_down, ep * fq, fq, 0)], 0)
        ffn_quarters = gather_quarters(ffn_q)

        slots = slot_ids_of(expert_ids.reshape(tokens, 2), num_experts, capacity)
        slots_all = lax.all_gather(slots, ('tp', 'ep'))

        u_own = [bias_vectors(bias_table[l], seq) for l in range(2)]
        u_peer = [bias_vectors(bias_peer[l], seq) for l in range(2)]
        x, kv0, kv0_got = attention_block(x, ln_attn[0], wqkv[0], wqkv_peer[0], w_out[0], wout_peer[0], u_own[0], u_peer[0])
        b = rms_norm(x, ln_ffn[0]).reshape(hb * seq, d_model)
        ffn = ffn_part(b, w_gate, w_up, w_down)
        for q in ffn_quarters:
            ffn = ffn + ffn_part(b, q[:d_model, :fq], q[:d_model, fq:], q[d_model:])
        x = (x.astype(F32) + ffn.reshape(x.shape)).astype(BF16)

        x, kv1, kv1_got = attention_block(x, ln_attn[1], wqkv[1], wqkv_peer[1], w_out[1], wout_peer[1], u_own[1], u_peer[1])
        k_cache = jnp.stack([cache_of(tp, kv0, kv0_got, 0), cache_of(tp, kv1, kv1_got, 0)])
        v_cache = jnp.stack([cache_of(tp, kv0, kv0_got, 1), cache_of(tp, kv1, kv1_got, 1)])

        half = hb // 2
        h_y = swap(x, 'tp', TP_SWAP)
        h_x = swap(x, 'ep', X_SWAP)
        d_lo = swap(h_y[:half], 'ep', X_SWAP)
        d_hi = swap(h_x[half:], 'tp', TP_SWAP)
        parts = [(0, 0, 0, x), (1, 0, 0, h_y), (0, 2, 0, h_x), (1, 2, 0, d_lo), (1, 2, half, d_hi)]
        parts += [(i, j ^ 1, o, swap(h, 'ep', CORE_SWAP)) for i, j, o, h in parts]
        b_groups = jnp.zeros((2, 4, nb, npos, d_model), BF16)
        for i, j, o, h in parts:
            rows = rms_norm(h, ln_ffn[1]).reshape(h.shape[0], 2, npos, d_model)
            rows = jnp.swapaxes(rows, 0, 1)[:, None]
            b_groups = lax.dynamic_update_slice(b_groups, rows, (0, ep ^ j, (tp ^ i) * hb + o, 0, 0))
        b_groups = b_groups.reshape(groups, tokens, d_model)

        own = lax.dynamic_slice_in_dim(x, tp * npos, npos, 1)
        peer = lax.dynamic_slice_in_dim(h_y, tp * npos, npos, 1)
        hidden = by_tp(tp, own, peer, 0)

        me = tp * 4 + ep
        local_slots = local_experts * capacity
        loc = slots_all - me * local_slots
        columns = jnp.arange(local_slots, dtype=jnp.int32)[None, :, None]
        select = ((loc[:, None, :, 0] == columns) | (loc[:, None, :, 1] == columns)).astype(BF16)
        rows = jnp.einsum('gsn,gnd->gsd', select, b_groups, preferred_element_type=F32).astype(BF16)
        rows = rows.reshape(groups, local_experts, capacity, d_model)
        rows = jnp.swapaxes(rows, 0, 1).reshape(local_experts, groups * capacity, d_model)
        expert_hidden = jnp.einsum('erd,edf->erf', rows, expert_in, preferred_element_type=F32)
        expert_hidden = jax.nn.gelu(expert_hidden).astype(BF16)
        result = jnp.einsum('erf,efd->erd', expert_hidden, expert_out, preferred_element_type=F32).astype(BF16)
        result = result.reshape(1, local_experts, groups * capacity, d_model)
        returned = lax.all_to_all(result, ('tp', 'ep'), 2, 0, tiled=True)
        returned = returned.reshape(num_experts * capacity, d_model)

        normed = rms_norm(hidden, ln_ffn[1]).reshape(tokens, d_model)
        logits = jnp.dot(normed.astype(F32), w_router, precision=lax.Precision.HIGHEST)
        probs = jax.nn.softmax(logits, axis=-1)
        ids = expert_ids.reshape(tokens, 2)
        experts = jnp.arange(num_experts, dtype=jnp.int32)
        picked = [jnp.sum(jnp.where(ids[:, c:c + 1] == experts, probs, 0.0), axis=1, keepdims=True) for c in range(2)]
        denom = picked[0] + picked[1]
        slot_columns = jnp.arange(num_experts * capacity, dtype=jnp.int32)
        moe_sum = sum((picked[c] / denom) * mm((slots[:, c:c + 1] == slot_columns).astype(BF16), returned) for c in range(2))
        hidden = (hidden.astype(F32) + moe_sum.reshape(hidden.shape)).astype(BF16)
        return hidden, k_cache, v_cache

    return jax.shard_map(device_fn, mesh=mesh, in_specs=in_specs, out_specs=(act_spec, cache_spec, cache_spec), check_vma=False)
```

```python
import functools

import jax
import jax.numpy as jnp
import numpy as np
from jax import lax
from jax.experimental import pallas as pl
from jax.experimental.pallas import tpu as pltpu
from jax.sharding import PartitionSpec as P

EXACT_BUCKETS = 16
THRESHOLDS = (18, 20, 23, 26, 30, 34, 39, 45, 51, 58, 66, 76, 86, 98, 112)
EPSILON = 1e-6
BF16 = jnp.bfloat16
F32 = jnp.float32

TP_SWAP = [(0, 1), (1, 0)]
CORE_SWAP = [(0, 1), (1, 0), (2, 3), (3, 2)]
X_SWAP = [(0, 2), (2, 0), (1, 3), (3, 1)]


def rms_norm(rows_in, ln_scale):
    wide_rows = rows_in.astype(F32)
    inv_rms = lax.rsqrt(jnp.mean(wide_rows * wide_rows, axis=-1, keepdims=True) + EPSILON)
    return (wide_rows * inv_rms * ln_scale).astype(BF16)


def swap(array_in, axis_name, pairs):
    return lax.ppermute(array_in, axis_name, pairs)


def bias_vectors(bias_rows, seq_len):
    rel = (-np.arange(seq_len)) % seq_len
    bucket = np.minimum(rel, EXACT_BUCKETS)
    for threshold in THRESHOLDS:
        bucket = bucket + (rel >= threshold)
    hot = jnp.asarray(bucket, jnp.int32)[None, None, :] == jnp.arange(bias_rows.shape[1])[None, :, None]
    return jnp.sum(jnp.where(hot, bias_rows[:, :, None], 0.0), axis=1)


MESH = pl.DeviceIdType.MESH
HEADS = 6
NQ = 192
NO = 96
NF = 128
FC = 512


def swap_targets():
    tp = lax.axis_index('tp')
    ep = lax.axis_index('ep')
    core = ep + 1 - 2 * lax.rem(ep, 2)
    across = lax.rem(ep + 2, 4)
    return tp, ep, {'tp': 1 - tp}, {'ep': across}, {'ep': core}


def greet(targets):
    barrier = pltpu.get_barrier_semaphore()
    for target in targets:
        pl.semaphore_signal(barrier, inc=1, device_id=target, device_id_type=MESH)
    pl.semaphore_wait(barrier, len(targets))


def attend_rows(qkv_ref, bias_ref, base, o_ref, side, s):
    width = HEADS * 64
    rows = 128
    lane = lax.broadcasted_iota(jnp.int32, (rows, 128), 1)
    units = [(pair, blk, sd) for pair in range(HEADS // 2) for blk in range(2) for sd in range(2)]
    scores = []
    for pair, blk, sd in units:
        lo = pair * 128
        keys = rows * (blk + 1)
        q = qkv_ref[blk * rows:(blk + 1) * rows, lo:lo + 128]
        k = qkv_ref[0:keys, width + lo:width + lo + 128]
        mine = (lane < 64) if sd == 0 else (lane >= 64)
        qh = jnp.where(mine, q, jnp.zeros_like(q))
        sc = lax.dot_general(qh, k, (((1,), (1,)), ((), ())), preferred_element_type=F32)
        scores.append(sc * 0.125 + bias_ref[base + 2 * pair + sd, blk * rows:(blk + 1) * rows, 0:keys])
    tops = [jnp.max(sc, axis=1, keepdims=True) for sc in scores]
    exps = [jnp.exp(sc - m) for sc, m in zip(scores, tops)]
    sums = [jnp.sum(p, axis=1, keepdims=True) for p in exps]
    probs = [(p * (1.0 / l)).astype(BF16) for p, l in zip(exps, sums)]
    outs = []
    for (pair, blk, sd), p in zip(units, probs):
        lo = pair * 128
        v = qkv_ref[0:rows * (blk + 1), 2 * width + lo:2 * width + lo + 128]
        outs.append(jnp.dot(p, v, preferred_element_type=F32))
    for i in range(0, len(units), 2):
        pair, blk, _ = units[i]
        o_ref[side, s, blk * rows:(blk + 1) * rows, pair * 128:pair * 128 + 128] = jnp.where(
            lane < 64, outs[i], outs[i + 1]).astype(BF16)


def dense_kernel(hid, lna, lnf, wq, wk, wv, wo, wg, wu, wd, u_own,
                 x_ref, kvp_ref, kc, vc,
                 own_qkv, own_o, own_g, own_u, own_d, peer_qkv, peer_o, peer_g, peer_u, peer_d,
                 u_peer, bias, qkv, o_all, b_all, acc, kvt, kvo, other,
                 ysend, yrecv, xsend, xrecv, csend, crecv, dsend, drecv, hsend, hrecv, lsem, osem):
    tp, ep, to_y, to_x, to_c = swap_targets()
    across = lax.rem(ep + 2, 4)
    hb, seq, d_model = x_ref.shape
    half = seq // 2
    width = HEADS * 64

    items = []
    for l in range(2):
        layer = [('w', l, m) for m in range(3)] + [('o', l, 0)]
        items += layer
        if l == 0:
            items += [(kind, c, 0) for c in range(3) for kind in ('g', 'u', 'd')]
    index = {item: i for i, item in enumerate(items)}

    def source(item):
        kind, l, m = item
        if kind == 'w':
            return (wq, wk, wv)[m].at[l, pl.ds(pl.multiple_of(ep * NQ, NQ), NQ), :]
        if kind == 'o':
            return wo.at[l, pl.ds(pl.multiple_of(ep * NO, NO), NO), :]
        at = pl.multiple_of(ep * (3 * NF) + l * NF, NF)
        if kind == 'd':
            return wd.at[pl.ds(at, NF), :]
        return (wg if kind == 'g' else wu).at[:, pl.ds(at, NF)]

    def place(item, r):
        kind, l, m = item
        if kind == 'w':
            return peer_qkv.at[l, m, pl.ds(pl.multiple_of(r * NQ, NQ), NQ), :]
        if kind == 'o':
            return peer_o.at[l, pl.ds(pl.multiple_of(r * NO, NO), NO), :]
        at = pl.multiple_of(r * NF, NF)
        if kind == 'd':
            return peer_d.at[l, pl.ds(at, NF), :]
        return (peer_g if kind == 'g' else peer_u).at[l, :, pl.ds(at, NF)]

    def remote(src, dst, send, recv, target):
        return pltpu.make_async_remote_copy(src_ref=src, dst_ref=dst, send_sem=send, recv_sem=recv,
                                            device_id=target, device_id_type=MESH)

    def y_copy(item):
        i = index[item]
        return remote(source(item), place(item, ep), ysend.at[i], yrecv.at[i], to_y)

    def x_copy(item):
        i = index[item]
        return remote(place(item, ep), place(item, ep), xsend.at[i], xrecv.at[i], to_x)

    def c_copy(item):
        i = index[item]
        return remote(place(item, ep), place(item, ep), csend.at[i], crecv.at[i], to_c)

    def d_copy(item):
        i = index[item]
        return remote(place(item, across), place(item, across), dsend.at[i], drecv.at[i], to_c)

    def pass_on(*names):
        for item in names:
            y_copy(item).wait_recv()
            x_copy(item).start()
            c_copy(item).start()

    def pass_core(*names):
        for item in names:
            x_copy(item).wait_recv()
            d_copy(item).start()

    def complete(*names):
        for item in names:
            c_copy(item).wait_recv()
            d_copy(item).wait_recv()

    mine_at = pl.ds(tp * hb, hb)
    peer_at = pl.ds((1 - tp) * hb, hb)
    rows_at = pl.ds(pl.multiple_of(tp * half, half), half)
    hid_a = remote(hid.at[peer_at], x_ref.at[:, rows_at, :], hsend.at[0], hrecv.at[0], to_y)
    hid_b = remote(hid.at[mine_at], other.at[:, rows_at, :], hsend.at[1], hrecv.at[1], to_y)
    u_copy = remote(u_own, u_peer, hsend.at[2], hrecv.at[2], to_y)
    loads = [pltpu.make_async_copy(s, d, lsem.at[i]) for i, (s, d) in enumerate([
        (hid.at[mine_at], x_ref.at[:, rows_at, :]),
        (wq, own_qkv.at[0]), (wk, own_qkv.at[1]), (wv, own_qkv.at[2]), (wo, own_o),
        (wg, own_g), (wu, own_u), (wd, own_d),
        (hid.at[peer_at], other.at[:, rows_at, :])])]

    greet([to_y, to_x, to_c])
    hid_a.start()
    u_copy.start()
    for item in items:
        y_copy(item).start()
    hid_b.start()
    for load in loads:
        load.start()

    def fill_bias(src, l, base):
        row = lax.broadcasted_iota(jnp.int32, (seq, seq), 0)
        col = lax.broadcasted_iota(jnp.int32, (seq, seq), 1)
        for h in range(HEADS):
            line = jnp.broadcast_to(src[l, h:h + 1, :], (seq, seq))
            toeplitz = pltpu.roll(line, 0, 1, stride=1, stride_axis=0)
            bias[base + h] = jnp.where(col <= row, toeplitz, -jnp.inf)

    def normed(rows, scale):
        wide = rows.astype(F32)
        inv = lax.rsqrt(jnp.mean(wide * wide, axis=-1, keepdims=True) + EPSILON)
        return (wide * inv * scale).astype(BF16)

    def heads_pass(l, side, lo, hi):
        def body(s, carry):
            a = normed(x_ref[s], lna[l:l + 1, :])
            for m in range(3):
                w = own_qkv[m, l] if side == 0 else peer_qkv[l, m]
                part = jnp.dot(a, w, preferred_element_type=F32).astype(BF16)
                qkv[:, m * width:(m + 1) * width] = part
                if m > 0:
                    if side == 0:
                        kvt[l, m - 1, s] = part.T
                    elif l == 1:
                        kvp_ref[m - 1, s] = part.T
            attend_rows(qkv, bias, side * HEADS, o_all, side, s)
            return carry
        lax.fori_loop(lo, hi, body, 0)

    def project_out(l):
        def body(s, carry):
            out = jnp.dot(o_all[0, s], own_o[l], preferred_element_type=F32)
            out = out + jnp.dot(o_all[1, s], peer_o[l], preferred_element_type=F32)
            x_ref[s] = (x_ref[s].astype(F32) + out).astype(BF16)
            return carry
        lax.fori_loop(0, hb, body, 0)

    def ffn_chunk(gate, up, down, first):
        def body(r, carry):
            at = pl.ds(pl.multiple_of(r * FC, FC), FC)
            b = b_all[at, :]
            g = jnp.dot(b, gate, preferred_element_type=F32)
            u = jnp.dot(b, up, preferred_element_type=F32)
            hidden = (jax.nn.gelu(g) * u).astype(BF16)
            out = jnp.dot(hidden, down, preferred_element_type=F32)
            acc[at, :] = out if first else acc[at, :] + out
            return carry
        lax.fori_loop(0, 2, body, 0)

    def ffn_own(c):
        at = slice(c * FC, (c + 1) * FC)
        ffn_chunk(own_g[:, at], own_u[:, at], own_d[at, :], c == 0)

    def ffn_peer(c):
        ffn_chunk(peer_g[c], peer_u[c], peer_d[c], False)

    w0 = [('w', 0, m) for m in range(3)]
    w1 = [('w', 1, m) for m in range(3)]
    o0, o1 = ('o', 0, 0), ('o', 1, 0)
    g = [('g', c, 0) for c in range(3)]
    u = [('u', c, 0) for c in range(3)]
    d = [('d', c, 0) for c in range(3)]

    fill_bias(u_own, 0, 0)
    u_copy.wait_recv()
    fill_bias(u_peer, 0, HEADS)
    loads[0].wait()
    hid_a.wait_recv()
    for load in loads[1:4]:
        load.wait()
    heads_pass(0, 0, 0, hb)
    pass_on(*w0, o0)
    pass_core(*w0)
    pass_on(g[0])
    pass_core(o0)
    complete(*w0, o0)
    pass_on(u[0])
    heads_pass(0, 1, 0, hb // 2)
    pass_on(d[0])
    pass_core(g[0])
    heads_pass(0, 1, hb // 2, hb)
    pass_core(u[0])
    pass_on(g[1])
    loads[4].wait()
    project_out(0)

    def norm_rows(s, carry):
        b_all[pl.ds(pl.multiple_of(s * seq, seq), seq), :] = normed(x_ref[s], lnf[0:1, :])
        return carry
    lax.fori_loop(0, hb, norm_rows, 0)
    for load in loads[5:8]:
        load.wait()
    ffn_own(0)
    pass_on(u[1])
    pass_core(d[0])
    ffn_own(1)
    pass_core(g[1])
    pass_on(d[1])
    pass_core(u[1])
    ffn_own(2)
    pass_on(g[2])
    complete(g[0], u[0], d[0])
    ffn_peer(0)
    pass_core(d[1], g[2])
    pass_on(u[2])
    complete(g[1], u[1], d[1])
    ffn_peer(1)
    fill_bias(u_own, 1, 0)
    pass_on(d[2])
    pass_core(u[2])
    fill_bias(u_peer, 1, HEADS)
    pass_on(w1[0])
    pass_core(d[2])
    complete(g[2], u[2], d[2])
    ffn_peer(2)

    def add_rows(s, carry):
        x_ref[s] = (x_ref[s].astype(F32) + acc[pl.ds(pl.multiple_of(s * seq, seq), seq), :]).astype(BF16)
        return carry
    lax.fori_loop(0, hb, add_rows, 0)

    pass_on(w1[1], w1[2])
    pass_core(w1[0])
    heads_pass(1, 0, 0, hb)
    pass_on(o1)
    pass_core(w1[1], w1[2], o1)
    complete(*w1, o1)
    stores = [pltpu.make_async_copy(kvt.at[l, m], (kc, vc)[m].at[l, mine_at], osem.at[2 * l + m])
              for l in range(2) for m in range(2)]
    for store in stores:
        store.start()
    heads_pass(1, 1, 0, hb)
    project_out(1)

    loads[8].wait()
    hid_b.wait_recv()

    def other_rows(s, carry):
        a = normed(other[s], lna[0:1, :])
        for m in range(2):
            kvo[m, s] = jnp.dot(a, own_qkv[m + 1, 0], preferred_element_type=F32).astype(BF16).T
        return carry
    lax.fori_loop(0, hb, other_rows, 0)
    stores += [pltpu.make_async_copy(kvo.at[m], (kc, vc)[m].at[0, peer_at], osem.at[4 + m]) for m in range(2)]
    for store in stores[4:]:
        store.start()
    for store in stores:
        store.wait()
    hid_a.wait_send()
    hid_b.wait_send()
    u_copy.wait_send()
    for item in items:
        y_copy(item).wait_send()
        x_copy(item).wait_send()
        c_copy(item).wait_send()
        d_copy(item).wait_send()


def dense_layers(hid, lna, lnf, wq, wk, wv, wo, wg, wu, wd, u_own):
    nb, npos, d_model = hid.shape
    hb, seq = nb // 2, 2 * npos
    width = HEADS * 64
    ff = wg.shape[1]
    any_spec = pl.BlockSpec(memory_space=pl.ANY)
    vmem = pl.BlockSpec(memory_space=pltpu.VMEM)
    n_items = 17
    dma = pltpu.SemaphoreType.DMA
    return pl.pallas_call(
        dense_kernel,
        in_specs=[any_spec, vmem, vmem] + [any_spec] * 7 + [vmem],
        out_specs=[vmem, vmem, any_spec, any_spec],
        out_shape=[jax.ShapeDtypeStruct((hb, seq, d_model), BF16),
                   jax.ShapeDtypeStruct((2, hb, width, seq), BF16),
                   jax.ShapeDtypeStruct((2, nb, width, seq), BF16),
                   jax.ShapeDtypeStruct((2, nb, width, seq), BF16)],
        scratch_shapes=[
            pltpu.VMEM((3, 2, d_model, width), BF16), pltpu.VMEM((2, width, d_model), BF16),
            pltpu.VMEM((d_model, ff), BF16), pltpu.VMEM((d_model, ff), BF16), pltpu.VMEM((ff, d_model), BF16),
            pltpu.VMEM((2, 3, d_model, width), BF16), pltpu.VMEM((2, width, d_model), BF16),
            pltpu.VMEM((3, d_model, FC), BF16), pltpu.VMEM((3, d_model, FC), BF16), pltpu.VMEM((3, FC, d_model), BF16),
            pltpu.VMEM((2, HEADS, seq), F32), pltpu.VMEM((2 * HEADS, seq, seq), F32),
            pltpu.VMEM((seq, 3 * width), BF16), pltpu.VMEM((2, hb, seq, width), BF16),
            pltpu.VMEM((hb * seq, d_model), BF16), pltpu.VMEM((hb * seq, d_model), F32),
            pltpu.VMEM((2, 2, hb, width, seq), BF16), pltpu.VMEM((2, hb, width, seq), BF16),
            pltpu.VMEM((hb, seq, d_model), BF16),
        ] + [dma((n_items,))] * 8 + [dma((3,)), dma((3,)), dma((9,)), dma((6,))],
        compiler_params=pltpu.CompilerParams(collective_id=0, has_side_effects=True, vmem_limit_bytes=62 * 1024 * 1024),
        name="dense_layers",
    )(hid, lna, lnf, wq, wk, wv, wo, wg, wu, wd, u_own)


def mm(a, b):
    return jnp.dot(a, b, preferred_element_type=F32)


def by_tp(tp, first, second, axis):
    return jnp.where(tp == 0, jnp.concatenate([first, second], axis), jnp.concatenate([second, first], axis))


def slot_ids_of(choices, num_experts, capacity):
    tokens = choices.shape[0]
    experts = jnp.arange(num_experts, dtype=jnp.int32)
    first_hot = choices[:, 0:1] == experts
    second_hot = choices[:, 1:2] == experts
    tri = (jnp.arange(tokens)[:, None] > jnp.arange(tokens)[None, :]).astype(BF16)
    before = mm(tri, jnp.concatenate([first_hot, second_hot], 1).astype(BF16))
    first_pos = jnp.sum(jnp.where(first_hot, before[:, :num_experts], 0.0), axis=1)
    totals = jnp.sum(first_hot.astype(F32), axis=0, keepdims=True)
    second_pos = jnp.sum(jnp.where(second_hot, before[:, num_experts:] + totals, 0.0), axis=1)
    position = jnp.stack([first_pos, second_pos], axis=1).astype(jnp.int32)
    return jnp.where(position < capacity, choices * capacity + position, -1)


def solution(mesh):
    act_spec = P(('dp', 'ep'), 'tp', None)
    col_spec = P(None, None, 'tp')
    row_spec = P(None, 'tp', None)
    expert_spec = P(('tp', 'ep'), None, None)
    cache_spec = P(None, ('dp', 'ep'), 'tp', None, None)
    in_specs = (act_spec, P(), P(), col_spec, col_spec, col_spec, row_spec, row_spec,
                P(None, 'tp'), P(None, 'tp'), P('tp', None), P(), expert_spec, expert_spec, act_spec)

    def device_fn(hidden_in, ln_attn, ln_ffn, w_query, w_key, w_value, w_out, bias_table, w_gate, w_up, w_down, w_router, expert_in, expert_out, expert_ids):
        tp = lax.axis_index('tp')
        ep = lax.axis_index('ep')
        nb, npos, d_model = hidden_in.shape
        hb = nb // 2
        seq = 2 * npos
        tokens = nb * npos
        num_experts = w_router.shape[1]
        local_experts = expert_in.shape[0]
        groups = num_experts // local_experts
        capacity = 4 * tokens // num_experts

        slots = slot_ids_of(expert_ids.reshape(tokens, 2), num_experts, capacity)
        slots_all = lax.all_gather(slots, ('tp', 'ep'))

        u_own = jnp.stack([bias_vectors(bias_table[l], seq) for l in range(2)])
        x, kv_peer, k_all, v_all = dense_layers(hidden_in, ln_attn, ln_ffn, w_query, w_key, w_value, w_out, w_gate, w_up, w_down, u_own)

        half = hb // 2
        h_y = swap(x, 'tp', TP_SWAP)
        h_x = swap(x, 'ep', X_SWAP)
        d_lo = swap(h_y[:half], 'ep', X_SWAP)
        d_hi = swap(h_x[half:], 'tp', TP_SWAP)
        parts = [(0, 0, 0, x), (1, 0, 0, h_y), (0, 2, 0, h_x), (1, 2, 0, d_lo), (1, 2, half, d_hi)]
        parts += [(i, j ^ 1, o, swap(h, 'ep', CORE_SWAP)) for i, j, o, h in parts]
        b_groups = jnp.zeros((2, 4, nb, npos, d_model), BF16)
        for i, j, o, h in parts:
            rows = rms_norm(h, ln_ffn[1]).reshape(h.shape[0], 2, npos, d_model)
            rows = jnp.swapaxes(rows, 0, 1)[:, None]
            b_groups = lax.dynamic_update_slice(b_groups, rows, (0, ep ^ j, (tp ^ i) * hb + o, 0, 0))
        b_groups = b_groups.reshape(groups, tokens, d_model)

        own = lax.dynamic_slice_in_dim(x, tp * npos, npos, 1)
        peer = lax.dynamic_slice_in_dim(h_y, tp * npos, npos, 1)
        hidden = by_tp(tp, own, peer, 0)

        me = tp * 4 + ep
        local_slots = local_experts * capacity
        loc = slots_all - me * local_slots
        columns = jnp.arange(local_slots, dtype=jnp.int32)[None, :, None]
        select = ((loc[:, None, :, 0] == columns) | (loc[:, None, :, 1] == columns)).astype(BF16)
        rows = jnp.einsum('gsn,gnd->gsd', select, b_groups, preferred_element_type=F32).astype(BF16)
        rows = rows.reshape(groups, local_experts, capacity, d_model)
        rows = jnp.swapaxes(rows, 0, 1).reshape(local_experts, groups * capacity, d_model)
        expert_hidden = jnp.einsum('erd,edf->erf', rows, expert_in, preferred_element_type=F32)
        expert_hidden = jax.nn.gelu(expert_hidden).astype(BF16)
        kv_peer, rows_done = lax.optimization_barrier((kv_peer, rows))
        kv_got = swap(kv_peer, 'tp', TP_SWAP)
        result = jnp.einsum('erf,efd->erd', expert_hidden, expert_out, preferred_element_type=F32).astype(BF16)
        result, kv_got = lax.optimization_barrier((result, kv_got))
        caches = []
        for m, full in enumerate((k_all, v_all)):
            full = lax.dynamic_update_slice(full, kv_got[m][None], (1, (1 - tp) * hb, 0, 0))
            caches.append(jnp.swapaxes(full.reshape(2, nb, -1, 64, seq), 3, 4))
        result = result.reshape(1, local_experts, groups * capacity, d_model)
        returned = lax.all_to_all(result, ('tp', 'ep'), 2, 0, tiled=True)
        returned = returned.reshape(num_experts * capacity, d_model)

        normed = rms_norm(hidden, ln_ffn[1]).reshape(tokens, d_model)
        logits = jnp.dot(normed.astype(F32), w_router, precision=lax.Precision.HIGHEST)
        probs = jax.nn.softmax(logits, axis=-1)
        ids = expert_ids.reshape(tokens, 2)
        experts = jnp.arange(num_experts, dtype=jnp.int32)
        picked = [jnp.sum(jnp.where(ids[:, c:c + 1] == experts, probs, 0.0), axis=1, keepdims=True) for c in range(2)]
        denom = picked[0] + picked[1]
        slot_columns = jnp.arange(num_experts * capacity, dtype=jnp.int32)
        moe_sum = sum((picked[c] / denom) * mm((slots[:, c:c + 1] == slot_columns).astype(BF16), returned) for c in range(2))
        hidden = (hidden.astype(F32) + moe_sum.reshape(hidden.shape)).astype(BF16)
        return hidden, caches[0], caches[1]

    return jax.shard_map(device_fn, mesh=mesh, in_specs=in_specs, out_specs=(act_spec, cache_spec, cache_spec), check_vma=False)
```

```python
import jax
import jax.numpy as jnp
import numpy as np
from jax import lax
from jax.experimental import pallas as pl
from jax.experimental.pallas import tpu as pltpu
from jax.sharding import PartitionSpec as P

EXACT_BUCKETS = 16
THRESHOLDS = (18, 20, 23, 26, 30, 34, 39, 45, 51, 58, 66, 76, 86, 98, 112)
EPSILON = 1e-6
BF16 = jnp.bfloat16
F32 = jnp.float32

def bias_vectors(bias_rows, seq_len):
    rel = (-np.arange(seq_len)) % seq_len
    bucket = np.minimum(rel, EXACT_BUCKETS)
    for threshold in THRESHOLDS:
        bucket = bucket + (rel >= threshold)
    hot = jnp.asarray(bucket, jnp.int32)[None, None, :] == jnp.arange(bias_rows.shape[1])[None, :, None]
    return jnp.sum(jnp.where(hot, bias_rows[:, :, None], 0.0), axis=1)


MESH = pl.DeviceIdType.MESH
HEADS = 6
NQ = 192
NO = 96
NF = 128
FC = 512


def swap_targets():
    tp = lax.axis_index('tp')
    ep = lax.axis_index('ep')
    core = ep + 1 - 2 * lax.rem(ep, 2)
    across = lax.rem(ep + 2, 4)
    return tp, ep, {'tp': 1 - tp}, {'ep': across}, {'ep': core}


def greet(targets):
    barrier = pltpu.get_barrier_semaphore()
    for target in targets:
        pl.semaphore_signal(barrier, inc=1, device_id=target, device_id_type=MESH)
    pl.semaphore_wait(barrier, len(targets))


def attend_rows(qkv_ref, bias_ref, base, o_ref, side, s):
    width = HEADS * 64
    rows = 128
    lane = lax.broadcasted_iota(jnp.int32, (rows, 128), 1)
    units = [(pair, blk, sd) for pair in range(HEADS // 2) for blk in range(2) for sd in range(2)]
    scores = []
    for pair, blk, sd in units:
        lo = pair * 128
        keys = rows * (blk + 1)
        q = qkv_ref[blk * rows:(blk + 1) * rows, lo:lo + 128]
        k = qkv_ref[0:keys, width + lo:width + lo + 128]
        mine = (lane < 64) if sd == 0 else (lane >= 64)
        qh = jnp.where(mine, q, jnp.zeros_like(q))
        sc = lax.dot_general(qh, k, (((1,), (1,)), ((), ())), preferred_element_type=F32)
        scores.append(sc * 0.125 + bias_ref[base + 2 * pair + sd, blk * rows:(blk + 1) * rows, 0:keys])
    tops = [jnp.max(sc, axis=1, keepdims=True) for sc in scores]
    exps = [jnp.exp(sc - m) for sc, m in zip(scores, tops)]
    sums = [jnp.sum(p, axis=1, keepdims=True) for p in exps]
    probs = [(p * (1.0 / l)).astype(BF16) for p, l in zip(exps, sums)]
    outs = []
    for (pair, blk, sd), p in zip(units, probs):
        lo = pair * 128
        v = qkv_ref[0:rows * (blk + 1), 2 * width + lo:2 * width + lo + 128]
        outs.append(jnp.dot(p, v, preferred_element_type=F32))
    for i in range(0, len(units), 2):
        pair, blk, _ = units[i]
        o_ref[side, s, blk * rows:(blk + 1) * rows, pair * 128:pair * 128 + 128] = jnp.where(
            lane < 64, outs[i], outs[i + 1]).astype(BF16)


def dense_kernel(hid, lna, lnf, wq, wk, wv, wo, wg, wu, wd, u_own,
                 x_ref, kvp_ref, kc, vc,
                 own_qkv, own_o, own_g, own_u, own_d, peer_qkv, peer_o, peer_g, peer_u, peer_d,
                 u_peer, bias, qkv, o_all, b_all, acc, kvt, kvo, other,
                 ysend, yrecv, xsend, xrecv, csend, crecv, dsend, drecv, hsend, hrecv, lsem, osem):
    tp, ep, to_y, to_x, to_c = swap_targets()
    across = lax.rem(ep + 2, 4)
    hb, seq, d_model = x_ref.shape
    half = seq // 2
    width = HEADS * 64

    items = []
    for l in range(2):
        layer = [('w', l, m) for m in range(3)] + [('o', l, 0)]
        items += layer
        if l == 0:
            items += [(kind, c, 0) for c in range(3) for kind in ('g', 'u', 'd')]
    index = {item: i for i, item in enumerate(items)}

    def source(item):
        kind, l, m = item
        if kind == 'w':
            return (wq, wk, wv)[m].at[l, pl.ds(pl.multiple_of(ep * NQ, NQ), NQ), :]
        if kind == 'o':
            return wo.at[l, pl.ds(pl.multiple_of(ep * NO, NO), NO), :]
        at = pl.multiple_of(ep * (3 * NF) + l * NF, NF)
        if kind == 'd':
            return wd.at[pl.ds(at, NF), :]
        return (wg if kind == 'g' else wu).at[:, pl.ds(at, NF)]

    def place(item, r):
        kind, l, m = item
        if kind == 'w':
            return peer_qkv.at[l, m, pl.ds(pl.multiple_of(r * NQ, NQ), NQ), :]
        if kind == 'o':
            return peer_o.at[l, pl.ds(pl.multiple_of(r * NO, NO), NO), :]
        at = pl.multiple_of(r * NF, NF)
        if kind == 'd':
            return peer_d.at[l, pl.ds(at, NF), :]
        return (peer_g if kind == 'g' else peer_u).at[l, :, pl.ds(at, NF)]

    def remote(src, dst, send, recv, target):
        return pltpu.make_async_remote_copy(src_ref=src, dst_ref=dst, send_sem=send, recv_sem=recv,
                                            device_id=target, device_id_type=MESH)

    def y_copy(item):
        i = index[item]
        return remote(source(item), place(item, ep), ysend.at[i], yrecv.at[i], to_y)

    def x_copy(item):
        i = index[item]
        return remote(place(item, ep), place(item, ep), xsend.at[i], xrecv.at[i], to_x)

    def c_copy(item):
        i = index[item]
        return remote(place(item, ep), place(item, ep), csend.at[i], crecv.at[i], to_c)

    def d_copy(item):
        i = index[item]
        return remote(place(item, across), place(item, across), dsend.at[i], drecv.at[i], to_c)

    def pass_on(*names):
        for item in names:
            y_copy(item).wait_recv()
            x_copy(item).start()
            c_copy(item).start()

    def pass_core(*names):
        for item in names:
            x_copy(item).wait_recv()
            d_copy(item).start()

    def complete(*names):
        for item in names:
            c_copy(item).wait_recv()
            d_copy(item).wait_recv()

    mine_at = pl.ds(tp * hb, hb)
    peer_at = pl.ds((1 - tp) * hb, hb)
    rows_at = pl.ds(pl.multiple_of(tp * half, half), half)
    hid_a = remote(hid.at[peer_at], x_ref.at[:, rows_at, :], hsend.at[0], hrecv.at[0], to_y)
    hid_b = remote(hid.at[mine_at], other.at[:, rows_at, :], hsend.at[1], hrecv.at[1], to_y)
    u_copy = remote(u_own, u_peer, hsend.at[2], hrecv.at[2], to_y)
    loads = [pltpu.make_async_copy(s, d, lsem.at[i]) for i, (s, d) in enumerate([
        (hid.at[mine_at], x_ref.at[:, rows_at, :]),
        (wq, own_qkv.at[0]), (wk, own_qkv.at[1]), (wv, own_qkv.at[2]), (wo, own_o),
        (wg, own_g), (wu, own_u), (wd, own_d),
        (hid.at[peer_at], other.at[:, rows_at, :])])]

    greet([to_y, to_x, to_c])
    hid_a.start()
    u_copy.start()
    for item in items:
        y_copy(item).start()
    hid_b.start()
    for load in loads:
        load.start()

    def fill_bias(src, l, base):
        row = lax.broadcasted_iota(jnp.int32, (seq, seq), 0)
        col = lax.broadcasted_iota(jnp.int32, (seq, seq), 1)
        for h in range(HEADS):
            line = jnp.broadcast_to(src[l, h:h + 1, :], (seq, seq))
            toeplitz = pltpu.roll(line, 0, 1, stride=1, stride_axis=0)
            bias[base + h] = jnp.where(col <= row, toeplitz, -jnp.inf)

    def normed(rows, scale):
        wide = rows.astype(F32)
        inv = lax.rsqrt(jnp.mean(wide * wide, axis=-1, keepdims=True) + EPSILON)
        return (wide * inv * scale).astype(BF16)

    def heads_pass(l, side, lo, hi):
        def body(s, carry):
            a = normed(x_ref[s], lna[l:l + 1, :])
            for m in range(3):
                w = own_qkv[m, l] if side == 0 else peer_qkv[l, m]
                part = jnp.dot(a, w, preferred_element_type=F32).astype(BF16)
                qkv[:, m * width:(m + 1) * width] = part
                if m > 0:
                    if side == 0:
                        kvt[l, m - 1, s] = part.T
                    elif l == 1:
                        kvp_ref[m - 1, s] = part.T
            attend_rows(qkv, bias, side * HEADS, o_all, side, s)
            return carry
        lax.fori_loop(lo, hi, body, 0)

    def project_out(l):
        def body(s, carry):
            out = jnp.dot(o_all[0, s], own_o[l], preferred_element_type=F32)
            out = out + jnp.dot(o_all[1, s], peer_o[l], preferred_element_type=F32)
            x_ref[s] = (x_ref[s].astype(F32) + out).astype(BF16)
            return carry
        lax.fori_loop(0, hb, body, 0)

    def ffn_chunk(gate, up, down, first):
        def body(r, carry):
            at = pl.ds(pl.multiple_of(r * FC, FC), FC)
            b = b_all[at, :]
            g = jnp.dot(b, gate, preferred_element_type=F32)
            u = jnp.dot(b, up, preferred_element_type=F32)
            hidden = (jax.nn.gelu(g) * u).astype(BF16)
            out = jnp.dot(hidden, down, preferred_element_type=F32)
            acc[at, :] = out if first else acc[at, :] + out
            return carry
        lax.fori_loop(0, 2, body, 0)

    def ffn_own(c):
        at = slice(c * FC, (c + 1) * FC)
        ffn_chunk(own_g[:, at], own_u[:, at], own_d[at, :], c == 0)

    def ffn_peer(c):
        ffn_chunk(peer_g[c], peer_u[c], peer_d[c], False)

    w0 = [('w', 0, m) for m in range(3)]
    w1 = [('w', 1, m) for m in range(3)]
    o0, o1 = ('o', 0, 0), ('o', 1, 0)
    g = [('g', c, 0) for c in range(3)]
    u = [('u', c, 0) for c in range(3)]
    d = [('d', c, 0) for c in range(3)]

    fill_bias(u_own, 0, 0)
    u_copy.wait_recv()
    fill_bias(u_peer, 0, HEADS)
    loads[0].wait()
    hid_a.wait_recv()
    for load in loads[1:4]:
        load.wait()
    heads_pass(0, 0, 0, hb)
    pass_on(*w0, o0)
    pass_core(*w0)
    pass_on(g[0])
    pass_core(o0)
    complete(*w0, o0)
    pass_on(u[0])
    heads_pass(0, 1, 0, hb // 2)
    pass_on(d[0])
    pass_core(g[0])
    heads_pass(0, 1, hb // 2, hb)
    pass_core(u[0])
    pass_on(g[1])
    loads[4].wait()
    project_out(0)

    def norm_rows(s, carry):
        b_all[pl.ds(pl.multiple_of(s * seq, seq), seq), :] = normed(x_ref[s], lnf[0:1, :])
        return carry
    lax.fori_loop(0, hb, norm_rows, 0)
    for load in loads[5:8]:
        load.wait()
    ffn_own(0)
    pass_on(u[1])
    pass_core(d[0])
    ffn_own(1)
    pass_core(g[1])
    pass_on(d[1])
    pass_core(u[1])
    ffn_own(2)
    pass_on(g[2])
    complete(g[0], u[0], d[0])
    ffn_peer(0)
    pass_core(d[1], g[2])
    pass_on(u[2])
    complete(g[1], u[1], d[1])
    ffn_peer(1)
    fill_bias(u_own, 1, 0)
    pass_on(d[2])
    pass_core(u[2])
    fill_bias(u_peer, 1, HEADS)
    pass_on(w1[0])
    pass_core(d[2])
    complete(g[2], u[2], d[2])
    ffn_peer(2)

    def add_rows(s, carry):
        x_ref[s] = (x_ref[s].astype(F32) + acc[pl.ds(pl.multiple_of(s * seq, seq), seq), :]).astype(BF16)
        return carry
    lax.fori_loop(0, hb, add_rows, 0)

    pass_on(w1[1], w1[2])
    pass_core(w1[0])
    heads_pass(1, 0, 0, hb)
    pass_on(o1)
    pass_core(w1[1], w1[2], o1)
    complete(*w1, o1)
    stores = [pltpu.make_async_copy(kvt.at[l, m], (kc, vc)[m].at[l, mine_at], osem.at[2 * l + m])
              for l in range(2) for m in range(2)]
    for store in stores:
        store.start()
    heads_pass(1, 1, 0, hb)
    project_out(1)

    loads[8].wait()
    hid_b.wait_recv()

    def other_rows(s, carry):
        a = normed(other[s], lna[0:1, :])
        for m in range(2):
            kvo[m, s] = jnp.dot(a, own_qkv[m + 1, 0], preferred_element_type=F32).astype(BF16).T
        return carry
    lax.fori_loop(0, hb, other_rows, 0)
    stores += [pltpu.make_async_copy(kvo.at[m], (kc, vc)[m].at[0, peer_at], osem.at[4 + m]) for m in range(2)]
    for store in stores[4:]:
        store.start()
    for store in stores:
        store.wait()
    hid_a.wait_send()
    hid_b.wait_send()
    u_copy.wait_send()
    for item in items:
        y_copy(item).wait_send()
        x_copy(item).wait_send()
        c_copy(item).wait_send()
        d_copy(item).wait_send()


def dense_layers(hid, lna, lnf, wq, wk, wv, wo, wg, wu, wd, u_own):
    nb, npos, d_model = hid.shape
    hb, seq = nb // 2, 2 * npos
    width = HEADS * 64
    ff = wg.shape[1]
    any_spec = pl.BlockSpec(memory_space=pl.ANY)
    vmem = pl.BlockSpec(memory_space=pltpu.VMEM)
    n_items = 17
    dma = pltpu.SemaphoreType.DMA
    return pl.pallas_call(
        dense_kernel,
        in_specs=[any_spec, vmem, vmem] + [any_spec] * 7 + [vmem],
        out_specs=[vmem, vmem, any_spec, any_spec],
        out_shape=[jax.ShapeDtypeStruct((hb, seq, d_model), BF16),
                   jax.ShapeDtypeStruct((2, hb, width, seq), BF16),
                   jax.ShapeDtypeStruct((2, nb, width, seq), BF16),
                   jax.ShapeDtypeStruct((2, nb, width, seq), BF16)],
        scratch_shapes=[
            pltpu.VMEM((3, 2, d_model, width), BF16), pltpu.VMEM((2, width, d_model), BF16),
            pltpu.VMEM((d_model, ff), BF16), pltpu.VMEM((d_model, ff), BF16), pltpu.VMEM((ff, d_model), BF16),
            pltpu.VMEM((2, 3, d_model, width), BF16), pltpu.VMEM((2, width, d_model), BF16),
            pltpu.VMEM((3, d_model, FC), BF16), pltpu.VMEM((3, d_model, FC), BF16), pltpu.VMEM((3, FC, d_model), BF16),
            pltpu.VMEM((2, HEADS, seq), F32), pltpu.VMEM((2 * HEADS, seq, seq), F32),
            pltpu.VMEM((seq, 3 * width), BF16), pltpu.VMEM((2, hb, seq, width), BF16),
            pltpu.VMEM((hb * seq, d_model), BF16), pltpu.VMEM((hb * seq, d_model), F32),
            pltpu.VMEM((2, 2, hb, width, seq), BF16), pltpu.VMEM((2, hb, width, seq), BF16),
            pltpu.VMEM((hb, seq, d_model), BF16),
        ] + [dma((n_items,))] * 8 + [dma((3,)), dma((3,)), dma((9,)), dma((6,))],
        compiler_params=pltpu.CompilerParams(collective_id=0, has_side_effects=True, vmem_limit_bytes=62 * 1024 * 1024),
        name="dense_layers",
    )(hid, lna, lnf, wq, wk, wv, wo, wg, wu, wd, u_own)


def moe_kernel(x_ref, ids_row, ids_col, scale, w_router, kv_in, w_in, w_out,
               out_ref, kv_out,
               h_all, slots_all, rows, res, ret, win, wout, acc, total, keys, gates, own_h,
               asend, arecv, ssend, srecv, rsend, rrecv, ksend, krecv, wsem):
    tp, ep, to_y, to_x, to_c = swap_targets()
    hb, seq, d_model = x_ref.shape
    half = seq // 2
    n_exp, _, capacity, _ = rows.shape
    tokens = 2 * hb * half
    local_slots = n_exp * capacity
    chunk = win.shape[2]
    n_chunks = w_in.shape[2] // chunk
    eps = [ep, to_c['ep'], to_x['ep'], lax.rem(to_c['ep'] + 2, 4)]
    tps = [tp, 1 - tp]
    me = tp * 4 + ep
    away = [(i, j) for i in (1, 0) for j in (2, 3, 0, 1) if (i, j) != (0, 0)]

    def target(i, j):
        return {'tp': tps[i], 'ep': eps[j]}

    def remote(src, dst, send, recv, to):
        return pltpu.make_async_remote_copy(src_ref=src, dst_ref=dst, send_sem=send, recv_sem=recv,
                                            device_id=to, device_id_type=MESH)

    def piece(i, j):
        return x_ref if (i, j) == (0, 0) else h_all.at[4 * i + j - 1]

    def fetch(n_sem, src, dst, part, to):
        lo, hi = part
        return remote(piece(*src).at[lo:hi], piece(*dst).at[lo:hi], asend.at[n_sem], arecv.at[n_sem], to)

    first, second, whole = (0, hb // 2), (hb // 2, hb), (0, hb)
    y_a = fetch(0, (0, 0), (1, 0), first, to_y)
    y_b = fetch(1, (0, 0), (1, 0), second, to_y)
    x_b = fetch(2, (0, 0), (0, 2), second, to_x)
    x_a = fetch(3, (0, 0), (0, 2), first, to_x)
    c_0 = fetch(4, (0, 0), (0, 1), whole, to_c)
    d_lo = fetch(5, (1, 0), (1, 2), first, to_x)
    d_hi = fetch(6, (0, 2), (1, 2), second, to_y)
    c_ya = fetch(7, (1, 0), (1, 1), first, to_c)
    c_yb = fetch(8, (1, 0), (1, 1), second, to_c)
    c_xb = fetch(9, (0, 2), (0, 3), second, to_c)
    c_xa = fetch(10, (0, 2), (0, 3), first, to_c)
    c_dlo = fetch(11, (1, 2), (1, 3), first, to_c)
    c_dhi = fetch(12, (1, 2), (1, 3), second, to_c)
    fetches = [y_a, y_b, x_b, x_a, c_0, d_lo, d_hi, c_ya, c_yb, c_xb, c_xa, c_dlo, c_dhi]

    def weight_copies(e, c):
        at = pl.ds(c * chunk, chunk)
        return (pltpu.make_async_copy(w_in.at[e, :, at], win.at[c], wsem.at[0, c]),
                pltpu.make_async_copy(w_out.at[e, at, :], wout.at[c], wsem.at[1, c]))

    greet([target(i, j) for i, j in away])
    for copy in (y_a, x_b, c_0, y_b, x_a):
        copy.start()

    experts = lax.broadcasted_iota(jnp.int32, (64, tokens), 0)
    hot = [experts == ids_row[c:c + 1, :] for c in range(2)]
    ones = [jnp.where(h, 1.0, 0.0) for h in hot]
    earlier = jnp.where(lax.broadcasted_iota(jnp.int32, (tokens, tokens), 0)
                        < lax.broadcasted_iota(jnp.int32, (tokens, tokens), 1), 1.0, 0.0).astype(BF16)
    before = [jnp.dot(o.astype(BF16), earlier, preferred_element_type=F32) for o in ones]
    before[1] = before[1] + jnp.sum(ones[0], axis=1, keepdims=True)
    for c in range(2):
        pos = jnp.sum(jnp.where(hot[c], before[c], 0.0), axis=0, keepdims=True).astype(jnp.int32)
        slots_all[me, c:c + 1, :] = jnp.where(pos < capacity, ids_row[c:c + 1, :] * capacity + pos, -1)
    slot_sends = [remote(slots_all.at[me], slots_all.at[me], ssend.at[4 * i + j], srecv.at[4 * i + j], target(i, j))
                  for i, j in away]
    for copy in slot_sends:
        copy.start()
    for c in range(n_chunks):
        for copy in weight_copies(0, c):
            copy.start()
    rows[...] = jnp.zeros_like(rows)
    total[...] = jnp.zeros_like(total)
    for c in range(2):
        slot = slots_all[me, c:c + 1, :]
        expert = lax.shift_right_arithmetic(slot, 6)
        key = lax.bitwise_and(expert, 7) * local_slots + lax.shift_right_arithmetic(expert, 3) * capacity + lax.bitwise_and(slot, 63)
        key = jnp.where(slot < 0, -1, key).astype(F32)
        keys[:, c * 8:(c + 1) * 8] = jnp.broadcast_to(key, (8, tokens)).T
    for copy in slot_sends:
        copy.wait_recv()

    def normed(h):
        wide = h.astype(F32)
        inv = lax.rsqrt(jnp.mean(wide * wide, axis=-1, keepdims=True) + EPSILON)
        return (wide * inv * scale[...]).astype(BF16)

    slot_iota = lax.broadcasted_iota(jnp.int32, (local_slots, 2 * half), 0)

    def pick(i, j, part):
        lo, _ = part
        ref = piece(i, j)
        off = pl.multiple_of(tps[i] * (hb * half) + lo * half, 2 * half)

        def body(p, carry):
            h = ref[lo:lo + 2, pl.ds(pl.multiple_of(p * half, half), half), :].reshape(2 * half, d_model)
            b = normed(h)
            g = p * 4 + eps[j]
            loc = slots_all[g, :, pl.ds(off, 2 * half)] - me * local_slots
            match = (slot_iota == loc[0:1, :]) | (slot_iota == loc[1:2, :])
            select = jnp.where(match, 1.0, 0.0).astype(BF16)
            got = jnp.dot(select, b, preferred_element_type=F32).astype(BF16)
            for e in range(n_exp):
                rows[e, g] = rows[e, g] + got[e * capacity:(e + 1) * capacity, :]
            return carry
        lax.fori_loop(0, 2, body, 0)

    pick(0, 0, first)
    pick(0, 0, second)
    c_0.wait_recv()
    pick(0, 1, first)
    pick(0, 1, second)
    y_a.wait_recv()
    d_lo.start()
    c_ya.start()
    x_b.wait_recv()
    d_hi.start()
    c_xb.start()
    pick(1, 0, first)
    pick(0, 2, second)
    c_ya.wait_recv()
    pick(1, 1, first)
    c_xb.wait_recv()
    pick(0, 3, second)
    y_b.wait_recv()
    c_yb.start()
    x_a.wait_recv()
    c_xa.start()
    pick(1, 0, second)
    pick(0, 2, first)
    c_yb.wait_recv()
    pick(1, 1, second)
    c_xa.wait_recv()
    pick(0, 3, first)

    pos_at = pl.ds(pl.multiple_of(tp * half, half), half)
    for i in range(2):
        at = pl.ds(pl.multiple_of(tps[i] * (hb * half), hb * half), hb * half)
        h = piece(i, 0)[:, pos_at, :].reshape(hb * half, d_model)
        own_h[at, :] = h
        logits = jnp.dot(normed(h).astype(F32), w_router[...], precision=lax.Precision.HIGHEST, preferred_element_type=F32)
        ex = jnp.exp(logits - jnp.max(logits, axis=1, keepdims=True))
        probs = ex / jnp.sum(ex, axis=1, keepdims=True)
        lanes = lax.broadcasted_iota(jnp.int32, probs.shape, 1)
        picked = [jnp.sum(jnp.where(lanes == ids_col[at, c:c + 1], probs, 0.0), axis=1, keepdims=True) for c in range(2)]
        denom = picked[0] + picked[1]
        for c in range(2):
            gates[at, c:c + 1] = picked[c] / denom

    d_lo.wait_recv()
    c_dlo.start()
    pick(1, 2, first)
    d_hi.wait_recv()
    c_dhi.start()
    pick(1, 2, second)
    c_dlo.wait_recv()
    pick(1, 3, first)
    c_dhi.wait_recv()
    pick(1, 3, second)

    def returns(e):
        return [remote(res.at[e, tps[i] * 4 + eps[j]], ret.at[e, me], rsend.at[4 * i + j, e], rrecv.at[4 * i + j, e], target(i, j))
                for i, j in away]

    def combine(e):
        for copy in returns(e):
            copy.wait_recv()
        block = 256
        columns = lax.broadcasted_iota(jnp.int32, (block, local_slots), 1).astype(F32)
        table = ret[e].reshape(local_slots, d_model)

        def body(r, carry):
            at = pl.ds(pl.multiple_of(r * block, block), block)
            add = total[at, :]
            for c in range(2):
                want = keys[at, c * 8:c * 8 + 1] - (e * local_slots).astype(F32)
                select = jnp.where(columns == want, 1.0, 0.0).astype(BF16)
                add = add + gates[at, c:c + 1] * jnp.dot(select, table, preferred_element_type=F32)
            total[at, :] = add
            return carry
        lax.fori_loop(0, tokens // block, body, 0)

    lag = 3

    def expert(e, carry):
        table = rows[e].reshape(8 * capacity, d_model)
        for c in range(n_chunks):
            for copy in weight_copies(e, c):
                copy.wait()
            up = jnp.dot(table, win[c], preferred_element_type=F32)
            out = jnp.dot(jax.nn.gelu(up).astype(BF16), wout[c], preferred_element_type=F32)
            if c == 0:
                acc[...] = out
            elif c < n_chunks - 1:
                acc[...] = acc[...] + out
            else:
                res[e] = (acc[...] + out).astype(BF16).reshape(8, capacity, d_model)

            @pl.when(e < n_exp - 1)
            def _():
                for copy in weight_copies(e + 1, c):
                    copy.start()
        for copy in returns(e):
            copy.start()
        ret[e, me] = res[e, me]

        @pl.when(e >= lag)
        def _():
            combine(e - lag)
        return carry
    lax.fori_loop(0, n_exp, expert, 0)
    kv_send = [remote(kv_in.at[m], kv_out.at[m], ksend.at[m], krecv.at[m], to_y) for m in range(2)]
    for copy in kv_send:
        copy.start()

    def last(e, carry):
        combine(e)
        return carry
    lax.fori_loop(n_exp - lag, n_exp, last, 0)
    out_ref[...] = (own_h[...].astype(F32) + total[...]).astype(BF16).reshape(out_ref.shape)

    for copy in fetches + slot_sends:
        copy.wait_send()

    def drain(e, carry):
        for copy in returns(e):
            copy.wait_send()
        return carry
    lax.fori_loop(0, n_exp, drain, 0)
    for copy in kv_send:
        copy.wait()


def moe_layer(x, ids, scale, w_router, kv_peer, w_in, w_out):
    hb, seq, d_model = x.shape
    tokens = hb * seq
    n_exp, _, ff = w_in.shape
    capacity = 4 * tokens // w_router.shape[1]
    chunk = 768
    n_chunks = ff // chunk
    vmem = pl.BlockSpec(memory_space=pltpu.VMEM)
    any_spec = pl.BlockSpec(memory_space=pl.ANY)
    dma = pltpu.SemaphoreType.DMA
    slot_rows = pltpu.VMEM((n_exp, 8, capacity, d_model), BF16)
    return pl.pallas_call(
        moe_kernel,
        in_specs=[vmem] * 6 + [any_spec] * 2,
        out_specs=[vmem, vmem],
        out_shape=[jax.ShapeDtypeStruct((2 * hb, seq // 2, d_model), BF16),
                   jax.ShapeDtypeStruct(kv_peer.shape, BF16)],
        scratch_shapes=[
            pltpu.VMEM((7, hb, seq, d_model), BF16), pltpu.VMEM((8, 2, tokens), jnp.int32),
            slot_rows, slot_rows, slot_rows,
            pltpu.VMEM((n_chunks, d_model, chunk), BF16), pltpu.VMEM((n_chunks, chunk, d_model), BF16),
            pltpu.VMEM((8 * capacity, d_model), F32), pltpu.VMEM((tokens, d_model), F32),
            pltpu.VMEM((tokens, 16), F32), pltpu.VMEM((tokens, 2), F32), pltpu.VMEM((tokens, d_model), BF16),
            dma((13,)), dma((13,)), dma((8,)), dma((8,)), dma((8, n_exp)), dma((8, n_exp)), dma((2,)), dma((2,)), dma((2, n_chunks)),
        ],
        compiler_params=pltpu.CompilerParams(collective_id=1, has_side_effects=True, vmem_limit_bytes=62 * 1024 * 1024),
        name="moe_layer",
    )(x, ids.T, ids, scale, w_router, kv_peer, w_in, w_out)


def solution(mesh):
    act_spec = P(('dp', 'ep'), 'tp', None)
    col_spec = P(None, None, 'tp')
    row_spec = P(None, 'tp', None)
    expert_spec = P(('tp', 'ep'), None, None)
    cache_spec = P(None, ('dp', 'ep'), 'tp', None, None)
    in_specs = (act_spec, P(), P(), col_spec, col_spec, col_spec, row_spec, row_spec,
                P(None, 'tp'), P(None, 'tp'), P('tp', None), P(), expert_spec, expert_spec, act_spec)

    def device_fn(hidden_in, ln_attn, ln_ffn, w_query, w_key, w_value, w_out, bias_table, w_gate, w_up, w_down, w_router, expert_in, expert_out, expert_ids):
        tp = lax.axis_index('tp')
        ep = lax.axis_index('ep')
        nb, npos, d_model = hidden_in.shape
        hb = nb // 2
        seq = 2 * npos

        u_own = jnp.stack([bias_vectors(bias_table[l], seq) for l in range(2)])
        x, kv_peer, k_all, v_all = dense_layers(hidden_in, ln_attn, ln_ffn, w_query, w_key, w_value, w_out, w_gate, w_up, w_down, u_own)

        hidden, kv_got = moe_layer(x, expert_ids.reshape(nb * npos, 2), ln_ffn[1:2], w_router, kv_peer, expert_in, expert_out)
        caches = []
        for m, full in enumerate((k_all, v_all)):
            full = lax.dynamic_update_slice(full, kv_got[m][None], (1, (1 - tp) * hb, 0, 0))
            caches.append(jnp.swapaxes(full.reshape(2, nb, -1, 64, seq), 3, 4))
        return hidden, caches[0], caches[1]

    return jax.shard_map(device_fn, mesh=mesh, in_specs=in_specs, out_specs=(act_spec, cache_spec, cache_spec), check_vma=False)
```

```python
import jax
import jax.numpy as jnp
import numpy as np
from jax import lax
from jax.experimental import pallas as pl
from jax.experimental.pallas import tpu as pltpu
from jax.sharding import PartitionSpec as P

EXACT_BUCKETS = 16
THRESHOLDS = (18, 20, 23, 26, 30, 34, 39, 45, 51, 58, 66, 76, 86, 98, 112)
EPSILON = 1e-6
BF16 = jnp.bfloat16
F32 = jnp.float32

def bucket_hot(buckets, seq_len):
    k = lax.broadcasted_iota(jnp.int32, (buckets, seq_len), 1)
    rel = jnp.where(k == 0, 0, seq_len - k)
    bucket = jnp.minimum(rel, EXACT_BUCKETS)
    for threshold in THRESHOLDS:
        bucket = bucket + jnp.where(rel >= threshold, 1, 0)
    return jnp.where(bucket == lax.broadcasted_iota(jnp.int32, (buckets, seq_len), 0), 1.0, 0.0)


MESH = pl.DeviceIdType.MESH
HEADS = 6
NQ = 192
NO = 96
NF = 128
FC = 512


def swap_targets():
    tp = lax.axis_index('tp')
    ep = lax.axis_index('ep')
    core = ep + 1 - 2 * lax.rem(ep, 2)
    across = lax.rem(ep + 2, 4)
    return tp, ep, {'tp': 1 - tp}, {'ep': across}, {'ep': core}


def greet(targets):
    barrier = pltpu.get_barrier_semaphore()
    for target in targets:
        pl.semaphore_signal(barrier, inc=1, device_id=target, device_id_type=MESH)
    pl.semaphore_wait(barrier, len(targets))


def attend_rows(qkv_ref, bias_ref, base, o_ref, side, s):
    width = HEADS * 64
    rows = 128
    lane = lax.broadcasted_iota(jnp.int32, (rows, 128), 1)
    units = [(pair, blk, sd) for pair in range(HEADS // 2) for blk in range(2) for sd in range(2)]
    scores = []
    for pair, blk, sd in units:
        lo = pair * 128
        keys = rows * (blk + 1)
        q = qkv_ref[blk * rows:(blk + 1) * rows, lo:lo + 128]
        k = qkv_ref[0:keys, width + lo:width + lo + 128]
        mine = (lane < 64) if sd == 0 else (lane >= 64)
        qh = jnp.where(mine, q, jnp.zeros_like(q))
        sc = lax.dot_general(qh, k, (((1,), (1,)), ((), ())), preferred_element_type=F32)
        scores.append(sc * 0.125 + bias_ref[base + 2 * pair + sd, blk * rows:(blk + 1) * rows, 0:keys])
    tops = [jnp.max(sc, axis=1, keepdims=True) for sc in scores]
    exps = [jnp.exp(sc - m) for sc, m in zip(scores, tops)]
    sums = [jnp.sum(p, axis=1, keepdims=True) for p in exps]
    probs = [(p * (1.0 / l)).astype(BF16) for p, l in zip(exps, sums)]
    outs = []
    for (pair, blk, sd), p in zip(units, probs):
        lo = pair * 128
        v = qkv_ref[0:rows * (blk + 1), 2 * width + lo:2 * width + lo + 128]
        outs.append(jnp.dot(p, v, preferred_element_type=F32))
    for i in range(0, len(units), 2):
        pair, blk, _ = units[i]
        o_ref[side, s, blk * rows:(blk + 1) * rows, pair * 128:pair * 128 + 128] = jnp.where(
            lane < 64, outs[i], outs[i + 1]).astype(BF16)


def dense_kernel(hid, lna, lnf, wq, wk, wv, wo, wg, wu, wd, table_own,
                 x_ref, kvp_ref, kc, vc,
                 own_qkv, own_o, own_g, own_u, own_d, peer_qkv, peer_o, peer_g, peer_u, peer_d,
                 table_peer, bias, qkv, o_all, b_all, acc, kvt, kvo, other,
                 ysend, yrecv, xsend, xrecv, csend, crecv, dsend, drecv, hsend, hrecv, lsem, osem):
    tp, ep, to_y, to_x, to_c = swap_targets()
    across = lax.rem(ep + 2, 4)
    hb, seq, d_model = x_ref.shape
    half = seq // 2
    width = HEADS * 64

    items = []
    for l in range(2):
        layer = [('w', l, m) for m in range(3)] + [('o', l, 0)]
        items += layer
        if l == 0:
            items += [(kind, c, 0) for c in range(3) for kind in ('g', 'u', 'd')]
    index = {item: i for i, item in enumerate(items)}

    def source(item):
        kind, l, m = item
        if kind == 'w':
            return (wq, wk, wv)[m].at[l, pl.ds(pl.multiple_of(ep * NQ, NQ), NQ), :]
        if kind == 'o':
            return wo.at[l, pl.ds(pl.multiple_of(ep * NO, NO), NO), :]
        at = pl.multiple_of(ep * (3 * NF) + l * NF, NF)
        if kind == 'd':
            return wd.at[pl.ds(at, NF), :]
        return (wg if kind == 'g' else wu).at[:, pl.ds(at, NF)]

    def place(item, r):
        kind, l, m = item
        if kind == 'w':
            return peer_qkv.at[l, m, pl.ds(pl.multiple_of(r * NQ, NQ), NQ), :]
        if kind == 'o':
            return peer_o.at[l, pl.ds(pl.multiple_of(r * NO, NO), NO), :]
        at = pl.multiple_of(r * NF, NF)
        if kind == 'd':
            return peer_d.at[l, pl.ds(at, NF), :]
        return (peer_g if kind == 'g' else peer_u).at[l, :, pl.ds(at, NF)]

    def remote(src, dst, send, recv, target):
        return pltpu.make_async_remote_copy(src_ref=src, dst_ref=dst, send_sem=send, recv_sem=recv,
                                            device_id=target, device_id_type=MESH)

    def y_copy(item):
        i = index[item]
        return remote(source(item), place(item, ep), ysend.at[i], yrecv.at[i], to_y)

    def x_copy(item):
        i = index[item]
        return remote(place(item, ep), place(item, ep), xsend.at[i], xrecv.at[i], to_x)

    def c_copy(item):
        i = index[item]
        return remote(place(item, ep), place(item, ep), csend.at[i], crecv.at[i], to_c)

    def d_copy(item):
        i = index[item]
        return remote(place(item, across), place(item, across), dsend.at[i], drecv.at[i], to_c)

    def pass_on(*names):
        for item in names:
            y_copy(item).wait_recv()
            x_copy(item).start()
            c_copy(item).start()

    def pass_core(*names):
        for item in names:
            x_copy(item).wait_recv()
            d_copy(item).start()

    def complete(*names):
        for item in names:
            c_copy(item).wait_recv()
            d_copy(item).wait_recv()

    mine_at = pl.ds(tp * hb, hb)
    peer_at = pl.ds((1 - tp) * hb, hb)
    rows_at = pl.ds(pl.multiple_of(tp * half, half), half)
    hid_a = remote(hid.at[peer_at], x_ref.at[:, rows_at, :], hsend.at[0], hrecv.at[0], to_y)
    hid_b = remote(hid.at[mine_at], other.at[:, rows_at, :], hsend.at[1], hrecv.at[1], to_y)
    u_copy = remote(table_own, table_peer, hsend.at[2], hrecv.at[2], to_y)
    loads = [pltpu.make_async_copy(s, d, lsem.at[i]) for i, (s, d) in enumerate([
        (hid.at[mine_at], x_ref.at[:, rows_at, :]),
        (wq, own_qkv.at[0]), (wk, own_qkv.at[1]), (wv, own_qkv.at[2]), (wo, own_o),
        (wg, own_g), (wu, own_u), (wd, own_d),
        (hid.at[peer_at], other.at[:, rows_at, :])])]

    greet([to_y, to_x, to_c])
    hid_a.start()
    u_copy.start()
    for item in items:
        y_copy(item).start()
    hid_b.start()
    for load in loads:
        load.start()

    def fill_bias(src, l, base):
        row = lax.broadcasted_iota(jnp.int32, (seq, seq), 0)
        col = lax.broadcasted_iota(jnp.int32, (seq, seq), 1)
        lines = jnp.dot(src[l], bucket_hot(src.shape[2], seq), precision=lax.Precision.HIGHEST, preferred_element_type=F32)
        for h in range(HEADS):
            line = jnp.broadcast_to(lines[h:h + 1, :], (seq, seq))
            toeplitz = pltpu.roll(line, 0, 1, stride=1, stride_axis=0)
            bias[base + h] = jnp.where(col <= row, toeplitz, -jnp.inf)

    def normed(rows, scale):
        wide = rows.astype(F32)
        inv = lax.rsqrt(jnp.mean(wide * wide, axis=-1, keepdims=True) + EPSILON)
        return (wide * inv * scale).astype(BF16)

    def heads_pass(l, side, lo, hi):
        def body(s, carry):
            a = normed(x_ref[s], lna[l:l + 1, :])
            for m in range(3):
                w = own_qkv[m, l] if side == 0 else peer_qkv[l, m]
                part = jnp.dot(a, w, preferred_element_type=F32).astype(BF16)
                qkv[:, m * width:(m + 1) * width] = part
                if m > 0:
                    if side == 0:
                        kvt[l, m - 1, s] = part.T
                    elif l == 1:
                        kvp_ref[m - 1, s] = part.T
            attend_rows(qkv, bias, side * HEADS, o_all, side, s)
            return carry
        lax.fori_loop(lo, hi, body, 0)

    def project_out(l):
        def body(s, carry):
            out = jnp.dot(o_all[0, s], own_o[l], preferred_element_type=F32)
            out = out + jnp.dot(o_all[1, s], peer_o[l], preferred_element_type=F32)
            x_ref[s] = (x_ref[s].astype(F32) + out).astype(BF16)
            return carry
        lax.fori_loop(0, hb, body, 0)

    def ffn_chunk(gate, up, down, first):
        def body(r, carry):
            at = pl.ds(pl.multiple_of(r * FC, FC), FC)
            b = b_all[at, :]
            g = jnp.dot(b, gate[...], preferred_element_type=F32)
            u = jnp.dot(b, up[...], preferred_element_type=F32)
            hidden = (jax.nn.gelu(g) * u).astype(BF16)
            out = jnp.dot(hidden, down[...], preferred_element_type=F32)
            acc[at, :] = out if first else acc[at, :] + out
            return carry
        lax.fori_loop(0, 2, body, 0)

    def ffn_own(c):
        at = pl.ds(c * FC, FC)
        ffn_chunk(own_g.at[:, at], own_u.at[:, at], own_d.at[at, :], c == 0)

    def ffn_peer(c):
        ffn_chunk(peer_g.at[c], peer_u.at[c], peer_d.at[c], False)

    w0 = [('w', 0, m) for m in range(3)]
    w1 = [('w', 1, m) for m in range(3)]
    o0, o1 = ('o', 0, 0), ('o', 1, 0)
    g = [('g', c, 0) for c in range(3)]
    u = [('u', c, 0) for c in range(3)]
    d = [('d', c, 0) for c in range(3)]

    fill_bias(table_own, 0, 0)
    u_copy.wait_recv()
    fill_bias(table_peer, 0, HEADS)
    loads[0].wait()
    hid_a.wait_recv()
    for load in loads[1:4]:
        load.wait()
    heads_pass(0, 0, 0, hb)
    pass_on(*w0, o0)
    pass_core(*w0)
    pass_on(g[0])
    pass_core(o0)
    complete(*w0, o0)
    pass_on(u[0])
    heads_pass(0, 1, 0, hb // 2)
    pass_on(d[0])
    pass_core(g[0])
    heads_pass(0, 1, hb // 2, hb)
    pass_core(u[0])
    pass_on(g[1])
    loads[4].wait()
    project_out(0)

    def norm_rows(s, carry):
        b_all[pl.ds(pl.multiple_of(s * seq, seq), seq), :] = normed(x_ref[s], lnf[0:1, :])
        return carry
    lax.fori_loop(0, hb, norm_rows, 0)
    for load in loads[5:8]:
        load.wait()
    ffn_own(0)
    pass_on(u[1])
    pass_core(d[0])
    ffn_own(1)
    pass_core(g[1])
    pass_on(d[1])
    pass_core(u[1])
    ffn_own(2)
    pass_on(g[2])
    complete(g[0], u[0], d[0])
    ffn_peer(0)
    pass_core(d[1], g[2])
    pass_on(u[2])
    complete(g[1], u[1], d[1])
    ffn_peer(1)
    fill_bias(table_own, 1, 0)
    pass_on(d[2])
    pass_core(u[2])
    fill_bias(table_peer, 1, HEADS)
    pass_on(w1[0])
    pass_core(d[2])
    complete(g[2], u[2], d[2])
    ffn_peer(2)

    def add_rows(s, carry):
        x_ref[s] = (x_ref[s].astype(F32) + acc[pl.ds(pl.multiple_of(s * seq, seq), seq), :]).astype(BF16)
        return carry
    lax.fori_loop(0, hb, add_rows, 0)

    pass_on(w1[1], w1[2])
    pass_core(w1[0])
    heads_pass(1, 0, 0, hb)
    pass_on(o1)
    pass_core(w1[1], w1[2], o1)
    complete(*w1, o1)
    stores = [pltpu.make_async_copy(kvt.at[l, m], (kc, vc)[m].at[l, mine_at], osem.at[2 * l + m])
              for l in range(2) for m in range(2)]
    for store in stores:
        store.start()
    heads_pass(1, 1, 0, hb)
    project_out(1)

    loads[8].wait()
    hid_b.wait_recv()

    def other_rows(s, carry):
        a = normed(other[s], lna[0:1, :])
        for m in range(2):
            kvo[m, s] = jnp.dot(a, own_qkv[m + 1, 0], preferred_element_type=F32).astype(BF16).T
        return carry
    lax.fori_loop(0, hb, other_rows, 0)
    stores += [pltpu.make_async_copy(kvo.at[m], (kc, vc)[m].at[0, peer_at], osem.at[4 + m]) for m in range(2)]
    for store in stores[4:]:
        store.start()
    for store in stores:
        store.wait()
    hid_a.wait_send()
    hid_b.wait_send()
    u_copy.wait_send()
    for item in items:
        y_copy(item).wait_send()
        x_copy(item).wait_send()
        c_copy(item).wait_send()
        d_copy(item).wait_send()


def dense_layers(hid, lna, lnf, wq, wk, wv, wo, wg, wu, wd, bias_table):
    nb, npos, d_model = hid.shape
    hb, seq = nb // 2, 2 * npos
    width = HEADS * 64
    ff = wg.shape[1]
    any_spec = pl.BlockSpec(memory_space=pl.ANY)
    vmem = pl.BlockSpec(memory_space=pltpu.VMEM)
    n_items = 17
    dma = pltpu.SemaphoreType.DMA
    return pl.pallas_call(
        dense_kernel,
        in_specs=[any_spec, vmem, vmem] + [any_spec] * 7 + [vmem],
        out_specs=[vmem, vmem, any_spec, any_spec],
        out_shape=[jax.ShapeDtypeStruct((hb, seq, d_model), BF16),
                   jax.ShapeDtypeStruct((2, hb, width, seq), BF16),
                   jax.ShapeDtypeStruct((2, nb, width, seq), BF16),
                   jax.ShapeDtypeStruct((2, nb, width, seq), BF16)],
        scratch_shapes=[
            pltpu.VMEM((3, 2, d_model, width), BF16), pltpu.VMEM((2, width, d_model), BF16),
            pltpu.VMEM((d_model, ff), BF16), pltpu.VMEM((d_model, ff), BF16), pltpu.VMEM((ff, d_model), BF16),
            pltpu.VMEM((2, 3, d_model, width), BF16), pltpu.VMEM((2, width, d_model), BF16),
            pltpu.VMEM((3, d_model, FC), BF16), pltpu.VMEM((3, d_model, FC), BF16), pltpu.VMEM((3, FC, d_model), BF16),
            pltpu.VMEM(bias_table.shape, F32), pltpu.VMEM((2 * HEADS, seq, seq), F32),
            pltpu.VMEM((seq, 3 * width), BF16), pltpu.VMEM((2, hb, seq, width), BF16),
            pltpu.VMEM((hb * seq, d_model), BF16), pltpu.VMEM((hb * seq, d_model), F32),
            pltpu.VMEM((2, 2, hb, width, seq), BF16), pltpu.VMEM((2, hb, width, seq), BF16),
            pltpu.VMEM((hb, seq, d_model), BF16),
        ] + [dma((n_items,))] * 8 + [dma((3,)), dma((3,)), dma((9,)), dma((6,))],
        compiler_params=pltpu.CompilerParams(collective_id=0, has_side_effects=True, vmem_limit_bytes=62 * 1024 * 1024),
        name="dense_layers",
    )(hid, lna, lnf, wq, wk, wv, wo, wg, wu, wd, bias_table)


def moe_kernel(x_ref, ids, lnf, w_router, kv_in, w_in, w_out,
               out_ref, kv_out,
               h_all, slots_all, rows, res, ret, win, wout, acc, total, keys, gates, own_h, ids_row,
               asend, arecv, ssend, srecv, rsend, rrecv, ksend, krecv, wsem):
    tp, ep, to_y, to_x, to_c = swap_targets()
    hb, seq, d_model = x_ref.shape
    half = seq // 2
    n_exp, _, capacity, _ = rows.shape
    tokens = 2 * hb * half
    local_slots = n_exp * capacity
    chunk = win.shape[2]
    n_chunks = w_in.shape[2] // chunk
    eps = [ep, to_c['ep'], to_x['ep'], lax.rem(to_c['ep'] + 2, 4)]
    tps = [tp, 1 - tp]
    me = tp * 4 + ep
    away = [(i, j) for i in (1, 0) for j in (2, 3, 0, 1) if (i, j) != (0, 0)]

    def target(i, j):
        return {'tp': tps[i], 'ep': eps[j]}

    def remote(src, dst, send, recv, to):
        return pltpu.make_async_remote_copy(src_ref=src, dst_ref=dst, send_sem=send, recv_sem=recv,
                                            device_id=to, device_id_type=MESH)

    def piece(i, j):
        return x_ref if (i, j) == (0, 0) else h_all.at[4 * i + j - 1]

    def fetch(n_sem, src, dst, part, to):
        lo, hi = part
        return remote(piece(*src).at[lo:hi], piece(*dst).at[lo:hi], asend.at[n_sem], arecv.at[n_sem], to)

    first, second, whole = (0, hb // 2), (hb // 2, hb), (0, hb)
    y_a = fetch(0, (0, 0), (1, 0), first, to_y)
    y_b = fetch(1, (0, 0), (1, 0), second, to_y)
    x_b = fetch(2, (0, 0), (0, 2), second, to_x)
    x_a = fetch(3, (0, 0), (0, 2), first, to_x)
    c_0 = fetch(4, (0, 0), (0, 1), whole, to_c)
    d_lo = fetch(5, (1, 0), (1, 2), first, to_x)
    d_hi = fetch(6, (1, 0), (1, 2), second, to_x)
    c_ya = fetch(7, (1, 0), (1, 1), first, to_c)
    c_yb = fetch(8, (1, 0), (1, 1), second, to_c)
    c_xb = fetch(9, (0, 2), (0, 3), second, to_c)
    c_xa = fetch(10, (0, 2), (0, 3), first, to_c)
    c_dlo = fetch(11, (1, 2), (1, 3), first, to_c)
    c_dhi = fetch(12, (1, 2), (1, 3), second, to_c)
    fetches = [y_a, y_b, x_b, x_a, c_0, d_lo, d_hi, c_ya, c_yb, c_xb, c_xa, c_dlo, c_dhi]

    def weight_copies(e, c):
        at = pl.ds(c * chunk, chunk)
        return (pltpu.make_async_copy(w_in.at[e, :, at], win.at[c], wsem.at[0, c]),
                pltpu.make_async_copy(w_out.at[e, at, :], wout.at[c], wsem.at[1, c]))

    greet([target(i, j) for i, j in away])
    kv_send = [remote(kv_in.at[m], kv_out.at[m], ksend.at[m], krecv.at[m], to_y) for m in range(2)]
    for copy in [y_a, x_a, c_0, y_b, x_b] + kv_send:
        copy.start()
    for s in range(ids.shape[0]):
        ids_row[:, s * half:(s + 1) * half] = ids[s]

    experts = lax.broadcasted_iota(jnp.int32, (64, tokens), 0)
    hot = [experts == ids_row[c:c + 1, :] for c in range(2)]
    ones = [jnp.where(h, 1.0, 0.0) for h in hot]
    earlier = jnp.where(lax.broadcasted_iota(jnp.int32, (tokens, tokens), 0)
                        < lax.broadcasted_iota(jnp.int32, (tokens, tokens), 1), 1.0, 0.0).astype(BF16)
    before = [jnp.dot(o.astype(BF16), earlier, preferred_element_type=F32) for o in ones]
    before[1] = before[1] + jnp.sum(ones[0], axis=1, keepdims=True)
    for c in range(2):
        pos = jnp.sum(jnp.where(hot[c], before[c], 0.0), axis=0, keepdims=True).astype(jnp.int32)
        slots_all[me, c:c + 1, :] = jnp.where(pos < capacity, ids_row[c:c + 1, :] * capacity + pos, -1)
    slot_sends = [remote(slots_all.at[me], slots_all.at[me], ssend.at[4 * i + j], srecv.at[4 * i + j], target(i, j))
                  for i, j in away]
    for copy in slot_sends:
        copy.start()
    for c in range(n_chunks):
        for copy in weight_copies(0, c):
            copy.start()
    rows[...] = jnp.zeros_like(rows)
    total[...] = jnp.zeros_like(total)
    for c in range(2):
        slot = slots_all[me, c:c + 1, :]
        expert = lax.shift_right_arithmetic(slot, 6)
        key = lax.bitwise_and(expert, 7) * local_slots + lax.shift_right_arithmetic(expert, 3) * capacity + lax.bitwise_and(slot, 63)
        key = jnp.where(slot < 0, -1, key).astype(F32)
        keys[:, c * 8:(c + 1) * 8] = jnp.broadcast_to(key, (8, tokens)).T
        keys[:, 16 + c * 8:24 + c * 8] = jnp.broadcast_to(ids_row[c:c + 1, :].astype(F32), (8, tokens)).T
    for copy in slot_sends:
        copy.wait_recv()

    def normed(h):
        wide = h.astype(F32)
        inv = lax.rsqrt(jnp.mean(wide * wide, axis=-1, keepdims=True) + EPSILON)
        return (wide * inv * lnf[1:2, :]).astype(BF16)

    slot_iota = lax.broadcasted_iota(jnp.int32, (local_slots, 2 * half), 0)

    def pick(i, j, part):
        lo, _ = part
        ref = piece(i, j)
        off = pl.multiple_of(tps[i] * (hb * half) + lo * half, 2 * half)

        def body(p, carry):
            h = ref[lo:lo + 2, pl.ds(pl.multiple_of(p * half, half), half), :].reshape(2 * half, d_model)
            b = normed(h)
            g = p * 4 + eps[j]
            loc = slots_all[g, :, pl.ds(off, 2 * half)] - me * local_slots
            match = (slot_iota == loc[0:1, :]) | (slot_iota == loc[1:2, :])
            select = jnp.where(match, 1.0, 0.0).astype(BF16)
            got = jnp.dot(select, b, preferred_element_type=F32).astype(BF16)
            for e in range(n_exp):
                rows[e, g] = rows[e, g] + got[e * capacity:(e + 1) * capacity, :]
            return carry
        lax.fori_loop(0, 2, body, 0)

    pick(0, 0, first)
    pick(0, 0, second)
    c_0.wait_recv()
    pick(0, 1, first)
    pick(0, 1, second)
    y_a.wait_recv()
    d_lo.start()
    c_ya.start()
    pick(1, 0, first)
    x_a.wait_recv()
    c_xa.start()
    pick(0, 2, first)
    c_ya.wait_recv()
    pick(1, 1, first)
    c_xa.wait_recv()
    pick(0, 3, first)
    y_b.wait_recv()
    d_hi.start()
    c_yb.start()
    x_b.wait_recv()
    c_xb.start()
    pick(1, 0, second)
    pick(0, 2, second)
    c_yb.wait_recv()
    pick(1, 1, second)
    c_xb.wait_recv()
    pick(0, 3, second)

    pos_at = pl.ds(pl.multiple_of(tp * half, half), half)
    for i in range(2):
        at = pl.ds(pl.multiple_of(tps[i] * (hb * half), hb * half), hb * half)
        h = piece(i, 0)[:, pos_at, :].reshape(hb * half, d_model)
        own_h[at, :] = h
        logits = lax.dot_general(normed(h).astype(F32), w_router[...], (((1,), (1,)), ((), ())),
                                 precision=lax.Precision.HIGHEST, preferred_element_type=F32)
        ex = jnp.exp(logits - jnp.max(logits, axis=1, keepdims=True))
        probs = ex / jnp.sum(ex, axis=1, keepdims=True)
        lanes = lax.broadcasted_iota(jnp.int32, probs.shape, 1).astype(F32)
        picked = [jnp.sum(jnp.where(lanes == keys[at, 16 + c * 8:17 + c * 8], probs, 0.0), axis=1, keepdims=True) for c in range(2)]
        denom = picked[0] + picked[1]
        for c in range(2):
            gates[at, c:c + 1] = picked[c] / denom

    d_lo.wait_recv()
    c_dlo.start()
    pick(1, 2, first)
    d_hi.wait_recv()
    c_dhi.start()
    pick(1, 2, second)
    c_dlo.wait_recv()
    pick(1, 3, first)
    c_dhi.wait_recv()
    pick(1, 3, second)

    def returns(e):
        return [remote(res.at[e, tps[i] * 4 + eps[j]], ret.at[e, me], rsend.at[4 * i + j, e], rrecv.at[4 * i + j, e], target(i, j))
                for i, j in away]

    def combine(e):
        for copy in returns(e):
            copy.wait_recv()
        block = 256
        columns = lax.broadcasted_iota(jnp.int32, (block, local_slots), 1).astype(F32)
        table = ret[e].reshape(local_slots, d_model)

        def body(r, carry):
            at = pl.ds(pl.multiple_of(r * block, block), block)
            add = total[at, :]
            for c in range(2):
                want = keys[at, c * 8:c * 8 + 1] - (e * local_slots).astype(F32)
                select = jnp.where(columns == want, 1.0, 0.0).astype(BF16)
                add = add + gates[at, c:c + 1] * jnp.dot(select, table, preferred_element_type=F32)
            total[at, :] = add
            return carry
        lax.fori_loop(0, tokens // block, body, 0)

    lag = 3

    def expert(e, carry):
        table = rows[e].reshape(8 * capacity, d_model)
        for c in range(n_chunks):
            for copy in weight_copies(e, c):
                copy.wait()
            up = jnp.dot(table, win[c], preferred_element_type=F32)
            out = jnp.dot(jax.nn.gelu(up).astype(BF16), wout[c], preferred_element_type=F32)
            if c == 0:
                acc[...] = out
            elif c < n_chunks - 1:
                acc[...] = acc[...] + out
            else:
                res[e] = (acc[...] + out).astype(BF16).reshape(8, capacity, d_model)

            @pl.when(e < n_exp - 1)
            def _():
                for copy in weight_copies(e + 1, c):
                    copy.start()
        for copy in returns(e):
            copy.start()
        ret[e, me] = res[e, me]

        @pl.when(e >= lag)
        def _():
            combine(e - lag)
        return carry
    lax.fori_loop(0, n_exp, expert, 0)

    def last(e, carry):
        combine(e)
        return carry
    lax.fori_loop(n_exp - lag, n_exp, last, 0)
    out_ref[...] = (own_h[...].astype(F32) + total[...]).astype(BF16).reshape(out_ref.shape)

    for copy in fetches + slot_sends:
        copy.wait_send()

    def drain(e, carry):
        for copy in returns(e):
            copy.wait_send()
        return carry
    lax.fori_loop(0, n_exp, drain, 0)
    for copy in kv_send:
        copy.wait()


def moe_layer(x, ids, lnf, w_router, kv_peer, w_in, w_out):
    hb, seq, d_model = x.shape
    tokens = hb * seq
    n_exp, _, ff = w_in.shape
    capacity = 4 * tokens // w_router.shape[0]
    chunk = 768
    n_chunks = ff // chunk
    vmem = pl.BlockSpec(memory_space=pltpu.VMEM)
    any_spec = pl.BlockSpec(memory_space=pl.ANY)
    dma = pltpu.SemaphoreType.DMA
    slot_rows = pltpu.VMEM((n_exp, 8, capacity, d_model), BF16)
    return pl.pallas_call(
        moe_kernel,
        in_specs=[vmem] * 5 + [any_spec] * 2,
        out_specs=[vmem, vmem],
        out_shape=[jax.ShapeDtypeStruct((2 * hb, seq // 2, d_model), BF16),
                   jax.ShapeDtypeStruct(kv_peer.shape, BF16)],
        scratch_shapes=[
            pltpu.VMEM((7, hb, seq, d_model), BF16), pltpu.VMEM((8, 2, tokens), jnp.int32),
            slot_rows, slot_rows, slot_rows,
            pltpu.VMEM((n_chunks, d_model, chunk), BF16), pltpu.VMEM((n_chunks, chunk, d_model), BF16),
            pltpu.VMEM((8 * capacity, d_model), F32), pltpu.VMEM((tokens, d_model), F32),
            pltpu.VMEM((tokens, 32), F32), pltpu.VMEM((tokens, 2), F32), pltpu.VMEM((tokens, d_model), BF16),
            pltpu.VMEM((2, tokens), jnp.int32),
            dma((13,)), dma((13,)), dma((8,)), dma((8,)), dma((8, n_exp)), dma((8, n_exp)), dma((2,)), dma((2,)), dma((2, n_chunks)),
        ],
        compiler_params=pltpu.CompilerParams(collective_id=1, has_side_effects=True, vmem_limit_bytes=62 * 1024 * 1024),
        name="moe_layer",
    )(x, ids, lnf, w_router, kv_peer, w_in, w_out)


def solution(mesh):
    act_spec = P(('dp', 'ep'), 'tp', None)
    col_spec = P(None, None, 'tp')
    row_spec = P(None, 'tp', None)
    expert_spec = P(('tp', 'ep'), None, None)
    cache_spec = P(None, ('dp', 'ep'), 'tp', None, None)
    in_specs = (act_spec, P(), P(), col_spec, col_spec, col_spec, row_spec, row_spec,
                P(None, 'tp'), P(None, 'tp'), P('tp', None), P(), expert_spec, expert_spec, act_spec)

    def device_fn(hidden_in, ln_attn, ln_ffn, w_query, w_key, w_value, w_out, bias_table, w_gate, w_up, w_down, w_router, expert_in, expert_out, expert_ids):
        tp = lax.axis_index('tp')
        nb, npos, d_model = hidden_in.shape
        hb = nb // 2
        seq = 2 * npos

        x, kv_peer, k_all, v_all = dense_layers(hidden_in, ln_attn, ln_ffn, w_query, w_key, w_value, w_out, w_gate, w_up, w_down, bias_table)

        hidden, kv_got = moe_layer(x, jnp.swapaxes(expert_ids, 1, 2), ln_ffn, w_router.T, kv_peer, expert_in, expert_out)
        fresh = jnp.zeros((2, nb, 1, 1), bool).at[1].set((jnp.arange(nb) // hb == 1 - tp)[:, None, None])
        caches = []
        for m, full in enumerate((k_all, v_all)):
            got = jnp.broadcast_to(kv_got[m][None, None], (2, 2) + kv_got.shape[1:]).reshape(full.shape)
            full = jnp.where(fresh, got, full)
            caches.append(jnp.swapaxes(full.reshape(2, nb, -1, 64, seq), 3, 4))
        return hidden, caches[0], caches[1]

    return jax.shard_map(device_fn, mesh=mesh, in_specs=in_specs, out_specs=(act_spec, cache_spec, cache_spec), check_vma=False)
```

```python
import jax
import jax.numpy as jnp
from jax import lax
from jax.experimental import pallas as pl
from jax.experimental.pallas import tpu as pltpu
from jax.sharding import PartitionSpec as P

EXACT_BUCKETS = 16
THRESHOLDS = (18, 20, 23, 26, 30, 34, 39, 45, 51, 58, 66, 76, 86, 98, 112)
EPSILON = 1e-6
BF16 = jnp.bfloat16
F32 = jnp.float32

def bucket_hot(buckets, seq_len):
    k = lax.broadcasted_iota(jnp.int32, (buckets, seq_len), 1)
    rel = jnp.where(k == 0, 0, seq_len - k)
    bucket = jnp.minimum(rel, EXACT_BUCKETS)
    for threshold in THRESHOLDS:
        bucket = bucket + jnp.where(rel >= threshold, 1, 0)
    return jnp.where(bucket == lax.broadcasted_iota(jnp.int32, (buckets, seq_len), 0), 1.0, 0.0)


MESH = pl.DeviceIdType.MESH
HEADS = 6
NQ = 192
NO = 96
NF = 128
FC = 512
WINDOW = 5
HERE, THERE = range(2)
SELF, CORE, ACROSS, CORNER = range(4)
LOCAL_EXPERTS = 8
CAPACITY = 64


def swap_targets():
    tp = lax.axis_index('tp')
    ep = lax.axis_index('ep')
    core = ep + 1 - 2 * lax.rem(ep, 2)
    across = lax.rem(ep + 2, 4)
    return tp, ep, {'tp': 1 - tp}, {'ep': across}, {'ep': core}


def greet(targets):
    barrier = pltpu.get_barrier_semaphore()
    for target in targets:
        pl.semaphore_signal(barrier, inc=1, device_id=target, device_id_type=MESH)
    pl.semaphore_wait(barrier, len(targets))


def attend_rows(qkv_ref, bias_ref, base, o_ref, side, s):
    width = HEADS * 64
    rows = 128
    lane = lax.broadcasted_iota(jnp.int32, (rows, 128), 1)
    units = [(pair, blk, sd) for pair in range(HEADS // 2) for blk in range(2) for sd in range(2)]
    scores = []
    for pair, blk, sd in units:
        lo = pair * 128
        keys = rows * (blk + 1)
        q = qkv_ref[blk * rows:(blk + 1) * rows, lo:lo + 128]
        k = qkv_ref[0:keys, width + lo:width + lo + 128]
        mine = (lane < 64) if sd == 0 else (lane >= 64)
        qh = jnp.where(mine, q, jnp.zeros_like(q))
        sc = lax.dot_general(qh, k, (((1,), (1,)), ((), ())), preferred_element_type=F32)
        scores.append(sc * 0.125 + bias_ref[base + 2 * pair + sd, blk * rows:(blk + 1) * rows, 0:keys])
    tops = [jnp.max(sc, axis=1, keepdims=True) for sc in scores]
    exps = [jnp.exp(sc - m) for sc, m in zip(scores, tops)]
    sums = [jnp.sum(p, axis=1, keepdims=True) for p in exps]
    probs = [(p * (1.0 / l)).astype(BF16) for p, l in zip(exps, sums)]
    outs = []
    for (pair, blk, sd), p in zip(units, probs):
        lo = pair * 128
        v = qkv_ref[0:rows * (blk + 1), 2 * width + lo:2 * width + lo + 128]
        outs.append(jnp.dot(p, v, preferred_element_type=F32))
    for i in range(0, len(units), 2):
        pair, blk, _ = units[i]
        o_ref[side, s, blk * rows:(blk + 1) * rows, pair * 128:pair * 128 + 128] = jnp.where(
            lane < 64, outs[i], outs[i + 1]).astype(BF16)


def dense_kernel(hid, lna, lnf, wq, wk, wv, wo, wg, wu, wd, table_own, ids, w_router,
                 rows_out, aux, own_h, kc, vc,
                 own_qkv, own_o, own_g, own_u, peer_qkv, peer_o, peer_g, peer_u, pool,
                 table_peer, bias, qkv, o_all, b_all, acc, kvt, other, x_ref, kvp_ref, h_all, slots_all, ids_row,
                 ysend, yrecv, xsend, xrecv, csend, crecv, dsend, drecv, hsend, hrecv, lsem, osem,
                 asend, arecv, ssend, srecv, ksend, krecv):
    tp, ep, to_y, to_x, to_c = swap_targets()
    eps = [ep, to_c['ep'], to_x['ep'], lax.rem(to_c['ep'] + 2, 4)]
    tps = [tp, 1 - tp]
    me = tp * 4 + ep
    away = [(i, j) for i in (1, 0) for j in (2, 3, 0, 1) if (i, j) != (0, 0)]
    n_exp, capacity = LOCAL_EXPERTS, CAPACITY
    local_slots = n_exp * capacity

    def target(i, j):
        return {'tp': tps[i], 'ep': eps[j]}

    across = lax.rem(ep + 2, 4)
    hb, seq, d_model = x_ref.shape
    half = seq // 2
    tokens = hb * seq
    width = HEADS * 64
    ff = wd.shape[0]

    attn = [[('w', l, m) for m in range(3)] + [('o', l, 0)] for l in range(2)]
    ffn = [[(kind, c, 0) for kind in ('g', 'u', 'd')] for c in range(3)]
    items = attn[0] + ffn[0] + ffn[1] + ffn[2] + attn[1]
    index = {item: i for i, item in enumerate(items)}

    def source(item):
        kind, l, m = item
        if kind == 'w':
            return (wq, wk, wv)[m].at[l, pl.ds(pl.multiple_of(ep * NQ, NQ), NQ), :]
        if kind == 'o':
            return wo.at[l, pl.ds(pl.multiple_of(ep * NO, NO), NO), :]
        at = pl.multiple_of(ep * (3 * NF) + l * NF, NF)
        if kind == 'd':
            return wd.at[pl.ds(at, NF), :]
        return (wg if kind == 'g' else wu).at[:, pl.ds(at, NF)]

    def place(item, r):
        kind, l, m = item
        if kind == 'w':
            return peer_qkv.at[l, m, pl.ds(pl.multiple_of(r * NQ, NQ), NQ), :]
        if kind == 'o':
            return peer_o.at[l, pl.ds(pl.multiple_of(r * NO, NO), NO), :]
        at = pl.multiple_of(r * NF, NF)
        if kind == 'd':
            return pool.at[pl.ds(pl.multiple_of(ff + l * FC + at, NF), NF), :]
        return (peer_g if kind == 'g' else peer_u).at[l, :, pl.ds(at, NF)]

    def remote(src, dst, send, recv, target):
        return pltpu.make_async_remote_copy(src_ref=src, dst_ref=dst, send_sem=send, recv_sem=recv,
                                            device_id=target, device_id_type=MESH)

    def y_copy(item):
        i = index[item]
        return remote(source(item), place(item, ep), ysend.at[i], yrecv.at[i], to_y)

    def x_copy(item):
        i = index[item]
        return remote(place(item, ep), place(item, ep), xsend.at[i], xrecv.at[i], to_x)

    def c_copy(item):
        i = index[item]
        return remote(place(item, ep), place(item, ep), csend.at[i], crecv.at[i], to_c)

    def d_copy(item):
        i = index[item]
        return remote(place(item, across), place(item, across), dsend.at[i], drecv.at[i], to_c)

    def pass_on(*names):
        for item in names:
            y_copy(item).wait_recv()
            if index[item] + WINDOW < len(sends):
                sends[index[item] + WINDOW].start()
            x_copy(item).start()
            c_copy(item).start()

    def pass_core(*names):
        for item in names:
            x_copy(item).wait_recv()
            d_copy(item).start()

    def complete(*names):
        for item in names:
            c_copy(item).wait_recv()
            d_copy(item).wait_recv()

    mine_at = pl.ds(tp * hb, hb)
    peer_at = pl.ds((1 - tp) * hb, hb)
    rows_at = pl.ds(pl.multiple_of(tp * half, half), half)
    hid_a = remote(hid.at[peer_at], x_ref.at[:, rows_at, :], hsend.at[0], hrecv.at[0], to_y)
    hid_b = remote(hid.at[mine_at], other.at[:, rows_at, :], hsend.at[1], hrecv.at[1], to_y)
    sends = [y_copy(item) for item in items] + [hid_b]
    u_copy = remote(table_own, table_peer, hsend.at[2], hrecv.at[2], to_y)
    loads = [pltpu.make_async_copy(s, d, lsem.at[i]) for i, (s, d) in enumerate([
        (hid.at[mine_at], x_ref.at[:, rows_at, :]),
        (wq, own_qkv.at[0]), (wk, own_qkv.at[1]), (wv, own_qkv.at[2]), (wo, own_o),
        (wg, own_g), (wu, own_u), (wd, pool.at[0:ff]),
        (hid.at[peer_at], other.at[:, rows_at, :])])]

    def piece(i, j):
        return x_ref if (i, j) == (0, 0) else h_all.at[4 * i + j - 1]

    def fetch(n_sem, src, dst, k, to):
        return remote(piece(*src).at[k], piece(*dst).at[k], asend.at[n_sem], arecv.at[n_sem], to)

    y = [fetch(k, (HERE, SELF), (THERE, SELF), k, to_y) for k in range(hb)]
    x = [fetch(4 + k, (HERE, SELF), (HERE, ACROSS), k, to_x) for k in range(hb)]
    dx = [fetch(8 + k, (THERE, SELF), (THERE, ACROSS), k, to_x) for k in range(hb)]
    c_y = [fetch(12 + k, (THERE, SELF), (THERE, CORE), k, to_c) for k in range(hb)]
    c_x = [fetch(16 + k, (HERE, ACROSS), (HERE, CORNER), k, to_c) for k in range(hb)]
    c_d = [fetch(20 + k, (THERE, ACROSS), (THERE, CORNER), k, to_c) for k in range(hb)]
    c_0 = [fetch(24 + k, (HERE, SELF), (HERE, CORE), k, to_c) for k in range(hb)]
    y_a, y_b, y_c, y_d = y
    x_a, x_b, x_c, x_d = x
    dx_a, dx_b, dx_c, dx_d = dx
    c_y_a, c_y_b, c_y_c, c_y_d = c_y
    c_x_a, c_x_b, c_x_c, c_x_d = c_x
    c_d_a, c_d_b, c_d_c, c_d_d = c_d
    c_0_a, c_0_b, c_0_c, c_0_d = c_0
    fetches = y + x + dx + c_y + c_x + c_d + c_0
    first, second = (0, hb // 2), (hb // 2, hb)

    def begin(*copies):
        for copy in copies:
            copy.start()

    def arrived(*copies):
        for copy in copies:
            copy.wait_recv()

    kv_send = [remote(kvp_ref.at[m], (kc, vc)[m].at[1, mine_at], ksend.at[m], krecv.at[m], to_y) for m in range(2)]

    greet([target(i, j) for i, j in away])
    hid_a.start()
    u_copy.start()
    sends[0].start()
    for load in loads:
        load.start()

    def fill_bias(src, l, base):
        row = lax.broadcasted_iota(jnp.int32, (seq, seq), 0)
        col = lax.broadcasted_iota(jnp.int32, (seq, seq), 1)
        lines = jnp.dot(src[:, l, :], bucket_hot(src.shape[2], seq), precision=lax.Precision.HIGHEST, preferred_element_type=F32)
        for h in range(HEADS):
            line = jnp.broadcast_to(lines[h:h + 1, :], (seq, seq))
            toeplitz = pltpu.roll(line, 0, 1, stride=1, stride_axis=0)
            bias[base + h] = jnp.where(col <= row, toeplitz, -jnp.inf)

    def normed(rows, scale):
        wide = rows.astype(F32)
        inv = lax.rsqrt(jnp.mean(wide * wide, axis=-1, keepdims=True) + EPSILON)
        return (wide * inv * scale).astype(BF16)

    def heads_pass(l, side, lo, hi):
        def body(s, carry):
            a = normed(x_ref[s], lna[l:l + 1, :])
            for m in range(3):
                w = own_qkv[m, l] if side == 0 else peer_qkv[l, m]
                part = jnp.dot(a, w, preferred_element_type=F32).astype(BF16)
                qkv[:, m * width:(m + 1) * width] = part
                if m > 0:
                    if side == 0:
                        kvt[l, m - 1, s] = part.T
                    elif l == 1:
                        kvp_ref[m - 1, s] = part.T
            attend_rows(qkv, bias, side * HEADS, o_all, side, s)
            return carry
        lax.fori_loop(lo, hi, body, 0)

    def project_out(l, lo, hi):
        def body(s, carry):
            out = jnp.dot(o_all[0, s], own_o[l], preferred_element_type=F32)
            out = out + jnp.dot(o_all[1, s], peer_o[l], preferred_element_type=F32)
            x_ref[s] = (x_ref[s].astype(F32) + out).astype(BF16)
            return carry
        lax.fori_loop(lo, hi, body, 0)

    def ffn_chunk(gate, up, down, first):
        def body(r, carry):
            at = pl.ds(pl.multiple_of(r * FC, FC), FC)
            b = b_all[at, :]
            g = jnp.dot(b, gate[...], preferred_element_type=F32)
            u = jnp.dot(b, up[...], preferred_element_type=F32)
            hidden = (jax.nn.gelu(g) * u).astype(BF16)
            out = jnp.dot(hidden, down[...], preferred_element_type=F32)
            acc[at, :] = out if first else acc[at, :] + out
            return carry
        lax.fori_loop(0, 2, body, 0)

    def ffn_own(c):
        at = pl.ds(c * FC, FC)
        ffn_chunk(own_g.at[:, at], own_u.at[:, at], pool.at[at, :], c == 0)

    def ffn_peer(c):
        ffn_chunk(peer_g.at[c], peer_u.at[c], pool.at[pl.ds(ff + c * FC, FC), :], False)

    slot_iota = lax.broadcasted_iota(jnp.int32, (local_slots, 2 * half), 0)

    def pick(i, j, part):
        lo, _ = part
        ref = piece(i, j)
        off = pl.multiple_of(tps[i] * (hb * half) + lo * half, 2 * half)

        def body(p, carry):
            h = ref[lo:lo + 2, pl.ds(pl.multiple_of(p * half, half), half), :].reshape(2 * half, d_model)
            b = normed(h, lnf[1:2, :])
            g = p * 4 + eps[j]
            loc = slots_all[g, :, pl.ds(off, 2 * half)] - me * local_slots
            match = (slot_iota == loc[0:1, :]) | (slot_iota == loc[1:2, :])
            select = jnp.where(match, 1.0, 0.0).astype(BF16)
            got = jnp.dot(select, b, preferred_element_type=F32).astype(BF16)
            for e in range(n_exp):
                at = pl.ds(pl.multiple_of(e * local_slots + g * capacity, capacity), capacity)
                pool[at, :] = pool[at, :] + got[e * capacity:(e + 1) * capacity, :]
            return carry
        lax.fori_loop(0, 2, body, 0)

    w0 = [('w', 0, m) for m in range(3)]
    w1 = [('w', 1, m) for m in range(3)]
    w1_a, w1_b, w1_c = w1
    o0, o1 = ('o', 0, 0), ('o', 1, 0)
    g = [('g', c, 0) for c in range(3)]
    u = [('u', c, 0) for c in range(3)]
    d = [('d', c, 0) for c in range(3)]
    g_a, g_b, g_c = g
    u_a, u_b, u_c = u
    d_a, d_b, d_c = d

    for k in range(ids.shape[0]):
        ids_row[:, k * half:(k + 1) * half] = ids[k]
    experts = lax.broadcasted_iota(jnp.int32, (64, tokens), 0)
    hot = [experts == ids_row[c:c + 1, :] for c in range(2)]
    ones = [jnp.where(h, 1.0, 0.0) for h in hot]
    earlier = jnp.where(lax.broadcasted_iota(jnp.int32, (tokens, tokens), 0)
                        < lax.broadcasted_iota(jnp.int32, (tokens, tokens), 1), 1.0, 0.0).astype(BF16)
    before = [jnp.dot(o.astype(BF16), earlier, preferred_element_type=F32) for o in ones]
    before[1] = before[1] + jnp.sum(ones[0], axis=1, keepdims=True)
    for c in range(2):
        pos = jnp.sum(jnp.where(hot[c], before[c], 0.0), axis=0, keepdims=True).astype(jnp.int32)
        slots_all[me, c:c + 1, :] = jnp.where(pos < capacity, ids_row[c:c + 1, :] * capacity + pos, -1)
    slot_sends = [remote(slots_all.at[me], slots_all.at[me], ssend.at[4 * i + j], srecv.at[4 * i + j], target(i, j))
                  for i, j in away]
    for copy in slot_sends:
        copy.start()
    for c in range(2):
        slot = slots_all[me, c:c + 1, :]
        expert = lax.shift_right_arithmetic(slot, 6)
        key = lax.bitwise_and(expert, 7) * local_slots + lax.shift_right_arithmetic(expert, 3) * capacity + lax.bitwise_and(slot, 63)
        key = jnp.where(slot < 0, -1, key).astype(F32)
        aux[:, c * 8:(c + 1) * 8] = jnp.broadcast_to(key, (8, tokens)).T
        aux[:, 16 + c * 8:24 + c * 8] = jnp.broadcast_to(ids_row[c:c + 1, :].astype(F32), (8, tokens)).T

    fill_bias(table_own, 0, 0)
    u_copy.wait_recv()
    fill_bias(table_peer, 0, HEADS)
    loads[0].wait()
    hid_a.wait_recv()
    for copy in sends[1:WINDOW]:
        copy.start()
    for load in loads[1:4]:
        load.wait()
    heads_pass(0, 0, 0, hb)
    pass_on(*w0, o0)
    pass_core(*w0)
    pass_on(g_a)
    pass_core(o0)
    complete(*w0, o0)
    pass_on(u_a)
    heads_pass(0, 1, 0, hb // 2)
    pass_on(d_a)
    pass_core(g_a)
    heads_pass(0, 1, hb // 2, hb)
    pass_core(u_a)
    pass_on(g_b)
    loads[4].wait()
    project_out(0, 0, hb)

    def norm_rows(s, carry):
        b_all[pl.ds(pl.multiple_of(s * seq, seq), seq), :] = normed(x_ref[s], lnf[0:1, :])
        return carry
    lax.fori_loop(0, hb, norm_rows, 0)
    for load in loads[5:8]:
        load.wait()
    ffn_own(0)
    pass_on(u_b)
    pass_core(d_a)
    ffn_own(1)
    pass_core(g_b)
    pass_on(d_b)
    pass_core(u_b)
    ffn_own(2)
    pass_on(g_c)
    complete(g_a, u_a, d_a)
    ffn_peer(0)
    pass_core(d_b, g_c)
    pass_on(u_c)
    complete(g_b, u_b, d_b)
    ffn_peer(1)
    fill_bias(table_own, 1, 0)
    pass_on(d_c)
    pass_core(u_c)
    fill_bias(table_peer, 1, HEADS)
    pass_on(w1_a)
    pass_core(d_c)
    complete(g_c, u_c, d_c)
    ffn_peer(2)

    def add_rows(s, carry):
        x_ref[s] = (x_ref[s].astype(F32) + acc[pl.ds(pl.multiple_of(s * seq, seq), seq), :]).astype(BF16)
        return carry
    lax.fori_loop(0, hb, add_rows, 0)

    pass_on(w1_b, w1_c)
    pass_core(w1_a)
    heads_pass(1, 0, 0, hb // 2)
    pass_on(o1)
    pass_core(w1_b, w1_c)
    heads_pass(1, 0, hb // 2, hb)
    pass_core(o1)
    complete(*w1, o1)
    for item in d:
        x_copy(item).wait_send()
        c_copy(item).wait_send()
        d_copy(item).wait_send()
    stores = [pltpu.make_async_copy(kvt.at[l, m], (kc, vc)[m].at[l, mine_at], osem.at[2 * l + m])
              for l in range(2) for m in range(2)]
    begin(*stores)
    heads_pass(1, 1, 0, hb // 2)
    project_out(1, 0, hb // 2)
    begin(y_a, x_a, y_b, x_b, c_0_a, c_0_b)
    heads_pass(1, 1, hb // 2, hb)
    project_out(1, hb // 2, hb)
    begin(c_0_c, c_0_d)

    pool[...] = jnp.zeros_like(pool)
    for copy in slot_sends:
        copy.wait_recv()
    pick(HERE, SELF, first)
    pick(HERE, SELF, second)
    loads[8].wait()
    hid_b.wait_recv()
    stores[0].wait()
    stores[1].wait()

    def other_rows(s, carry):
        a = normed(other[s], lna[0:1, :])
        for m in range(2):
            kvt[0, m, s] = jnp.dot(a, own_qkv[m + 1, 0], preferred_element_type=F32).astype(BF16).T
        return carry
    lax.fori_loop(0, hb, other_rows, 0)
    more = [pltpu.make_async_copy(kvt.at[0, m], (kc, vc)[m].at[0, peer_at], osem.at[4 + m]) for m in range(2)]
    begin(*more)

    arrived(*c_0)
    pick(HERE, CORE, first)
    pick(HERE, CORE, second)
    arrived(x_a)
    begin(x_c, c_x_a)
    arrived(x_b)
    begin(x_d, c_x_b)
    arrived(y_a)
    begin(y_c, dx_a, c_y_a)
    arrived(y_b)
    begin(y_d, dx_b, c_y_b)
    pick(HERE, ACROSS, first)
    pick(THERE, SELF, first)
    arrived(c_x_a, c_x_b)
    pick(HERE, CORNER, first)
    arrived(c_y_a, c_y_b)
    pick(THERE, CORE, first)
    arrived(y_c)
    begin(dx_c, kv_send[0], c_y_c)
    arrived(y_d)
    begin(dx_d, kv_send[1], c_y_d)
    pick(THERE, SELF, second)
    arrived(c_y_c, c_y_d)
    pick(THERE, CORE, second)

    pos_at = pl.ds(pl.multiple_of(tp * half, half), half)
    for i in range(2):
        at = pl.ds(pl.multiple_of(tps[i] * (hb * half), hb * half), hb * half)
        h = piece(i, 0)[:, pos_at, :].reshape(hb * half, d_model)
        own_h[at, :] = h
        logits = lax.dot_general(normed(h, lnf[1:2, :]).astype(F32), w_router[...], (((1,), (1,)), ((), ())),
                                 precision=lax.Precision.HIGHEST, preferred_element_type=F32)
        ex = jnp.exp(logits - jnp.max(logits, axis=1, keepdims=True))
        probs = ex / jnp.sum(ex, axis=1, keepdims=True)
        lanes = lax.broadcasted_iota(jnp.int32, probs.shape, 1).astype(F32)
        picked = [jnp.sum(jnp.where(lanes == aux[at, 16 + c * 8:17 + c * 8], probs, 0.0), axis=1, keepdims=True) for c in range(2)]
        denom = picked[0] + picked[1]
        for c in range(2):
            aux[at, 32 + c:33 + c] = picked[c] / denom

    arrived(x_c)
    begin(c_x_c)
    arrived(x_d)
    begin(c_x_d)
    pick(HERE, ACROSS, second)
    arrived(c_x_c, c_x_d)
    pick(HERE, CORNER, second)
    arrived(dx_a)
    begin(c_d_a)
    arrived(dx_b)
    begin(c_d_b)
    pick(THERE, ACROSS, first)
    arrived(c_d_a, c_d_b)
    pick(THERE, CORNER, first)
    arrived(dx_c)
    begin(c_d_c)
    arrived(dx_d)
    begin(c_d_d)
    pick(THERE, ACROSS, second)
    arrived(c_d_c, c_d_d)
    pick(THERE, CORNER, second)

    out = [pltpu.make_async_copy(pool.at[e * local_slots:(e + 1) * local_slots], rows_out.at[e], lsem.at[e]) for e in range(n_exp)]
    begin(*out)
    for copy in out + stores[2:] + more:
        copy.wait()
    for copy in [hid_a, hid_b, u_copy] + fetches + slot_sends:
        copy.wait_send()
    for copy in kv_send:
        copy.wait()
    for item in items:
        y_copy(item).wait_send()
        if item not in d:
            x_copy(item).wait_send()
            c_copy(item).wait_send()
            d_copy(item).wait_send()


def dense_layers(hid, lna, lnf, wq, wk, wv, wo, wg, wu, wd, bias_table, ids, w_router):
    nb, npos, d_model = hid.shape
    hb, seq = nb // 2, 2 * npos
    tokens = nb * npos
    width = HEADS * 64
    ff = wg.shape[1]
    any_spec = pl.BlockSpec(memory_space=pl.ANY)
    vmem = pl.BlockSpec(memory_space=pltpu.VMEM)
    n_items = 17
    dma = pltpu.SemaphoreType.DMA
    slots = LOCAL_EXPERTS * CAPACITY
    return pl.pallas_call(
        dense_kernel,
        in_specs=[any_spec, vmem, vmem] + [any_spec] * 7 + [vmem] * 3,
        out_specs=[any_spec, vmem, vmem, any_spec, any_spec],
        out_shape=[jax.ShapeDtypeStruct((LOCAL_EXPERTS, slots, d_model), BF16),
                   jax.ShapeDtypeStruct((tokens, 128), F32),
                   jax.ShapeDtypeStruct((tokens, d_model), BF16),
                   jax.ShapeDtypeStruct((2, nb, width, seq), BF16),
                   jax.ShapeDtypeStruct((2, nb, width, seq), BF16)],
        scratch_shapes=[
            pltpu.VMEM((3, 2, d_model, width), BF16), pltpu.VMEM((2, width, d_model), BF16),
            pltpu.VMEM((d_model, ff), BF16), pltpu.VMEM((d_model, ff), BF16),
            pltpu.VMEM((2, 3, d_model, width), BF16), pltpu.VMEM((2, width, d_model), BF16),
            pltpu.VMEM((3, d_model, FC), BF16), pltpu.VMEM((3, d_model, FC), BF16),
            pltpu.VMEM((LOCAL_EXPERTS * slots, d_model), BF16),
            pltpu.VMEM(bias_table.shape, F32), pltpu.VMEM((2 * HEADS, seq, seq), F32),
            pltpu.VMEM((seq, 3 * width), BF16), pltpu.VMEM((2, hb, seq, width), BF16),
            pltpu.VMEM((hb * seq, d_model), BF16), pltpu.VMEM((hb * seq, d_model), F32),
            pltpu.VMEM((2, 2, hb, width, seq), BF16), pltpu.VMEM((hb, seq, d_model), BF16),
            pltpu.VMEM((hb, seq, d_model), BF16), pltpu.VMEM((2, hb, width, seq), BF16),
            pltpu.VMEM((7, hb, seq, d_model), BF16), pltpu.VMEM((8, 2, tokens), jnp.int32), pltpu.VMEM((2, tokens), jnp.int32),
        ] + [dma((n_items,))] * 8 + [dma((3,)), dma((3,)), dma((9,)), dma((6,)),
                                     dma((28,)), dma((28,)), dma((8,)), dma((8,)), dma((2,)), dma((2,))],
        compiler_params=pltpu.CompilerParams(collective_id=0, has_side_effects=True, vmem_limit_bytes=65470 * 1024),
        name="dense_layers",
    )(hid, lna, lnf, wq, wk, wv, wo, wg, wu, wd, bias_table, ids, w_router)


def moe_kernel(rows_in, aux, own_h, w_in, w_out,
               out_ref,
               rows, res, ret, win, wout, acc, total,
               rsend, rrecv, wsem, isem):
    tp, ep, to_y, to_x, to_c = swap_targets()
    n_exp, local_slots, d_model = rows.shape
    capacity = local_slots // 8
    tokens = own_h.shape[0]
    chunk = win.shape[2]
    n_chunks = w_in.shape[2] // chunk
    eps = [ep, to_c['ep'], to_x['ep'], lax.rem(to_c['ep'] + 2, 4)]
    tps = [tp, 1 - tp]
    me = tp * 4 + ep
    away = [(i, j) for i in (1, 0) for j in (2, 3, 0, 1) if (i, j) != (0, 0)]

    def target(i, j):
        return {'tp': tps[i], 'ep': eps[j]}

    def remote(src, dst, send, recv, to):
        return pltpu.make_async_remote_copy(src_ref=src, dst_ref=dst, send_sem=send, recv_sem=recv,
                                            device_id=to, device_id_type=MESH)

    def weight_copies(e, c):
        at = pl.ds(c * chunk, chunk)
        return (pltpu.make_async_copy(w_in.at[e, :, at], win.at[c], wsem.at[0, c]),
                pltpu.make_async_copy(w_out.at[e, at, :], wout.at[c], wsem.at[1, c]))

    def row_copy(e):
        return pltpu.make_async_copy(rows_in.at[e], rows.at[e], isem.at[e])

    row_copy(0).start()
    for c in range(n_chunks):
        for copy in weight_copies(0, c):
            copy.start()
    for e in range(1, n_exp):
        row_copy(e).start()
    greet([target(i, j) for i, j in away])
    total[...] = jnp.zeros_like(total)

    def returns(e):
        return [remote(res.at[e, tps[i] * 4 + eps[j]], ret.at[e, me], rsend.at[4 * i + j, e], rrecv.at[4 * i + j, e], target(i, j))
                for i, j in away]

    def combine(e):
        for copy in returns(e):
            copy.wait_recv()
        block = 256
        columns = lax.broadcasted_iota(jnp.int32, (block, local_slots), 1).astype(F32)
        table = ret[e].reshape(local_slots, d_model)

        def body(r, carry):
            at = pl.ds(pl.multiple_of(r * block, block), block)
            add = total[at, :]
            for c in range(2):
                want = aux[at, c * 8:c * 8 + 1] - (e * local_slots).astype(F32)
                select = jnp.where(columns == want, 1.0, 0.0).astype(BF16)
                add = add + aux[at, 32 + c:33 + c] * jnp.dot(select, table, preferred_element_type=F32)
            total[at, :] = add
            return carry
        lax.fori_loop(0, tokens // block, body, 0)

    lag = 3

    def expert(e, carry):
        row_copy(e).wait()
        table = rows[e]
        for c in range(n_chunks):
            for copy in weight_copies(e, c):
                copy.wait()
            up = jnp.dot(table, win[c], preferred_element_type=F32)
            out = jnp.dot(jax.nn.gelu(up).astype(BF16), wout[c], preferred_element_type=F32)
            if c == 0:
                acc[...] = out
            elif c < n_chunks - 1:
                acc[...] = acc[...] + out
            else:
                res[e] = (acc[...] + out).astype(BF16).reshape(8, capacity, d_model)

            @pl.when(e < n_exp - 1)
            def _():
                for copy in weight_copies(e + 1, c):
                    copy.start()
        for copy in returns(e):
            copy.start()
        ret[e, me] = res[e, me]

        @pl.when(e >= lag)
        def _():
            combine(e - lag)
        return carry
    lax.fori_loop(0, n_exp, expert, 0)

    def last(e, carry):
        combine(e)
        return carry
    lax.fori_loop(n_exp - lag, n_exp, last, 0)
    out_ref[...] = (own_h[...].astype(F32) + total[...]).astype(BF16).reshape(out_ref.shape)


    def drain(e, carry):
        for copy in returns(e):
            copy.wait_send()
        return carry
    lax.fori_loop(0, n_exp, drain, 0)


def moe_layer(rows, aux, own_h, w_in, w_out, out_shape):
    n_exp, slots, d_model = rows.shape
    tokens = own_h.shape[0]
    ff = w_in.shape[2]
    capacity = slots // 8
    chunk = 768
    n_chunks = ff // chunk
    vmem = pl.BlockSpec(memory_space=pltpu.VMEM)
    any_spec = pl.BlockSpec(memory_space=pl.ANY)
    dma = pltpu.SemaphoreType.DMA
    slot_rows = pltpu.VMEM((n_exp, 8, capacity, d_model), BF16)
    return pl.pallas_call(
        moe_kernel,
        in_specs=[any_spec, vmem, vmem] + [any_spec] * 2,
        out_specs=vmem,
        out_shape=jax.ShapeDtypeStruct(out_shape, BF16),
        scratch_shapes=[
            pltpu.VMEM((n_exp, slots, d_model), BF16), slot_rows, slot_rows,
            pltpu.VMEM((n_chunks, d_model, chunk), BF16), pltpu.VMEM((n_chunks, chunk, d_model), BF16),
            pltpu.VMEM((slots, d_model), F32), pltpu.VMEM((tokens, d_model), F32),
            dma((8, n_exp)), dma((8, n_exp)), dma((2, n_chunks)), dma((n_exp,)),
        ],
        compiler_params=pltpu.CompilerParams(collective_id=1, has_side_effects=True, vmem_limit_bytes=62 * 1024 * 1024),
        name="moe_layer",
    )(rows, aux, own_h, w_in, w_out)


def solution(mesh):
    act_spec = P(('dp', 'ep'), 'tp', None)
    col_spec = P(None, None, 'tp')
    row_spec = P(None, 'tp', None)
    expert_spec = P(('tp', 'ep'), None, None)
    cache_spec = P(None, ('dp', 'ep'), 'tp', None, None)
    in_specs = (act_spec, P(), P(), col_spec, col_spec, col_spec, row_spec, row_spec,
                P(None, 'tp'), P(None, 'tp'), P('tp', None), P(), expert_spec, expert_spec, act_spec)

    def device_fn(hidden_in, ln_attn, ln_ffn, w_query, w_key, w_value, w_out, bias_table, w_gate, w_up, w_down, w_router, expert_in, expert_out, expert_ids):
        nb, npos, d_model = hidden_in.shape
        rows, aux, own_h, k_all, v_all = dense_layers(
            hidden_in, ln_attn, ln_ffn, w_query, w_key, w_value, w_out, w_gate, w_up, w_down,
            jnp.swapaxes(bias_table, 0, 1), jnp.swapaxes(expert_ids, 1, 2), w_router.T)
        hidden = moe_layer(rows, aux, own_h, expert_in, expert_out, hidden_in.shape)
        caches = [jnp.swapaxes(full.reshape(2, nb, -1, 64, 2 * npos), 3, 4) for full in (k_all, v_all)]
        return hidden, caches[0], caches[1]

    return jax.shard_map(device_fn, mesh=mesh, in_specs=in_specs, out_specs=(act_spec, cache_spec, cache_spec), check_vma=False)
```

```python
import jax
import jax.numpy as jnp
from jax import lax
from jax.experimental import pallas as pl
from jax.experimental.pallas import tpu as pltpu
from jax.sharding import PartitionSpec as P

EXACT_BUCKETS = 16
THRESHOLDS = (18, 20, 23, 26, 30, 34, 39, 45, 51, 58, 66, 76, 86, 98, 112)
EPSILON = 1e-6
BF16 = jnp.bfloat16
F32 = jnp.float32

def bucket_hot(buckets, seq_len):
    k = lax.broadcasted_iota(jnp.int32, (buckets, seq_len), 1)
    rel = jnp.where(k == 0, 0, seq_len - k)
    bucket = jnp.minimum(rel, EXACT_BUCKETS)
    for threshold in THRESHOLDS:
        bucket = bucket + jnp.where(rel >= threshold, 1, 0)
    return jnp.where(bucket == lax.broadcasted_iota(jnp.int32, (buckets, seq_len), 0), 1.0, 0.0)


MESH = pl.DeviceIdType.MESH
HEADS = 6
NQ = 192
NO = 96
NF = 128
FC = 512
WINDOW = 5
HERE, THERE = range(2)
SELF, CORE, ACROSS, CORNER = range(4)
LOCAL_EXPERTS = 8
CAPACITY = 64


def swap_targets():
    tp = lax.axis_index('tp')
    ep = lax.axis_index('ep')
    core = ep + 1 - 2 * lax.rem(ep, 2)
    across = lax.rem(ep + 2, 4)
    return tp, ep, {'tp': 1 - tp}, {'ep': across}, {'ep': core}


def greet(targets):
    barrier = pltpu.get_barrier_semaphore()
    for target in targets:
        pl.semaphore_signal(barrier, inc=1, device_id=target, device_id_type=MESH)
    pl.semaphore_wait(barrier, len(targets))


def attend_rows(qkv_ref, bias_ref, base, o_ref, side, s):
    width = HEADS * 64
    rows = 128
    lane = lax.broadcasted_iota(jnp.int32, (rows, 128), 1)
    units = [(pair, blk, sd) for pair in range(HEADS // 2) for blk in range(2) for sd in range(2)]
    scores = []
    for pair, blk, sd in units:
        lo = pair * 128
        keys = rows * (blk + 1)
        q = qkv_ref[blk * rows:(blk + 1) * rows, lo:lo + 128]
        k = qkv_ref[0:keys, width + lo:width + lo + 128]
        mine = (lane < 64) if sd == 0 else (lane >= 64)
        qh = jnp.where(mine, q, jnp.zeros_like(q))
        sc = lax.dot_general(qh, k, (((1,), (1,)), ((), ())), preferred_element_type=F32)
        scores.append(sc * 0.125 + bias_ref[base + 2 * pair + sd, blk * rows:(blk + 1) * rows, 0:keys])
    tops = [jnp.max(sc, axis=1, keepdims=True) for sc in scores]
    exps = [jnp.exp(sc - m) for sc, m in zip(scores, tops)]
    sums = [jnp.sum(p, axis=1, keepdims=True) for p in exps]
    probs = [(p * (1.0 / l)).astype(BF16) for p, l in zip(exps, sums)]
    outs = []
    for (pair, blk, sd), p in zip(units, probs):
        lo = pair * 128
        v = qkv_ref[0:rows * (blk + 1), 2 * width + lo:2 * width + lo + 128]
        outs.append(jnp.dot(p, v, preferred_element_type=F32))
    for i in range(0, len(units), 2):
        pair, blk, _ = units[i]
        o_ref[side, s, blk * rows:(blk + 1) * rows, pair * 128:pair * 128 + 128] = jnp.where(
            lane < 64, outs[i], outs[i + 1]).astype(BF16)


def dense_kernel(hid, lna, lnf, wq, wk, wv, wo, wg, wu, wd, table_own, ids, w_router,
                 rows_out, aux, own_h, kc, vc,
                 own_qkv, own_o, own_g, own_u, peer_qkv, peer_o, peer_g, peer_u, pool,
                 table_peer, bias, qkv, o_all, b_all, acc, kvt, other, kvp_ref, h_all, slots_all, ids_row,
                 ysend, yrecv, xsend, xrecv, csend, crecv, dsend, drecv, hsend, hrecv, lsem, osem,
                 asend, arecv, ssend, srecv, ksend, krecv):
    tp, ep, to_y, to_x, to_c = swap_targets()
    eps = [ep, to_c['ep'], to_x['ep'], lax.rem(to_c['ep'] + 2, 4)]
    tps = [tp, 1 - tp]
    me = tp * 4 + ep
    away = [(i, j) for i in (1, 0) for j in (2, 3, 0, 1) if (i, j) != (0, 0)]
    n_exp, capacity = LOCAL_EXPERTS, CAPACITY
    local_slots = n_exp * capacity

    def target(i, j):
        return {'tp': tps[i], 'ep': eps[j]}

    across = lax.rem(ep + 2, 4)
    x_ref = h_all.at[0]
    _, hb, seq, d_model = h_all.shape
    half = seq // 2
    tokens = hb * seq
    width = HEADS * 64
    ff = wd.shape[0]

    attn = [[('w', l, m) for m in range(3)] + [('o', l, 0)] for l in range(2)]
    ffn = [[(kind, c, 0) for kind in ('g', 'u', 'd')] for c in range(3)]
    items = attn[0] + ffn[0] + ffn[1] + ffn[2] + attn[1]
    index = {item: i for i, item in enumerate(items)}

    def source(item):
        kind, l, m = item
        if kind == 'w':
            return (wq, wk, wv)[m].at[l, pl.ds(pl.multiple_of(ep * NQ, NQ), NQ), :]
        if kind == 'o':
            return wo.at[l, pl.ds(pl.multiple_of(ep * NO, NO), NO), :]
        at = pl.multiple_of(ep * (3 * NF) + l * NF, NF)
        if kind == 'd':
            return wd.at[pl.ds(at, NF), :]
        return (wg if kind == 'g' else wu).at[:, pl.ds(at, NF)]

    def place(item, r):
        kind, l, m = item
        if kind == 'w':
            return peer_qkv.at[l, m, pl.ds(pl.multiple_of(r * NQ, NQ), NQ), :]
        if kind == 'o':
            return peer_o.at[l, pl.ds(pl.multiple_of(r * NO, NO), NO), :]
        at = pl.multiple_of(r * NF, NF)
        if kind == 'd':
            return pool.at[pl.ds(pl.multiple_of(ff + l * FC + at, NF), NF), :]
        return (peer_g if kind == 'g' else peer_u).at[l, :, pl.ds(at, NF)]

    def remote(src, dst, send, recv, target):
        return pltpu.make_async_remote_copy(src_ref=src, dst_ref=dst, send_sem=send, recv_sem=recv,
                                            device_id=target, device_id_type=MESH)

    def y_copy(item):
        i = index[item]
        return remote(source(item), place(item, ep), ysend.at[i], yrecv.at[i], to_y)

    def x_copy(item):
        i = index[item]
        return remote(place(item, ep), place(item, ep), xsend.at[i], xrecv.at[i], to_x)

    def c_copy(item):
        i = index[item]
        return remote(place(item, ep), place(item, ep), csend.at[i], crecv.at[i], to_c)

    def d_copy(item):
        i = index[item]
        return remote(place(item, across), place(item, across), dsend.at[i], drecv.at[i], to_c)

    def pass_on(*names):
        for item in names:
            y_copy(item).wait_recv()
            if index[item] + WINDOW < len(sends):
                sends[index[item] + WINDOW].start()
            x_copy(item).start()
            c_copy(item).start()

    def pass_core(*names):
        for item in names:
            x_copy(item).wait_recv()
            d_copy(item).start()

    def complete(*names):
        for item in names:
            c_copy(item).wait_recv()
            d_copy(item).wait_recv()

    mine_at = pl.ds(tp * hb, hb)
    peer_at = pl.ds((1 - tp) * hb, hb)
    rows_at = pl.ds(pl.multiple_of(tp * half, half), half)
    hid_a = remote(hid.at[peer_at], x_ref.at[:, rows_at, :], hsend.at[0], hrecv.at[0], to_y)
    hid_b = remote(hid.at[mine_at], other.at[:, rows_at, :], hsend.at[1], hrecv.at[1], to_y)
    sends = [y_copy(item) for item in items] + [hid_b]
    u_copy = remote(table_own, table_peer, hsend.at[2], hrecv.at[2], to_y)
    loads = [pltpu.make_async_copy(s, d, lsem.at[i]) for i, (s, d) in enumerate([
        (hid.at[mine_at], x_ref.at[:, rows_at, :]),
        (wq, own_qkv.at[0]), (wk, own_qkv.at[1]), (wv, own_qkv.at[2]), (wo, own_o),
        (wg, own_g), (wu, own_u), (wd, pool.at[0:ff]),
        (hid.at[peer_at], other.at[:, rows_at, :])])]

    def piece(i, j):
        return h_all.at[4 * i + j]

    def fetch(n_sem, src, dst, k, to):
        return remote(piece(*src).at[k], piece(*dst).at[k], asend.at[n_sem], arecv.at[n_sem], to)

    y = [fetch(k, (HERE, SELF), (THERE, SELF), k, to_y) for k in range(hb)]
    x = [fetch(4 + k, (HERE, SELF), (HERE, ACROSS), k, to_x) for k in range(hb)]
    dx = [fetch(8 + k, (THERE, SELF), (THERE, ACROSS), k, to_x) for k in range(hb)]
    c_y = [fetch(12 + k, (THERE, SELF), (THERE, CORE), k, to_c) for k in range(hb)]
    c_x = [fetch(16 + k, (HERE, ACROSS), (HERE, CORNER), k, to_c) for k in range(hb)]
    c_d = [fetch(20 + k, (THERE, ACROSS), (THERE, CORNER), k, to_c) for k in range(hb)]
    c_0 = [fetch(24 + k, (HERE, SELF), (HERE, CORE), k, to_c) for k in range(hb)]
    y_a, y_b, y_c, y_d = y
    x_a, x_b, x_c, x_d = x
    dx_a, dx_b, dx_c, dx_d = dx
    c_y_a, c_y_b, c_y_c, c_y_d = c_y
    c_x_a, c_x_b, c_x_c, c_x_d = c_x
    c_d_a, c_d_b, c_d_c, c_d_d = c_d
    c_0_a, c_0_b, c_0_c, c_0_d = c_0
    fetches = y + x + dx + c_y + c_x + c_d + c_0
    first, second = (0, hb // 2), (hb // 2, hb)

    def begin(*copies):
        for copy in copies:
            copy.start()

    def arrived(*copies):
        for copy in copies:
            copy.wait_recv()

    kv_send = [remote(kvp_ref.at[m], (kc, vc)[m].at[1, mine_at], ksend.at[m], krecv.at[m], to_y) for m in range(2)]

    greet([target(i, j) for i, j in away])
    hid_a.start()
    u_copy.start()
    sends[0].start()
    for load in loads:
        load.start()

    def fill_bias(src, l, base):
        row = lax.broadcasted_iota(jnp.int32, (seq, seq), 0)
        col = lax.broadcasted_iota(jnp.int32, (seq, seq), 1)
        lines = jnp.dot(src[:, l, :], bucket_hot(src.shape[2], seq), precision=lax.Precision.HIGHEST, preferred_element_type=F32)
        for h in range(HEADS):
            line = jnp.broadcast_to(lines[h:h + 1, :], (seq, seq))
            toeplitz = pltpu.roll(line, 0, 1, stride=1, stride_axis=0)
            bias[base + h] = jnp.where(col <= row, toeplitz, -jnp.inf)

    def normed(rows, scale):
        wide = rows.astype(F32)
        inv = lax.rsqrt(jnp.mean(wide * wide, axis=-1, keepdims=True) + EPSILON)
        return (wide * inv * scale).astype(BF16)

    def heads_pass(l, side, midway=None):
        def body(s, carry):
            if midway is not None:
                pl.when(s == hb // 2)(midway)
            a = normed(x_ref[s], lna[l:l + 1, :])
            for m in range(3):
                w = own_qkv[m, l] if side == 0 else peer_qkv[l, m]
                part = jnp.dot(a, w, preferred_element_type=F32).astype(BF16)
                qkv[:, m * width:(m + 1) * width] = part
                if m > 0:
                    if side == 0:
                        kvt[l, m - 1, s] = part.T
                    elif l == 1:
                        kvp_ref[m - 1, s] = part.T
            attend_rows(qkv, bias, side * HEADS, o_all, side, s)
            if side == 1:
                out = jnp.dot(o_all[0, s], own_o[l], preferred_element_type=F32)
                out = out + jnp.dot(o_all[1, s], peer_o[l], preferred_element_type=F32)
                x_ref[s] = (x_ref[s].astype(F32) + out).astype(BF16)
            return carry
        lax.fori_loop(0, hb, body, 0)

    def ffn_chunk(gate, up, down):
        def body(r, carry):
            at = pl.ds(pl.multiple_of(r * FC, FC), FC)
            b = b_all[at, :]
            g = jnp.dot(b, gate[...], preferred_element_type=F32)
            u = jnp.dot(b, up[...], preferred_element_type=F32)
            hidden = (jax.nn.gelu(g) * u).astype(BF16)
            out = jnp.dot(hidden, down[...], preferred_element_type=F32)
            acc[at, :] = acc[at, :] + out
            return carry
        lax.fori_loop(0, 2, body, 0)

    def ffn_loop(own, steps):
        def body(c, carry):
            at = pl.ds(pl.multiple_of(c * FC, FC), FC)
            if own:
                ffn_chunk(own_g.at[:, at], own_u.at[:, at], pool.at[at, :])
            else:
                ffn_chunk(peer_g.at[c], peer_u.at[c], pool.at[pl.ds(pl.multiple_of(ff + c * FC, FC), FC), :])
            for k, step in enumerate(steps):
                pl.when(c == k)(step)
            return carry
        lax.fori_loop(0, ff // FC, body, 0)

    slot_iota = lax.broadcasted_iota(jnp.int32, (local_slots, 2 * half), 0)

    def pick(*units):
        start, end = units[0], units[-1]

        def blend(n, low, high):
            return low + n * (high - low)

        def body(step, carry):
            n, p = step // 2, lax.rem(step, 2)
            lo = blend(n, start[2][0], end[2][0])
            index_of = blend(n, 4 * start[0] + start[1], 4 * end[0] + end[1])
            tp_of = blend(n, tps[start[0]], tps[end[0]])
            ep_of = blend(n, eps[start[1]], eps[end[1]])
            h = h_all[index_of, pl.ds(lo, 2), pl.ds(pl.multiple_of(p * half, half), half), :].reshape(2 * half, d_model)
            b = normed(h, lnf[1:2, :])
            g = p * 4 + ep_of
            off = pl.multiple_of(tp_of * (hb * half) + lo * half, 2 * half)
            loc = slots_all[g, :, pl.ds(off, 2 * half)] - me * local_slots
            match = (slot_iota == loc[0:1, :]) | (slot_iota == loc[1:2, :])
            select = jnp.where(match, 1.0, 0.0).astype(BF16)
            got = jnp.dot(select, b, preferred_element_type=F32).astype(BF16)
            for e in range(n_exp):
                at = pl.ds(pl.multiple_of(e * local_slots + g * capacity, capacity), capacity)
                pool[at, :] = pool[at, :] + got[e * capacity:(e + 1) * capacity, :]
            return carry
        lax.fori_loop(0, 2 * len(units), body, 0)

    w0 = [('w', 0, m) for m in range(3)]
    w1 = [('w', 1, m) for m in range(3)]
    w1_a, w1_b, w1_c = w1
    o0, o1 = ('o', 0, 0), ('o', 1, 0)
    g = [('g', c, 0) for c in range(3)]
    u = [('u', c, 0) for c in range(3)]
    d = [('d', c, 0) for c in range(3)]
    g_a, g_b, g_c = g
    u_a, u_b, u_c = u
    d_a, d_b, d_c = d

    for k in range(ids.shape[0]):
        ids_row[:, k * half:(k + 1) * half] = ids[k]
    experts = lax.broadcasted_iota(jnp.int32, (64, tokens), 0)
    hot = [experts == ids_row[c:c + 1, :] for c in range(2)]
    ones = [jnp.where(h, 1.0, 0.0) for h in hot]
    earlier = jnp.where(lax.broadcasted_iota(jnp.int32, (tokens, tokens), 0)
                        < lax.broadcasted_iota(jnp.int32, (tokens, tokens), 1), 1.0, 0.0).astype(BF16)
    before = [jnp.dot(o.astype(BF16), earlier, preferred_element_type=F32) for o in ones]
    before[1] = before[1] + jnp.sum(ones[0], axis=1, keepdims=True)
    for c in range(2):
        pos = jnp.sum(jnp.where(hot[c], before[c], 0.0), axis=0, keepdims=True).astype(jnp.int32)
        slots_all[me, c:c + 1, :] = jnp.where(pos < capacity, ids_row[c:c + 1, :] * capacity + pos, -1)
    slot_sends = [remote(slots_all.at[me], slots_all.at[me], ssend.at[4 * i + j], srecv.at[4 * i + j], target(i, j))
                  for i, j in away]
    for copy in slot_sends:
        copy.start()
    for c in range(2):
        slot = slots_all[me, c:c + 1, :]
        expert = lax.shift_right_arithmetic(slot, 6)
        key = lax.bitwise_and(expert, 7) * local_slots + lax.shift_right_arithmetic(expert, 3) * capacity + lax.bitwise_and(slot, 63)
        key = jnp.where(slot < 0, -1, key).astype(F32)
        aux[:, c * 8:(c + 1) * 8] = jnp.broadcast_to(key, (8, tokens)).T
        aux[:, 16 + c * 8:24 + c * 8] = jnp.broadcast_to(ids_row[c:c + 1, :].astype(F32), (8, tokens)).T

    fill_bias(table_own, 0, 0)
    u_copy.wait_recv()
    fill_bias(table_peer, 0, HEADS)
    loads[0].wait()
    hid_a.wait_recv()
    for copy in sends[1:WINDOW]:
        copy.start()
    for load in loads[1:4]:
        load.wait()
    heads_pass(0, 0)
    pass_on(*w0, o0)
    pass_core(*w0)
    pass_on(g_a)
    pass_core(o0)
    complete(*w0, o0)
    pass_on(u_a)
    loads[4].wait()

    def midway():
        pass_on(d_a)
        pass_core(g_a)
    heads_pass(0, 1, midway)
    pass_core(u_a)
    pass_on(g_b)

    def norm_rows(s, carry):
        b_all[pl.ds(pl.multiple_of(s * seq, seq), seq), :] = normed(x_ref[s], lnf[0:1, :])
        return carry
    lax.fori_loop(0, hb, norm_rows, 0)
    for load in loads[5:8]:
        load.wait()
    acc[...] = jnp.zeros_like(acc)

    def own_a():
        pass_on(u_b)
        pass_core(d_a)

    def own_b():
        pass_core(g_b)
        pass_on(d_b)
        pass_core(u_b)

    def own_c():
        pass_on(g_c)
        complete(g_a, u_a, d_a)
    ffn_loop(True, [own_a, own_b, own_c])

    def peer_a():
        pass_core(d_b, g_c)
        pass_on(u_c)
        complete(g_b, u_b, d_b)

    def peer_b():
        fill_bias(table_own, 1, 0)
        pass_on(d_c)
        pass_core(u_c)
        fill_bias(table_peer, 1, HEADS)
        pass_on(w1_a)
        pass_core(d_c)
        complete(g_c, u_c, d_c)
    ffn_loop(False, [peer_a, peer_b])

    def add_rows(s, carry):
        x_ref[s] = (x_ref[s].astype(F32) + acc[pl.ds(pl.multiple_of(s * seq, seq), seq), :]).astype(BF16)
        return carry
    lax.fori_loop(0, hb, add_rows, 0)

    pass_on(w1_b, w1_c)
    pass_core(w1_a)

    def own_midway():
        pass_on(o1)
        pass_core(w1_b, w1_c)
    heads_pass(1, 0, own_midway)
    pass_core(o1)
    complete(*w1, o1)
    for item in d:
        x_copy(item).wait_send()
        c_copy(item).wait_send()
        d_copy(item).wait_send()
    stores = [pltpu.make_async_copy(kvt.at[l, m], (kc, vc)[m].at[l, mine_at], osem.at[2 * l + m])
              for l in range(2) for m in range(2)]
    begin(*stores)
    heads_pass(1, 1, lambda: begin(y_a, x_a, y_b, x_b, c_0_a, c_0_b))
    begin(c_0_c, c_0_d)

    pool[...] = jnp.zeros_like(pool)
    for copy in slot_sends:
        copy.wait_recv()
    pick((HERE, SELF, first), (HERE, SELF, second))
    loads[8].wait()
    hid_b.wait_recv()
    stores[0].wait()
    stores[1].wait()

    def other_rows(s, carry):
        a = normed(other[s], lna[0:1, :])
        for m in range(2):
            kvt[0, m, s] = jnp.dot(a, own_qkv[m + 1, 0], preferred_element_type=F32).astype(BF16).T
        return carry
    lax.fori_loop(0, hb, other_rows, 0)
    more = [pltpu.make_async_copy(kvt.at[0, m], (kc, vc)[m].at[0, peer_at], osem.at[4 + m]) for m in range(2)]
    begin(*more)

    arrived(*c_0)
    pick((HERE, CORE, first), (HERE, CORE, second))
    arrived(x_a)
    begin(x_c, c_x_a)
    arrived(x_b)
    begin(x_d, c_x_b)
    arrived(y_a)
    begin(y_c, dx_a, c_y_a)
    arrived(y_b)
    begin(y_d, dx_b, c_y_b)
    pick((HERE, ACROSS, first), (THERE, SELF, first))
    arrived(c_x_a, c_x_b, c_y_a, c_y_b)
    pick((HERE, CORNER, first), (THERE, CORE, first))
    arrived(y_c)
    begin(dx_c, kv_send[0], c_y_c)
    arrived(y_d)
    begin(dx_d, kv_send[1], c_y_d)
    arrived(c_y_c, c_y_d)
    pick((THERE, SELF, second), (THERE, CORE, second))

    pos_at = pl.ds(pl.multiple_of(tp * half, half), half)
    for i in range(2):
        at = pl.ds(pl.multiple_of(tps[i] * (hb * half), hb * half), hb * half)
        h = piece(i, 0)[:, pos_at, :].reshape(hb * half, d_model)
        own_h[at, :] = h
        logits = lax.dot_general(normed(h, lnf[1:2, :]).astype(F32), w_router[...], (((1,), (1,)), ((), ())),
                                 precision=lax.Precision.HIGHEST, preferred_element_type=F32)
        ex = jnp.exp(logits - jnp.max(logits, axis=1, keepdims=True))
        probs = ex / jnp.sum(ex, axis=1, keepdims=True)
        lanes = lax.broadcasted_iota(jnp.int32, probs.shape, 1).astype(F32)
        picked = [jnp.sum(jnp.where(lanes == aux[at, 16 + c * 8:17 + c * 8], probs, 0.0), axis=1, keepdims=True) for c in range(2)]
        denom = picked[0] + picked[1]
        for c in range(2):
            aux[at, 32 + c:33 + c] = picked[c] / denom

    arrived(x_c)
    begin(c_x_c)
    arrived(x_d)
    begin(c_x_d)
    arrived(c_x_c, c_x_d)
    pick((HERE, ACROSS, second), (HERE, CORNER, second))
    arrived(dx_a)
    begin(c_d_a)
    arrived(dx_b)
    begin(c_d_b)
    arrived(c_d_a, c_d_b)
    pick((THERE, ACROSS, first), (THERE, CORNER, first))
    arrived(dx_c)
    begin(c_d_c)
    arrived(dx_d)
    begin(c_d_d)
    pick((THERE, ACROSS, second))
    arrived(c_d_c, c_d_d)
    pick((THERE, CORNER, second))

    out = [pltpu.make_async_copy(pool.at[e * local_slots:(e + 1) * local_slots], rows_out.at[e], lsem.at[e]) for e in range(n_exp)]
    begin(*out)
    for copy in out + stores[2:] + more:
        copy.wait()
    for copy in [hid_a, hid_b, u_copy] + fetches + slot_sends:
        copy.wait_send()
    for copy in kv_send:
        copy.wait()
    for item in items:
        y_copy(item).wait_send()
        if item not in d:
            x_copy(item).wait_send()
            c_copy(item).wait_send()
            d_copy(item).wait_send()


def dense_layers(hid, lna, lnf, wq, wk, wv, wo, wg, wu, wd, bias_table, ids, w_router):
    nb, npos, d_model = hid.shape
    hb, seq = nb // 2, 2 * npos
    tokens = nb * npos
    width = HEADS * 64
    ff = wg.shape[1]
    any_spec = pl.BlockSpec(memory_space=pl.ANY)
    vmem = pl.BlockSpec(memory_space=pltpu.VMEM)
    n_items = 17
    dma = pltpu.SemaphoreType.DMA
    slots = LOCAL_EXPERTS * CAPACITY
    return pl.pallas_call(
        dense_kernel,
        in_specs=[any_spec, vmem, vmem] + [any_spec] * 7 + [vmem] * 3,
        out_specs=[any_spec, vmem, vmem, any_spec, any_spec],
        out_shape=[jax.ShapeDtypeStruct((LOCAL_EXPERTS, slots, d_model), BF16),
                   jax.ShapeDtypeStruct((tokens, 128), F32),
                   jax.ShapeDtypeStruct((tokens, d_model), BF16),
                   jax.ShapeDtypeStruct((2, nb, width, seq), BF16),
                   jax.ShapeDtypeStruct((2, nb, width, seq), BF16)],
        scratch_shapes=[
            pltpu.VMEM((3, 2, d_model, width), BF16), pltpu.VMEM((2, width, d_model), BF16),
            pltpu.VMEM((d_model, ff), BF16), pltpu.VMEM((d_model, ff), BF16),
            pltpu.VMEM((2, 3, d_model, width), BF16), pltpu.VMEM((2, width, d_model), BF16),
            pltpu.VMEM((3, d_model, FC), BF16), pltpu.VMEM((3, d_model, FC), BF16),
            pltpu.VMEM((LOCAL_EXPERTS * slots, d_model), BF16),
            pltpu.VMEM(bias_table.shape, F32), pltpu.VMEM((2 * HEADS, seq, seq), F32),
            pltpu.VMEM((seq, 3 * width), BF16), pltpu.VMEM((2, hb, seq, width), BF16),
            pltpu.VMEM((hb * seq, d_model), BF16), pltpu.VMEM((hb * seq, d_model), F32),
            pltpu.VMEM((2, 2, hb, width, seq), BF16), pltpu.VMEM((hb, seq, d_model), BF16),
            pltpu.VMEM((2, hb, width, seq), BF16), pltpu.VMEM((8, hb, seq, d_model), BF16), pltpu.VMEM((8, 2, tokens), jnp.int32), pltpu.VMEM((2, tokens), jnp.int32),
        ] + [dma((n_items,))] * 8 + [dma((3,)), dma((3,)), dma((9,)), dma((6,)),
                                     dma((28,)), dma((28,)), dma((8,)), dma((8,)), dma((2,)), dma((2,))],
        compiler_params=pltpu.CompilerParams(collective_id=0, has_side_effects=True, vmem_limit_bytes=65470 * 1024),
        name="dense_layers",
    )(hid, lna, lnf, wq, wk, wv, wo, wg, wu, wd, bias_table, ids, w_router)


def moe_kernel(rows_in, aux, own_h, w_in, w_out,
               out_ref,
               rows, res, ret, win, wout, acc, total,
               rsend, rrecv, wsem, isem):
    tp, ep, to_y, to_x, to_c = swap_targets()
    n_exp, local_slots, d_model = rows.shape
    capacity = local_slots // 8
    tokens = own_h.shape[0]
    chunk = win.shape[2]
    n_chunks = w_in.shape[2] // chunk
    eps = [ep, to_c['ep'], to_x['ep'], lax.rem(to_c['ep'] + 2, 4)]
    tps = [tp, 1 - tp]
    me = tp * 4 + ep
    away = [(i, j) for i in (1, 0) for j in (2, 3, 0, 1) if (i, j) != (0, 0)]

    def target(i, j):
        return {'tp': tps[i], 'ep': eps[j]}

    def remote(src, dst, send, recv, to):
        return pltpu.make_async_remote_copy(src_ref=src, dst_ref=dst, send_sem=send, recv_sem=recv,
                                            device_id=to, device_id_type=MESH)

    def weight_copies(e, c):
        at = pl.ds(c * chunk, chunk)
        return (pltpu.make_async_copy(w_in.at[e, :, at], win.at[c], wsem.at[0, c]),
                pltpu.make_async_copy(w_out.at[e, at, :], wout.at[c], wsem.at[1, c]))

    def row_copy(e):
        return pltpu.make_async_copy(rows_in.at[e], rows.at[e], isem.at[e])

    row_copy(0).start()
    for c in range(n_chunks):
        for copy in weight_copies(0, c):
            copy.start()
    for e in range(1, n_exp):
        row_copy(e).start()
    greet([target(i, j) for i, j in away])
    total[...] = jnp.zeros_like(total)

    def returns(e):
        return [remote(res.at[e, tps[i] * 4 + eps[j]], ret.at[e, me], rsend.at[4 * i + j, e], rrecv.at[4 * i + j, e], target(i, j))
                for i, j in away]

    def combine(e):
        for copy in returns(e):
            copy.wait_recv()
        block = 256
        columns = lax.broadcasted_iota(jnp.int32, (block, local_slots), 1).astype(F32)
        table = ret[e].reshape(local_slots, d_model)

        def body(r, carry):
            at = pl.ds(pl.multiple_of(r * block, block), block)
            add = total[at, :]
            for c in range(2):
                want = aux[at, c * 8:c * 8 + 1] - (e * local_slots).astype(F32)
                select = jnp.where(columns == want, 1.0, 0.0).astype(BF16)
                add = add + aux[at, 32 + c:33 + c] * jnp.dot(select, table, preferred_element_type=F32)
            total[at, :] = add
            return carry
        lax.fori_loop(0, tokens // block, body, 0)

    lag = 3

    def expert(e, carry):
        row_copy(e).wait()
        table = rows[e]
        for c in range(n_chunks):
            for copy in weight_copies(e, c):
                copy.wait()
            up = jnp.dot(table, win[c], preferred_element_type=F32)
            out = jnp.dot(jax.nn.gelu(up).astype(BF16), wout[c], preferred_element_type=F32)
            if c == 0:
                acc[...] = out
            elif c < n_chunks - 1:
                acc[...] = acc[...] + out
            else:
                res[e] = (acc[...] + out).astype(BF16).reshape(8, capacity, d_model)

            @pl.when(e < n_exp - 1)
            def _():
                for copy in weight_copies(e + 1, c):
                    copy.start()
        for copy in returns(e):
            copy.start()
        ret[e, me] = res[e, me]

        @pl.when(e >= lag)
        def _():
            combine(e - lag)
        return carry
    lax.fori_loop(0, n_exp, expert, 0)

    def last(e, carry):
        combine(e)
        return carry
    lax.fori_loop(n_exp - lag, n_exp, last, 0)
    out_ref[...] = (own_h[...].astype(F32) + total[...]).astype(BF16).reshape(out_ref.shape)


    def drain(e, carry):
        for copy in returns(e):
            copy.wait_send()
        return carry
    lax.fori_loop(0, n_exp, drain, 0)


def moe_layer(rows, aux, own_h, w_in, w_out, out_shape):
    n_exp, slots, d_model = rows.shape
    tokens = own_h.shape[0]
    ff = w_in.shape[2]
    capacity = slots // 8
    chunk = 768
    n_chunks = ff // chunk
    vmem = pl.BlockSpec(memory_space=pltpu.VMEM)
    any_spec = pl.BlockSpec(memory_space=pl.ANY)
    dma = pltpu.SemaphoreType.DMA
    slot_rows = pltpu.VMEM((n_exp, 8, capacity, d_model), BF16)
    return pl.pallas_call(
        moe_kernel,
        in_specs=[any_spec, vmem, vmem] + [any_spec] * 2,
        out_specs=vmem,
        out_shape=jax.ShapeDtypeStruct(out_shape, BF16),
        scratch_shapes=[
            pltpu.VMEM((n_exp, slots, d_model), BF16), slot_rows, slot_rows,
            pltpu.VMEM((n_chunks, d_model, chunk), BF16), pltpu.VMEM((n_chunks, chunk, d_model), BF16),
            pltpu.VMEM((slots, d_model), F32), pltpu.VMEM((tokens, d_model), F32),
            dma((8, n_exp)), dma((8, n_exp)), dma((2, n_chunks)), dma((n_exp,)),
        ],
        compiler_params=pltpu.CompilerParams(collective_id=1, has_side_effects=True, vmem_limit_bytes=62 * 1024 * 1024),
        name="moe_layer",
    )(rows, aux, own_h, w_in, w_out)


def solution(mesh):
    act_spec = P(('dp', 'ep'), 'tp', None)
    col_spec = P(None, None, 'tp')
    row_spec = P(None, 'tp', None)
    expert_spec = P(('tp', 'ep'), None, None)
    cache_spec = P(None, ('dp', 'ep'), 'tp', None, None)
    in_specs = (act_spec, P(), P(), col_spec, col_spec, col_spec, row_spec, row_spec,
                P(None, 'tp'), P(None, 'tp'), P('tp', None), P(), expert_spec, expert_spec, act_spec)

    def device_fn(hidden_in, ln_attn, ln_ffn, w_query, w_key, w_value, w_out, bias_table, w_gate, w_up, w_down, w_router, expert_in, expert_out, expert_ids):
        nb, npos, d_model = hidden_in.shape
        rows, aux, own_h, k_all, v_all = dense_layers(
            hidden_in, ln_attn, ln_ffn, w_query, w_key, w_value, w_out, w_gate, w_up, w_down,
            jnp.swapaxes(bias_table, 0, 1), jnp.swapaxes(expert_ids, 1, 2), w_router.T)
        hidden = moe_layer(rows, aux, own_h, expert_in, expert_out, hidden_in.shape)
        caches = [jnp.swapaxes(full.reshape(2, nb, -1, 64, 2 * npos), 3, 4) for full in (k_all, v_all)]
        return hidden, caches[0], caches[1]

    return jax.shard_map(device_fn, mesh=mesh, in_specs=in_specs, out_specs=(act_spec, cache_spec, cache_spec), check_vma=False)
```

```python
import jax
import jax.numpy as jnp
from jax import lax
from jax.experimental import pallas as pl
from jax.experimental.pallas import tpu as pltpu
from jax.sharding import PartitionSpec as P

EXACT_BUCKETS = 16
THRESHOLDS = (18, 20, 23, 26, 30, 34, 39, 45, 51, 58, 66, 76, 86, 98, 112)
EPSILON = 1e-6
BF16 = jnp.bfloat16
F32 = jnp.float32

def bucket_hot(buckets, seq_len):
    k = lax.broadcasted_iota(jnp.int32, (buckets, seq_len), 1)
    rel = jnp.where(k == 0, 0, seq_len - k)
    bucket = jnp.minimum(rel, EXACT_BUCKETS)
    for threshold in THRESHOLDS:
        bucket = bucket + jnp.where(rel >= threshold, 1, 0)
    return jnp.where(bucket == lax.broadcasted_iota(jnp.int32, (buckets, seq_len), 0), 1.0, 0.0)


MESH = pl.DeviceIdType.MESH
HEADS = 6
NQ = 192
NO = 96
NF = 128
FC = 512
WINDOW = 5
HERE, THERE = range(2)
SELF, CORE, ACROSS, CORNER = range(4)
LOCAL_EXPERTS = 8
CAPACITY = 64


def swap_targets():
    tp = lax.axis_index('tp')
    ep = lax.axis_index('ep')
    core = ep + 1 - 2 * lax.rem(ep, 2)
    across = lax.rem(ep + 2, 4)
    return tp, ep, {'tp': 1 - tp}, {'ep': across}, {'ep': core}


def greet(targets):
    barrier = pltpu.get_barrier_semaphore()
    for target in targets:
        pl.semaphore_signal(barrier, inc=1, device_id=target, device_id_type=MESH)
    pl.semaphore_wait(barrier, len(targets))


def attend_rows(qkv_ref, bias_ref, base, o_ref, side, s):
    width = HEADS * 64
    rows = 128
    lane = lax.broadcasted_iota(jnp.int32, (rows, 128), 1)
    units = [(pair, blk, sd) for pair in range(HEADS // 2) for blk in range(2) for sd in range(2)]
    scores = []
    for pair, blk, sd in units:
        lo = pair * 128
        keys = rows * (blk + 1)
        q = qkv_ref[blk * rows:(blk + 1) * rows, lo:lo + 128]
        k = qkv_ref[0:keys, width + lo:width + lo + 128]
        mine = (lane < 64) if sd == 0 else (lane >= 64)
        qh = jnp.where(mine, q, jnp.zeros_like(q))
        sc = lax.dot_general(qh, k, (((1,), (1,)), ((), ())), preferred_element_type=F32)
        scores.append(sc * 0.125 + bias_ref[base + 2 * pair + sd, blk * rows:(blk + 1) * rows, 0:keys])
    tops = [jnp.max(sc, axis=1, keepdims=True) for sc in scores]
    exps = [jnp.exp(sc - m) for sc, m in zip(scores, tops)]
    sums = [jnp.sum(p, axis=1, keepdims=True) for p in exps]
    probs = [(p * (1.0 / l)).astype(BF16) for p, l in zip(exps, sums)]
    outs = []
    for (pair, blk, sd), p in zip(units, probs):
        lo = pair * 128
        v = qkv_ref[0:rows * (blk + 1), 2 * width + lo:2 * width + lo + 128]
        outs.append(jnp.dot(p, v, preferred_element_type=F32))
    for i in range(0, len(units), 2):
        pair, blk, _ = units[i]
        o_ref[side, s, blk * rows:(blk + 1) * rows, pair * 128:pair * 128 + 128] = jnp.where(
            lane < 64, outs[i], outs[i + 1]).astype(BF16)


def dense_kernel(hid, lna, lnf, wq, wk, wv, wo, wg, wu, wd, table_own, ids, w_router,
                 rows_out, aux, own_h, kc, vc,
                 own_qkv, own_o, own_g, own_u, peer_qkv, peer_o, peer_g, peer_u, pool,
                 table_peer, bias, qkv, o_all, b_all, acc, kvt, other, kvp_ref, h_all, slots_all, ids_row,
                 ysend, yrecv, xsend, xrecv, csend, crecv, dsend, drecv, hsend, hrecv, lsem, osem,
                 asend, arecv, ssend, srecv, ksend, krecv):
    tp, ep, to_y, to_x, to_c = swap_targets()
    eps = [ep, to_c['ep'], to_x['ep'], lax.rem(to_c['ep'] + 2, 4)]
    tps = [tp, 1 - tp]
    me = tp * 4 + ep
    away = [(i, j) for i in (1, 0) for j in (2, 3, 0, 1) if (i, j) != (0, 0)]
    n_exp, capacity = LOCAL_EXPERTS, CAPACITY
    local_slots = n_exp * capacity

    def target(i, j):
        return {'tp': tps[i], 'ep': eps[j]}

    across = lax.rem(ep + 2, 4)
    x_ref = h_all.at[0]
    _, hb, seq, d_model = h_all.shape
    half = seq // 2
    tokens = hb * seq
    width = HEADS * 64
    ff = wd.shape[0]

    attn = [[('w', l, m) for m in range(3)] + [('o', l, 0)] for l in range(2)]
    ffn = [[(kind, c, 0) for kind in ('g', 'u', 'd')] for c in range(3)]
    items = attn[0] + ffn[0] + ffn[1] + ffn[2] + attn[1]
    index = {item: i for i, item in enumerate(items)}

    def source(item):
        kind, l, m = item
        if kind == 'w':
            return (wq, wk, wv)[m].at[l, pl.ds(pl.multiple_of(ep * NQ, NQ), NQ), :]
        if kind == 'o':
            return wo.at[l, pl.ds(pl.multiple_of(ep * NO, NO), NO), :]
        at = pl.multiple_of(ep * (3 * NF) + l * NF, NF)
        if kind == 'd':
            return wd.at[pl.ds(at, NF), :]
        return (wg if kind == 'g' else wu).at[:, pl.ds(at, NF)]

    def place(item, r):
        kind, l, m = item
        if kind == 'w':
            return peer_qkv.at[l, m, pl.ds(pl.multiple_of(r * NQ, NQ), NQ), :]
        if kind == 'o':
            return peer_o.at[l, pl.ds(pl.multiple_of(r * NO, NO), NO), :]
        at = pl.multiple_of(r * NF, NF)
        if kind == 'd':
            return pool.at[pl.ds(pl.multiple_of(ff + l * FC + at, NF), NF), :]
        return (peer_g if kind == 'g' else peer_u).at[l, :, pl.ds(at, NF)]

    def remote(src, dst, send, recv, target):
        return pltpu.make_async_remote_copy(src_ref=src, dst_ref=dst, send_sem=send, recv_sem=recv,
                                            device_id=target, device_id_type=MESH)

    def y_copy(item):
        i = index[item]
        return remote(source(item), place(item, ep), ysend.at[i], yrecv.at[i], to_y)

    def x_copy(item):
        i = index[item]
        return remote(place(item, ep), place(item, ep), xsend.at[i], xrecv.at[i], to_x)

    def c_copy(item):
        i = index[item]
        return remote(place(item, ep), place(item, ep), csend.at[i], crecv.at[i], to_c)

    def d_copy(item):
        i = index[item]
        return remote(place(item, across), place(item, across), dsend.at[i], drecv.at[i], to_c)

    def pass_on(*names):
        for item in names:
            y_copy(item).wait_recv()
            if index[item] + WINDOW < len(sends):
                sends[index[item] + WINDOW].start()
            x_copy(item).start()
            c_copy(item).start()

    def pass_core(*names):
        for item in names:
            x_copy(item).wait_recv()
            d_copy(item).start()

    def complete(*names):
        for item in names:
            c_copy(item).wait_recv()
            d_copy(item).wait_recv()

    mine_at = pl.ds(tp * hb, hb)
    peer_at = pl.ds((1 - tp) * hb, hb)
    rows_at = pl.ds(pl.multiple_of(tp * half, half), half)
    hid_a = remote(hid.at[peer_at], x_ref.at[:, rows_at, :], hsend.at[0], hrecv.at[0], to_y)
    hid_b = remote(hid.at[mine_at], other.at[:, rows_at, :], hsend.at[1], hrecv.at[1], to_y)
    sends = [y_copy(item) for item in items] + [hid_b]
    u_copy = remote(table_own, table_peer, hsend.at[2], hrecv.at[2], to_y)
    loads = [pltpu.make_async_copy(s, d, lsem.at[i]) for i, (s, d) in enumerate([
        (hid.at[mine_at], x_ref.at[:, rows_at, :]),
        (wq, own_qkv.at[0]), (wk, own_qkv.at[1]), (wv, own_qkv.at[2]), (wo, own_o),
        (wg, own_g), (wu, own_u), (wd, pool.at[0:ff]),
        (hid.at[peer_at], other.at[:, rows_at, :])])]

    def piece(i, j):
        return h_all.at[4 * i + j]

    def fetch(n_sem, src, dst, k, to):
        return remote(piece(*src).at[k], piece(*dst).at[k], asend.at[n_sem], arecv.at[n_sem], to)

    y = [fetch(k, (HERE, SELF), (THERE, SELF), k, to_y) for k in range(hb)]
    x = [fetch(4 + k, (HERE, SELF), (HERE, ACROSS), k, to_x) for k in range(hb)]
    dx = [fetch(8 + k, (THERE, SELF), (THERE, ACROSS), k, to_x) for k in range(hb)]
    c_y = [fetch(12 + k, (THERE, SELF), (THERE, CORE), k, to_c) for k in range(hb)]
    c_x = [fetch(16 + k, (HERE, ACROSS), (HERE, CORNER), k, to_c) for k in range(hb)]
    c_d = [fetch(20 + k, (THERE, ACROSS), (THERE, CORNER), k, to_c) for k in range(hb)]
    c_0 = [fetch(24 + k, (HERE, SELF), (HERE, CORE), k, to_c) for k in range(hb)]
    y_a, y_b, y_c, y_d = y
    x_a, x_b, x_c, x_d = x
    dx_a, dx_b, dx_c, dx_d = dx
    c_y_a, c_y_b, c_y_c, c_y_d = c_y
    c_x_a, c_x_b, c_x_c, c_x_d = c_x
    c_d_a, c_d_b, c_d_c, c_d_d = c_d
    c_0_a, c_0_b, c_0_c, c_0_d = c_0
    fetches = y + x + dx + c_y + c_x + c_d + c_0
    first, second = (0, hb // 2), (hb // 2, hb)

    def begin(*copies):
        for copy in copies:
            copy.start()

    def arrived(*copies):
        for copy in copies:
            copy.wait_recv()

    kv_send = [remote(kvp_ref.at[m], (kc, vc)[m].at[1, mine_at], ksend.at[m], krecv.at[m], to_y) for m in range(2)]

    greet([target(i, j) for i, j in away])
    hid_a.start()
    u_copy.start()
    sends[0].start()
    for load in loads:
        load.start()

    def fill_bias(src, l, base):
        row = lax.broadcasted_iota(jnp.int32, (seq, seq), 0)
        col = lax.broadcasted_iota(jnp.int32, (seq, seq), 1)
        lines = jnp.dot(src[:, l, :], bucket_hot(src.shape[2], seq), precision=lax.Precision.HIGHEST, preferred_element_type=F32)
        for h in range(HEADS):
            line = jnp.broadcast_to(lines[h:h + 1, :], (seq, seq))
            toeplitz = pltpu.roll(line, 0, 1, stride=1, stride_axis=0)
            bias[base + h] = jnp.where(col <= row, toeplitz, -jnp.inf)

    def normed(rows, scale):
        wide = rows.astype(F32)
        inv = lax.rsqrt(jnp.mean(wide * wide, axis=-1, keepdims=True) + EPSILON)
        return (wide * inv * scale).astype(BF16)

    def heads_pass(l, side, midway):
        def body(s, carry):
            for k, step in midway.items():
                pl.when(s == k)(step)
            a = normed(x_ref[s], lna[l:l + 1, :])
            for m in range(3):
                w = own_qkv[m, l] if side == 0 else peer_qkv[l, m]
                part = jnp.dot(a, w, preferred_element_type=F32).astype(BF16)
                qkv[:, m * width:(m + 1) * width] = part
                if m > 0:
                    if side == 0:
                        kvt[l, m - 1, s] = part.T
                    elif l == 1:
                        kvp_ref[m - 1, s] = part.T
            attend_rows(qkv, bias, side * HEADS, o_all, side, s)
            if side == 1:
                out = jnp.dot(o_all[0, s], own_o[l], preferred_element_type=F32)
                out = out + jnp.dot(o_all[1, s], peer_o[l], preferred_element_type=F32)
                x_ref[s] = (x_ref[s].astype(F32) + out).astype(BF16)
            return carry
        lax.fori_loop(0, hb, body, 0)

    def ffn_chunk(gate, up, down):
        def body(r, carry):
            at = pl.ds(pl.multiple_of(r * FC, FC), FC)
            b = b_all[at, :]
            g = jnp.dot(b, gate[...], preferred_element_type=F32)
            u = jnp.dot(b, up[...], preferred_element_type=F32)
            hidden = (jax.nn.gelu(g) * u).astype(BF16)
            out = jnp.dot(hidden, down[...], preferred_element_type=F32)
            acc[at, :] = acc[at, :] + out
            return carry
        lax.fori_loop(0, 2, body, 0)

    def ffn_loop(own, steps):
        def body(c, carry):
            at = pl.ds(pl.multiple_of(c * FC, FC), FC)
            if own:
                ffn_chunk(own_g.at[:, at], own_u.at[:, at], pool.at[at, :])
            else:
                ffn_chunk(peer_g.at[c], peer_u.at[c], pool.at[pl.ds(pl.multiple_of(ff + c * FC, FC), FC), :])
            for k, step in enumerate(steps):
                pl.when(c == k)(step)
            return carry
        lax.fori_loop(0, ff // FC, body, 0)

    slot_iota = lax.broadcasted_iota(jnp.int32, (local_slots, 2 * half), 0)

    def pick(*units):
        start, end = units[0], units[-1]

        def blend(n, low, high):
            return low + n * (high - low)

        def body(step, carry):
            n, p = step // 2, lax.rem(step, 2)
            lo = blend(n, start[2][0], end[2][0])
            index_of = blend(n, 4 * start[0] + start[1], 4 * end[0] + end[1])
            tp_of = blend(n, tps[start[0]], tps[end[0]])
            ep_of = blend(n, eps[start[1]], eps[end[1]])
            h = h_all[index_of, pl.ds(lo, 2), pl.ds(pl.multiple_of(p * half, half), half), :].reshape(2 * half, d_model)
            b = normed(h, lnf[1:2, :])
            g = p * 4 + ep_of
            off = pl.multiple_of(tp_of * (hb * half) + lo * half, 2 * half)
            loc = slots_all[g, :, pl.ds(off, 2 * half)] - me * local_slots
            match = (slot_iota == loc[0:1, :]) | (slot_iota == loc[1:2, :])
            select = jnp.where(match, 1.0, 0.0).astype(BF16)
            got = jnp.dot(select, b, preferred_element_type=F32).astype(BF16)
            for e in range(n_exp):
                at = pl.ds(pl.multiple_of(e * local_slots + g * capacity, capacity), capacity)
                pool[at, :] = pool[at, :] + got[e * capacity:(e + 1) * capacity, :]
            return carry
        lax.fori_loop(0, 2 * len(units), body, 0)

    w0 = [('w', 0, m) for m in range(3)]
    w1 = [('w', 1, m) for m in range(3)]
    w1_a, w1_b, w1_c = w1
    o0, o1 = ('o', 0, 0), ('o', 1, 0)
    g = [('g', c, 0) for c in range(3)]
    u = [('u', c, 0) for c in range(3)]
    d = [('d', c, 0) for c in range(3)]
    g_a, g_b, g_c = g
    u_a, u_b, u_c = u
    d_a, d_b, d_c = d

    for k in range(ids.shape[0]):
        ids_row[:, k * half:(k + 1) * half] = ids[k]
    experts = lax.broadcasted_iota(jnp.int32, (64, tokens), 0)
    hot = [experts == ids_row[c:c + 1, :] for c in range(2)]
    ones = [jnp.where(h, 1.0, 0.0) for h in hot]
    earlier = jnp.where(lax.broadcasted_iota(jnp.int32, (tokens, tokens), 0)
                        < lax.broadcasted_iota(jnp.int32, (tokens, tokens), 1), 1.0, 0.0).astype(BF16)
    before = [jnp.dot(o.astype(BF16), earlier, preferred_element_type=F32) for o in ones]
    before[1] = before[1] + jnp.sum(ones[0], axis=1, keepdims=True)
    for c in range(2):
        pos = jnp.sum(jnp.where(hot[c], before[c], 0.0), axis=0, keepdims=True).astype(jnp.int32)
        slots_all[me, c:c + 1, :] = jnp.where(pos < capacity, ids_row[c:c + 1, :] * capacity + pos, -1)
    slot_sends = [remote(slots_all.at[me], slots_all.at[me], ssend.at[4 * i + j], srecv.at[4 * i + j], target(i, j))
                  for i, j in away]
    for copy in slot_sends:
        copy.start()
    for c in range(2):
        slot = slots_all[me, c:c + 1, :]
        expert = lax.shift_right_arithmetic(slot, 6)
        key = lax.bitwise_and(expert, 7) * local_slots + lax.shift_right_arithmetic(expert, 3) * capacity + lax.bitwise_and(slot, 63)
        key = jnp.where(slot < 0, -1, key).astype(F32)
        aux[:, c * 8:(c + 1) * 8] = jnp.broadcast_to(key, (8, tokens)).T
        aux[:, 16 + c * 8:24 + c * 8] = jnp.broadcast_to(ids_row[c:c + 1, :].astype(F32), (8, tokens)).T

    fill_bias(table_own, 0, 0)
    u_copy.wait_recv()
    fill_bias(table_peer, 0, HEADS)
    loads[0].wait()
    hid_a.wait_recv()
    for copy in sends[1:WINDOW]:
        copy.start()
    for load in loads[1:4]:
        load.wait()
    heads_pass(0, 0, {})
    pass_on(*w0, o0)
    pass_core(*w0)
    pass_on(g_a)
    pass_core(o0)
    complete(*w0, o0)
    pass_on(u_a)
    loads[4].wait()

    def midway():
        pass_on(d_a)
        pass_core(g_a)
    heads_pass(0, 1, {hb // 2: midway})
    pass_core(u_a)
    pass_on(g_b)

    def norm_rows(s, carry):
        b_all[pl.ds(pl.multiple_of(s * seq, seq), seq), :] = normed(x_ref[s], lnf[0:1, :])
        return carry
    lax.fori_loop(0, hb, norm_rows, 0)
    for load in loads[5:8]:
        load.wait()
    acc[...] = jnp.zeros_like(acc)

    def own_a():
        pass_on(u_b)
        pass_core(d_a)

    def own_b():
        pass_core(g_b)
        pass_on(d_b)
        pass_core(u_b)

    def own_c():
        pass_on(g_c)
        complete(g_a, u_a, d_a)
    ffn_loop(True, [own_a, own_b, own_c])

    def peer_a():
        pass_core(d_b, g_c)
        pass_on(u_c)
        complete(g_b, u_b, d_b)

    def peer_b():
        fill_bias(table_own, 1, 0)
        pass_on(d_c)
        pass_core(u_c)
        fill_bias(table_peer, 1, HEADS)
        pass_on(w1_a)
        pass_core(d_c)
        complete(g_c, u_c, d_c)
    ffn_loop(False, [peer_a, peer_b])

    def add_rows(s, carry):
        x_ref[s] = (x_ref[s].astype(F32) + acc[pl.ds(pl.multiple_of(s * seq, seq), seq), :]).astype(BF16)
        return carry
    lax.fori_loop(0, hb, add_rows, 0)

    pass_on(w1_b, w1_c)
    pass_core(w1_a)

    def own_midway():
        pass_on(o1)
        pass_core(w1_b, w1_c)
    heads_pass(1, 0, {hb // 2: own_midway})
    pass_core(o1)
    complete(*w1, o1)
    for item in d:
        x_copy(item).wait_send()
        c_copy(item).wait_send()
        d_copy(item).wait_send()
    stores = [pltpu.make_async_copy(kvt.at[l, m], (kc, vc)[m].at[l, mine_at], osem.at[2 * l + m])
              for l in range(2) for m in range(2)]
    begin(*stores)
    ready = [lambda: begin(y_a, x_a, c_0_a), lambda: begin(y_b, x_b, c_0_b), lambda: begin(y_c, x_c, c_0_c)]
    heads_pass(1, 1, {k + 1: step for k, step in enumerate(ready)})
    begin(c_0_d)

    pool[...] = jnp.zeros_like(pool)
    for copy in slot_sends:
        copy.wait_recv()
    pick((HERE, SELF, first), (HERE, SELF, second))
    loads[8].wait()
    hid_b.wait_recv()
    stores[0].wait()
    stores[1].wait()

    def other_rows(s, carry):
        a = normed(other[s], lna[0:1, :])
        for m in range(2):
            kvt[0, m, s] = jnp.dot(a, own_qkv[m + 1, 0], preferred_element_type=F32).astype(BF16).T
        return carry
    lax.fori_loop(0, hb, other_rows, 0)
    more = [pltpu.make_async_copy(kvt.at[0, m], (kc, vc)[m].at[0, peer_at], osem.at[4 + m]) for m in range(2)]
    begin(*more)

    arrived(*c_0)
    pick((HERE, CORE, first), (HERE, CORE, second))
    arrived(x_a)
    begin(x_d, c_x_a)
    arrived(x_b)
    begin(c_x_b)
    arrived(y_a)
    begin(y_d, dx_a, c_y_a)
    arrived(y_b)
    begin(dx_b, kv_send[0], c_y_b)
    pick((HERE, ACROSS, first), (THERE, SELF, first))
    arrived(c_x_a, c_x_b, c_y_a, c_y_b)
    pick((HERE, CORNER, first), (THERE, CORE, first))
    arrived(y_c)
    begin(dx_c, kv_send[1], c_y_c)
    arrived(y_d)
    begin(dx_d, c_y_d)
    arrived(c_y_c, c_y_d)
    pick((THERE, SELF, second), (THERE, CORE, second))

    pos_at = pl.ds(pl.multiple_of(tp * half, half), half)
    for i in range(2):
        at = pl.ds(pl.multiple_of(tps[i] * (hb * half), hb * half), hb * half)
        h = piece(i, 0)[:, pos_at, :].reshape(hb * half, d_model)
        own_h[at, :] = h
        logits = lax.dot_general(normed(h, lnf[1:2, :]).astype(F32), w_router[...], (((1,), (1,)), ((), ())),
                                 precision=lax.Precision.HIGHEST, preferred_element_type=F32)
        ex = jnp.exp(logits - jnp.max(logits, axis=1, keepdims=True))
        probs = ex / jnp.sum(ex, axis=1, keepdims=True)
        lanes = lax.broadcasted_iota(jnp.int32, probs.shape, 1).astype(F32)
        picked = [jnp.sum(jnp.where(lanes == aux[at, 16 + c * 8:17 + c * 8], probs, 0.0), axis=1, keepdims=True) for c in range(2)]
        denom = picked[0] + picked[1]
        for c in range(2):
            aux[at, 32 + c:33 + c] = picked[c] / denom

    arrived(x_c)
    begin(c_x_c)
    arrived(x_d)
    begin(c_x_d)
    arrived(c_x_c, c_x_d)
    pick((HERE, ACROSS, second), (HERE, CORNER, second))
    arrived(dx_a)
    begin(c_d_a)
    arrived(dx_b)
    begin(c_d_b)
    arrived(c_d_a, c_d_b)
    pick((THERE, ACROSS, first), (THERE, CORNER, first))
    arrived(dx_c)
    begin(c_d_c)
    arrived(dx_d)
    begin(c_d_d)
    pick((THERE, ACROSS, second))
    arrived(c_d_c, c_d_d)
    pick((THERE, CORNER, second))

    out = [pltpu.make_async_copy(pool.at[e * local_slots:(e + 1) * local_slots], rows_out.at[e], lsem.at[e]) for e in range(n_exp)]
    begin(*out)
    for copy in out + stores[2:] + more:
        copy.wait()
    for copy in [hid_a, hid_b, u_copy] + fetches + slot_sends:
        copy.wait_send()
    for copy in kv_send:
        copy.wait()
    for item in items:
        y_copy(item).wait_send()
        if item not in d:
            x_copy(item).wait_send()
            c_copy(item).wait_send()
            d_copy(item).wait_send()


def dense_layers(hid, lna, lnf, wq, wk, wv, wo, wg, wu, wd, bias_table, ids, w_router):
    nb, npos, d_model = hid.shape
    hb, seq = nb // 2, 2 * npos
    tokens = nb * npos
    width = HEADS * 64
    ff = wg.shape[1]
    any_spec = pl.BlockSpec(memory_space=pl.ANY)
    vmem = pl.BlockSpec(memory_space=pltpu.VMEM)
    n_items = 17
    dma = pltpu.SemaphoreType.DMA
    slots = LOCAL_EXPERTS * CAPACITY
    return pl.pallas_call(
        dense_kernel,
        in_specs=[any_spec, vmem, vmem] + [any_spec] * 7 + [vmem] * 3,
        out_specs=[any_spec, vmem, vmem, any_spec, any_spec],
        out_shape=[jax.ShapeDtypeStruct((LOCAL_EXPERTS, slots, d_model), BF16),
                   jax.ShapeDtypeStruct((tokens, 128), F32),
                   jax.ShapeDtypeStruct((tokens, d_model), BF16),
                   jax.ShapeDtypeStruct((2, nb, width, seq), BF16),
                   jax.ShapeDtypeStruct((2, nb, width, seq), BF16)],
        scratch_shapes=[
            pltpu.VMEM((3, 2, d_model, width), BF16), pltpu.VMEM((2, width, d_model), BF16),
            pltpu.VMEM((d_model, ff), BF16), pltpu.VMEM((d_model, ff), BF16),
            pltpu.VMEM((2, 3, d_model, width), BF16), pltpu.VMEM((2, width, d_model), BF16),
            pltpu.VMEM((3, d_model, FC), BF16), pltpu.VMEM((3, d_model, FC), BF16),
            pltpu.VMEM((LOCAL_EXPERTS * slots, d_model), BF16),
            pltpu.VMEM(bias_table.shape, F32), pltpu.VMEM((2 * HEADS, seq, seq), F32),
            pltpu.VMEM((seq, 3 * width), BF16), pltpu.VMEM((2, hb, seq, width), BF16),
            pltpu.VMEM((hb * seq, d_model), BF16), pltpu.VMEM((hb * seq, d_model), F32),
            pltpu.VMEM((2, 2, hb, width, seq), BF16), pltpu.VMEM((hb, seq, d_model), BF16),
            pltpu.VMEM((2, hb, width, seq), BF16), pltpu.VMEM((8, hb, seq, d_model), BF16), pltpu.VMEM((8, 2, tokens), jnp.int32), pltpu.VMEM((2, tokens), jnp.int32),
        ] + [dma((n_items,))] * 8 + [dma((3,)), dma((3,)), dma((9,)), dma((6,)),
                                     dma((28,)), dma((28,)), dma((8,)), dma((8,)), dma((2,)), dma((2,))],
        compiler_params=pltpu.CompilerParams(collective_id=0, has_side_effects=True, vmem_limit_bytes=65470 * 1024),
        name="dense_layers",
    )(hid, lna, lnf, wq, wk, wv, wo, wg, wu, wd, bias_table, ids, w_router)


def moe_kernel(rows_in, aux, own_h, w_in, w_out,
               out_ref,
               rows, res, ret, win, wout, acc, total,
               rsend, rrecv, wsem, isem):
    tp, ep, to_y, to_x, to_c = swap_targets()
    n_exp, local_slots, d_model = rows.shape
    capacity = local_slots // 8
    tokens = own_h.shape[0]
    chunk = win.shape[2]
    n_chunks = w_in.shape[2] // chunk
    eps = [ep, to_c['ep'], to_x['ep'], lax.rem(to_c['ep'] + 2, 4)]
    tps = [tp, 1 - tp]
    me = tp * 4 + ep
    away = [(i, j) for i in (1, 0) for j in (2, 3, 0, 1) if (i, j) != (0, 0)]

    def target(i, j):
        return {'tp': tps[i], 'ep': eps[j]}

    def remote(src, dst, send, recv, to):
        return pltpu.make_async_remote_copy(src_ref=src, dst_ref=dst, send_sem=send, recv_sem=recv,
                                            device_id=to, device_id_type=MESH)

    def weight_copies(e, c):
        at = pl.ds(c * chunk, chunk)
        return (pltpu.make_async_copy(w_in.at[e, :, at], win.at[c], wsem.at[0, c]),
                pltpu.make_async_copy(w_out.at[e, at, :], wout.at[c], wsem.at[1, c]))

    def row_copy(e):
        return pltpu.make_async_copy(rows_in.at[e], rows.at[e], isem.at[e])

    row_copy(0).start()
    for c in range(n_chunks):
        for copy in weight_copies(0, c):
            copy.start()
    for e in range(1, n_exp):
        row_copy(e).start()
    greet([target(i, j) for i, j in away])
    total[...] = jnp.zeros_like(total)

    def returns(e):
        return [remote(res.at[e, tps[i] * 4 + eps[j]], ret.at[e, me], rsend.at[4 * i + j, e], rrecv.at[4 * i + j, e], target(i, j))
                for i, j in away]

    def combine(e):
        for copy in returns(e):
            copy.wait_recv()
        block = 256
        columns = lax.broadcasted_iota(jnp.int32, (block, local_slots), 1).astype(F32)
        table = ret[e].reshape(local_slots, d_model)

        def body(r, carry):
            at = pl.ds(pl.multiple_of(r * block, block), block)
            add = total[at, :]
            for c in range(2):
                want = aux[at, c * 8:c * 8 + 1] - (e * local_slots).astype(F32)
                select = jnp.where(columns == want, 1.0, 0.0).astype(BF16)
                add = add + aux[at, 32 + c:33 + c] * jnp.dot(select, table, preferred_element_type=F32)
            total[at, :] = add
            return carry
        lax.fori_loop(0, tokens // block, body, 0)

    def first_expert():
        part = rows.shape[1] // 2
        for i in (1, 0):
            at = pl.ds(pl.multiple_of(tps[i] * part, part), part)
            for c in range(n_chunks):
                if i == 1:
                    for copy in weight_copies(0, c):
                        copy.wait()
                up = jnp.dot(rows[0, at, :], win[c], preferred_element_type=F32)
                out = jnp.dot(jax.nn.gelu(up).astype(BF16), wout[c], preferred_element_type=F32)
                acc[at, :] = out if c == 0 else acc[at, :] + out
                if i == 0:
                    for copy in weight_copies(1, c):
                        copy.start()
            res[0, pl.ds(tps[i] * 4, 4)] = acc[at, :].astype(BF16).reshape(4, capacity, d_model)
            for to, copy in zip(away, returns(0)):
                if to[0] == i:
                    copy.start()
        ret[0, me] = res[0, me]

    lag = 3

    def expert(e, carry):
        row_copy(e).wait()
        table = rows[e]
        for c in range(n_chunks):
            for copy in weight_copies(e, c):
                copy.wait()
            up = jnp.dot(table, win[c], preferred_element_type=F32)
            out = jnp.dot(jax.nn.gelu(up).astype(BF16), wout[c], preferred_element_type=F32)
            if c == 0:
                acc[...] = out
            elif c < n_chunks - 1:
                acc[...] = acc[...] + out
            else:
                res[e] = (acc[...] + out).astype(BF16).reshape(8, capacity, d_model)

            @pl.when(e < n_exp - 1)
            def _():
                for copy in weight_copies(e + 1, c):
                    copy.start()
        for copy in returns(e):
            copy.start()
        ret[e, me] = res[e, me]

        @pl.when(e >= lag)
        def _():
            combine(e - lag)
        return carry
    row_copy(0).wait()
    first_expert()
    lax.fori_loop(1, n_exp, expert, 0)

    def last(e, carry):
        combine(e)
        return carry
    lax.fori_loop(n_exp - lag, n_exp, last, 0)
    out_ref[...] = (own_h[...].astype(F32) + total[...]).astype(BF16).reshape(out_ref.shape)


    def drain(e, carry):
        for copy in returns(e):
            copy.wait_send()
        return carry
    lax.fori_loop(0, n_exp, drain, 0)


def moe_layer(rows, aux, own_h, w_in, w_out, out_shape):
    n_exp, slots, d_model = rows.shape
    tokens = own_h.shape[0]
    ff = w_in.shape[2]
    capacity = slots // 8
    chunk = 768
    n_chunks = ff // chunk
    vmem = pl.BlockSpec(memory_space=pltpu.VMEM)
    any_spec = pl.BlockSpec(memory_space=pl.ANY)
    dma = pltpu.SemaphoreType.DMA
    slot_rows = pltpu.VMEM((n_exp, 8, capacity, d_model), BF16)
    return pl.pallas_call(
        moe_kernel,
        in_specs=[any_spec, vmem, vmem] + [any_spec] * 2,
        out_specs=vmem,
        out_shape=jax.ShapeDtypeStruct(out_shape, BF16),
        scratch_shapes=[
            pltpu.VMEM((n_exp, slots, d_model), BF16), slot_rows, slot_rows,
            pltpu.VMEM((n_chunks, d_model, chunk), BF16), pltpu.VMEM((n_chunks, chunk, d_model), BF16),
            pltpu.VMEM((slots, d_model), F32), pltpu.VMEM((tokens, d_model), F32),
            dma((8, n_exp)), dma((8, n_exp)), dma((2, n_chunks)), dma((n_exp,)),
        ],
        compiler_params=pltpu.CompilerParams(collective_id=1, has_side_effects=True, vmem_limit_bytes=62 * 1024 * 1024),
        name="moe_layer",
    )(rows, aux, own_h, w_in, w_out)


def solution(mesh):
    act_spec = P(('dp', 'ep'), 'tp', None)
    col_spec = P(None, None, 'tp')
    row_spec = P(None, 'tp', None)
    expert_spec = P(('tp', 'ep'), None, None)
    cache_spec = P(None, ('dp', 'ep'), 'tp', None, None)
    in_specs = (act_spec, P(), P(), col_spec, col_spec, col_spec, row_spec, row_spec,
                P(None, 'tp'), P(None, 'tp'), P('tp', None), P(), expert_spec, expert_spec, act_spec)

    def device_fn(hidden_in, ln_attn, ln_ffn, w_query, w_key, w_value, w_out, bias_table, w_gate, w_up, w_down, w_router, expert_in, expert_out, expert_ids):
        nb, npos, d_model = hidden_in.shape
        rows, aux, own_h, k_all, v_all = dense_layers(
            hidden_in, ln_attn, ln_ffn, w_query, w_key, w_value, w_out, w_gate, w_up, w_down,
            jnp.swapaxes(bias_table, 0, 1), jnp.swapaxes(expert_ids, 1, 2), w_router.T)
        hidden = moe_layer(rows, aux, own_h, expert_in, expert_out, hidden_in.shape)
        caches = [jnp.swapaxes(full.reshape(2, nb, -1, 64, 2 * npos), 3, 4) for full in (k_all, v_all)]
        return hidden, caches[0], caches[1]

    return jax.shard_map(device_fn, mesh=mesh, in_specs=in_specs, out_specs=(act_spec, cache_spec, cache_spec), check_vma=False)
```
